128 devices in a mesh: dp: 8 (over x, z_lo), vocab: 16 (over z_hi, y, core).
Axes of the slice: x: 4, y: 4, z: 4 (z_hi: 2, z_lo: 2; z = z_hi * 2 + z_lo), core: 2. Of those that a mesh axis runs over, the one named last changes fastest.
Arguments:
- hidden: bfloat16 [1024, 2048], P('dp'), may hold values from -6 to 6
- mix_weight: bfloat16 [2048, 4], replicated, may hold values from -0.125 to 0.125
- proj_weight: bfloat16 [4, 2048, 2048], P(None, None, 'vocab'), may hold values from -0.125 to 0.125
- out_weight: bfloat16 [2048, 65536], P(None, 'vocab'), may hold values from -0.15625 to 0.15625
- saved_lse: float32 [1024, 4], P('dp'), may hold values from 1 to 30
- targets: int32 [1024], P('dp'), may hold values from 0 to 65535
- loss_scale: float32 [1024], P('dp'), may hold values from 4 to 32
Outputs:
- grad_hidden: bfloat16 [1024, 2048], P('dp', 'vocab')
- grad_mix: float32 [2048, 4], P('dp')
- grad_proj: bfloat16 [4, 2048, 2048], P(None, 'dp', 'vocab')
- grad_out: bfloat16 [2048, 65536], P('dp', 'vocab')
The draws below stay inside these ranges and needn't reach their ends.
All inputs are finite; a program needn't handle non-finite values.
Results may differ from the reference program's by a relative error of at most 0.023.
Values may be sent and summed in bfloat16 or wider, within the bound.
A program may use at most 128 MiB of HBM per device.

```python
import math
import jax
import jax.numpy as jnp
from jax import lax

D = 2048
K = 4
TOK_DEV = 128
TOKENS = 1024
VOCAB = 65536
N_DP = 8


def draw_saved_lse(key, part):
    center = jnp.log(jnp.float32(VOCAB)) - 1.9
    spread = jax.random.uniform(key, (TOKENS, K), jnp.float32, -0.3, 0.3)
    return (center + spread).astype(jnp.float32)


def draw_hidden(key, part):
    random_part = jax.random.normal(jax.random.fold_in(key, 11), (TOKENS, D), jnp.float32)
    values = random_part
    return jnp.clip(values, -6.0, 6.0).astype(jnp.bfloat16)


def touch_ends(values, rng, low, high):
    place = [jax.random.randint(jax.random.fold_in(rng, axis), (), 0, length) for axis, length in enumerate(values.shape)]
    widest = values.shape.index(max(values.shape))
    neighbour = place[:widest] + [(place[widest] + 1) % values.shape[widest]] + place[widest + 1:]
    return values.at[tuple(place)].set(low).at[tuple(neighbour)].set(high)


def steps_of(stream_key, extent, split, low, top_value):
    def one(position, blocks):
        heights = jax.random.uniform(jax.random.fold_in(jax.random.fold_in(stream_key, 6), position), (blocks,), jnp.float32, low / len(split), top_value / len(split))
        return jnp.repeat(jnp.exp(heights), extent[position] // blocks).reshape((-1,) + (1,) * (len(extent) - position - 1))

    loudness = one(*split[0])
    for cut in split[1:]:
        loudness = loudness * one(*cut)
    return loudness


def normal_values(stream_key, dims, scale, limit, pieces=(), kind=jnp.bfloat16):
    loudness = steps_of(stream_key, dims, pieces, -0.22, 0.18) if pieces else 1.0
    array = jax.random.normal(stream_key, dims, jnp.float32) * scale * loudness
    return jnp.minimum(jnp.maximum(array, -limit), limit).astype(kind)


def setup_inputs(seed: int = 0) -> dict:
    key_list = jax.random.split(jax.random.key(seed), 8)
    hidden = draw_hidden(jax.random.fold_in(key_list[7], 71), 0)
    mix_weight = normal_values(key_list[1], (D, K), D ** -0.5, 0.125)
    proj_weight = normal_values(key_list[2], (K, D, D), D ** -0.5, 0.125, ((2, 16),))
    out_weight = normal_values(key_list[3], (D, VOCAB), (4 * D // 5) ** -0.5, 0.15625, ((1, 16),))
    saved_lse = draw_saved_lse(jax.random.fold_in(key_list[7], 71), 0)
    targets = touch_ends(jax.random.randint(key_list[5], (TOKENS,), 0, VOCAB), jax.random.fold_in(key_list[5], 1), 0, VOCAB - 1).astype(jnp.int32)
    loss_scale = jnp.clip(jnp.exp(math.log(32.0) - 2.0794415 * jax.random.uniform(key_list[6], (TOKENS,), jnp.float32) ** steps_of(key_list[6], (TOKENS,), ((0, 8),), -0.2, 0.2)), 4.0, 32.0)
    return dict(hidden=hidden, mix_weight=mix_weight, proj_weight=proj_weight, out_weight=out_weight, saved_lse=saved_lse, targets=targets, loss_scale=loss_scale)


def reference(hidden, mix_weight, proj_weight, out_weight, saved_lse, targets, loss_scale):
    proj_float = proj_weight.astype(jnp.float32)
    mix_float = mix_weight.astype(jnp.float32)
    vocab_total = out_weight.shape[1]
    hidden_groups = hidden.reshape(N_DP, TOK_DEV, D)
    lse_groups = saved_lse.reshape(N_DP, TOK_DEV, K)
    target_groups = targets.reshape(N_DP, TOK_DEV)
    scale_groups = loss_scale.reshape(N_DP, TOK_DEV)

    def group_step(carry, inputs):
        embed_acc, proj_acc, mix_acc = carry
        group_hidden, group_lse, group_targets, group_scale = inputs
        hidden_float = group_hidden.astype(jnp.float32)
        mix_logits = jnp.dot(group_hidden, mix_weight, preferred_element_type=jnp.float32)
        log_mix = mix_logits - jnp.log(jnp.sum(jnp.exp(mix_logits), axis=1, keepdims=True))
        mix_prob = jnp.exp(log_mix)
        pre_act = jnp.einsum("td,kde->tke", hidden_float, proj_float, precision=lax.Precision.HIGHEST)
        comp = jnp.tanh(pre_act).astype(jnp.bfloat16)
        comp_rows = comp.reshape(TOK_DEV * K, D)
        logits = jnp.dot(comp_rows, out_weight, preferred_element_type=jnp.float32)
        lse_flat = group_lse.reshape(TOK_DEV * K)
        probabilities = jnp.exp(logits - lse_flat[:, None])
        target_rows = jnp.broadcast_to(group_targets[:, None], (TOK_DEV, K)).reshape(TOK_DEV * K).astype(jnp.int32)
        target_logit = jnp.take_along_axis(logits, target_rows[:, None], axis=1)[:, 0].reshape(TOK_DEV, K)
        weights = jnp.exp(log_mix + target_logit - group_lse)
        responsibility = weights / jnp.sum(weights, axis=1, keepdims=True)
        coefficient = (group_scale[:, None] * responsibility).reshape(TOK_DEV * K)
        onehot = (jnp.arange(vocab_total, dtype=jnp.int32)[None, :] == target_rows[:, None]).astype(jnp.float32)
        grad_logits = (coefficient[:, None] * (probabilities - onehot)).astype(jnp.bfloat16)
        embed_term = jnp.dot(comp_rows.T, grad_logits, preferred_element_type=jnp.float32)
        embed_round = lax.optimization_barrier(embed_term.astype(jnp.bfloat16)).astype(jnp.float32)
        grad_comp = jnp.dot(grad_logits, out_weight.T, preferred_element_type=jnp.float32)
        comp_float = comp.astype(jnp.float32)
        grad_pre = (grad_comp.reshape(TOK_DEV, K, D) * (1.0 - comp_float * comp_float)).astype(jnp.bfloat16)
        pre_float = grad_pre.astype(jnp.float32)
        proj_term = jnp.einsum("td,tke->kde", hidden_float, pre_float, precision=lax.Precision.HIGHEST)
        grad_mix_logit = -group_scale[:, None] * (responsibility - mix_prob)
        mix_term = jnp.dot(hidden_float.T, grad_mix_logit, precision=lax.Precision.HIGHEST)
        hidden_grad = jnp.einsum("tke,kde->td", pre_float, proj_float, precision=lax.Precision.HIGHEST)
        hidden_grad = hidden_grad + jnp.dot(grad_mix_logit, mix_float.T, precision=lax.Precision.HIGHEST)
        new_carry = (embed_acc + embed_round, proj_acc + proj_term, mix_acc + mix_term)
        return new_carry, hidden_grad.astype(jnp.bfloat16)

    initial = (jnp.zeros((D, vocab_total), jnp.float32), jnp.zeros((K, D, D), jnp.float32), jnp.zeros((D, K), jnp.float32))
    totals, hidden_grads = lax.scan(group_step, initial, (hidden_groups, lse_groups, target_groups, scale_groups))
    embed_acc, proj_acc, mix_acc = totals
    grad_hidden = hidden_grads.reshape(N_DP * TOK_DEV, D)
    return grad_hidden, mix_acc, proj_acc.astype(jnp.bfloat16), embed_acc.astype(jnp.bfloat16)
```

```python
import functools

import jax
import jax.numpy as jnp
from jax import lax
from jax.experimental import pallas as pl
from jax.experimental.pallas import tpu as pltpu
from jax.sharding import Mesh
from jax.sharding import PartitionSpec as P

AXES = ("x", "zl", "zh", "y", "c")
DP = ("x", "zl")
VOC = ("zh", "y", "c")
MESH_ID = pl.DeviceIdType.MESH
F32 = jnp.float32
BF16 = jnp.bfloat16

T = 128
K = 4
R = T * K
U = 128
D = 2048
VL = 4096
VH = VL // 2
NC = 8
C = VH // NC


def nt(a, b):
    return lax.dot_general(a, b, (((1,), (1,)), ((), ())), preferred_element_type=F32)


def nn(a, b):
    return lax.dot_general(a, b, (((1,), (0,)), ((), ())), preferred_element_type=F32)


def kernel(
    mix_t,
    lse_t,
    scale,
    target,
    hidden_hbm,
    proj_hbm,
    w_hbm,
    gh_out,
    gm_out,
    gp_out,
    go_out,
    hidden,
    proj,
    w,
    comp,
    comp_t,
    gl,
    part,
    r1x,
    rfx,
    gcb,
    rd,
    r1a,
    rfa,
    r1b,
    rfb,
    wt,
    hs,
    hst,
    gpx,
    gpall,
    prods,
    prodr,
    gms,
    gmr,
    hts,
    hrecv,
    info2,
    lsec,
    coefc,
    tgtc,
    tl,
    pbuf,
    gh_v,
    gm_v,
    gp_v,
    sem_w,
    sem_i,
    p_s,
    p_r,
    sem_o,
    ag_s,
    ag_r,
    hs_s,
    hs_r,
    tl_s,
    tl_r,
    x_s,
    x_r,
    zx_s,
    zx_r,
    zx_l,
    d_s,
    d_r,
    a_s,
    a_r,
    b_s,
    b_r,
    h_s,
    h_r,
    g_s,
    g_r,
):
    x = lax.axis_index("x")
    zl = lax.axis_index("zl")
    zh = lax.axis_index("zh")
    y = lax.axis_index("y")
    c = lax.axis_index("c")
    z = zh * 2 + zl
    v = zh * 8 + y * 2 + c
    d = x * 2 + zl

    def m4(i):
        return lax.rem(i + 4, 4)

    def dev(x_=None, z_=None, y_=None, c_=None):
        zz = z if z_ is None else z_
        return (
            x if x_ is None else x_,
            lax.rem(zz, 2),
            lax.div(zz, 2),
            y if y_ is None else y_,
            c if c_ is None else c_,
        )

    def rc(src, dst, ss, rs, to):
        return pltpu.make_async_remote_copy(
            src_ref=src, dst_ref=dst, send_sem=ss, recv_sem=rs, device_id=to, device_id_type=MESH_ID
        )

    partner_c = dev(c_=1 - c)
    partner_z = (x, 1 - zl, zh, y, c)

    q32 = z * 8 + y * 2 + c

    def mate(o):
        p = lax.rem(q32 + o, 32)
        zz = lax.div(p, 8)
        return (x, lax.rem(zz, 2), lax.div(zz, 2), lax.rem(lax.div(p, 2), 4), lax.rem(p, 2))

    barrier = pltpu.get_barrier_semaphore()

    def greet(o, carry):
        pl.semaphore_signal(barrier, inc=1, device_id=mate(o), device_id_type=MESH_ID)
        return carry

    lax.fori_loop(1, 32, greet, 0)
    for o in range(1, 4):
        pl.semaphore_signal(barrier, inc=1, device_id=dev(x_=m4(x + o)), device_id_type=MESH_ID)

    hidden_copy = pltpu.make_async_copy(hidden_hbm, hidden, sem_w.at[0])
    proj_copy = pltpu.make_async_copy(proj_hbm, proj, sem_w.at[1])
    w_copy = pltpu.make_async_copy(
        w_hbm.at[:, pl.ds(pl.multiple_of(zl * VH, VH), VH)], w, sem_w.at[2]
    )
    hidden_copy.start()
    proj_copy.start()
    w_copy.start()
    hidden_copy.wait()
    mix_logits = nt(mix_t[...], hidden[...])
    info2[zl, 0:4] = lse_t[...]
    info2[zl, 4:8] = mix_logits - jnp.log(jnp.sum(jnp.exp(mix_logits), axis=0, keepdims=True))
    info2[zl, 8:9] = scale[...]
    info2[zl, 9:10] = target[...].astype(F32)
    info2[zl, 10:16] = jnp.zeros((6, T), F32)

    def row_columns(g):
        cols = jnp.transpose(jnp.concatenate([info2[g], jnp.zeros((112, T), F32)], axis=0))
        local = cols[:, 9:10] - (v * VL + zl * VH).astype(F32)
        for k in range(K):
            rows = pl.ds(pl.multiple_of(g * R + k * T, T), T)
            lsec[rows, :] = jnp.broadcast_to(cols[:, k : k + 1], (T, 128))
            tgtc[rows, :] = jnp.broadcast_to(local, (T, 128))

    row_columns(zl)
    info_copy = rc(info2.at[zl], info2.at[zl], sem_i.at[0], sem_i.at[1], partner_z)

    own_rows = pl.multiple_of(zl * R, R)
    own_cols = pl.multiple_of(v * U, U)

    def blk(col, z_, y_, c_, r0=0, n=2 * T):
        row = lax.rem(z_, 2) * R + col * 2 * T + r0
        lane = (lax.div(z_, 2) * 8 + y_ * 2 + c_) * U
        return comp.at[pl.ds(pl.multiple_of(row, T), n), pl.ds(pl.multiple_of(lane, U), U)]

    def pos(col):
        return (y, z) if col == 0 else (z, y)

    def at_ab(col, a_, b_, c_, r0=0, n=2 * T):
        return blk(col, b_, a_, c_, r0, n) if col == 0 else blk(col, a_, b_, c_, r0, n)

    def dev_ab(col, a_, b_):
        return dev(y_=a_, z_=b_) if col == 0 else dev(z_=a_, y_=b_)

    def ag_copy(col, i, ref, to):
        return rc(ref, ref, ag_s.at[col * 36 + i], ag_r.at[col * 36 + i], to)

    ag_sent = []

    def ag_send(col, i, ref, to):
        cp = ag_copy(col, i, ref, to)
        cp.start()
        ag_sent.append(cp)

    def ag_wait(col, i, ref):
        ag_copy(col, i, ref, partner_c).wait_recv()

    def second(col, i, ref):
        a, b = pos(col)
        ag_send(col, 4 + 4 * i, ref, dev_ab(col, a, m4(b + 1)))
        ag_send(col, 4 + 4 * i + 1, ref, dev_ab(col, a, m4(b - 1)))

    def across(col, i, j, ref):
        ag_send(col, 20 + i * 4 + j, ref, partner_c)

    proj_copy.wait()
    for k in range(K):
        pre = nn(hidden[...], proj[k])
        comp[pl.ds(pl.multiple_of(own_rows + k * T, T), T), pl.ds(own_cols, U)] = jnp.tanh(
            pre
        ).astype(BF16)
    pl.semaphore_wait(barrier, 34)
    for col in range(2):
        a, b = pos(col)
        own = at_ab(col, a, b, c)
        ag_send(col, 0, own, dev_ab(col, m4(a + 1), b))
        ag_send(col, 1, own, dev_ab(col, m4(a - 1), b))
    info_copy.start()
    for col in range(2):
        a, b = pos(col)
        own = at_ab(col, a, b, c)
        second(col, 0, own)
        across(col, 0, 0, own)

    def hs_copy(i):
        p = m4(x + (0, 1, -1, 2)[i])
        return rc(
            hidden.at[:, pl.ds(pl.multiple_of(p * 512, 512), 512)],
            hs.at[i],
            hs_s.at[i],
            hs_r.at[i],
            dev(x_=p),
        )

    for i in range(1, 4):
        hs_copy(i).start()
    hs[0] = hidden[:, pl.ds(pl.multiple_of(x * 512, 512), 512)]

    def pick(n, carry):
        rows = pl.ds(pl.multiple_of(n * 512, 512), 512)
        acc = jnp.zeros((2 * T, 512), F32)
        for q in range(4):
            lane = lax.broadcasted_iota(jnp.int32, (T, 512), 1).astype(F32) + float(q * 512)
            hot = jnp.concatenate(
                [
                    (lane == tgtc[pl.ds(g * R, T), :][:, 0:1]).astype(F32).astype(BF16)
                    for g in range(2)
                ],
                axis=0,
            )
            acc = acc + nt(hot, w[rows, pl.ds(q * 512, 512)])
        wt[:, rows] = acc.astype(BF16)
        return carry

    for col in range(2):
        a, b = pos(col)
        prev, nxt = m4(a - 1), m4(a + 1)
        ag_wait(col, 0, at_ab(col, prev, b, c))
        ag_send(col, 2, at_ab(col, prev, b, c, 0, T), dev_ab(col, nxt, b))
        second(col, 1, at_ab(col, prev, b, c))
        across(col, 1, 0, at_ab(col, prev, b, c))
        ag_wait(col, 1, at_ab(col, nxt, b, c))
        ag_send(col, 3, at_ab(col, nxt, b, c, T, T), dev_ab(col, prev, b))
        second(col, 2, at_ab(col, nxt, b, c))
        across(col, 2, 0, at_ab(col, nxt, b, c))
    info_in = rc(info2.at[1 - zl], info2.at[1 - zl], sem_i.at[0], sem_i.at[1], partner_z)
    info_in.wait_recv()
    row_columns(1 - zl)
    w_copy.wait()
    lax.fori_loop(0, 4, pick, 0)
    for col in range(2):
        a, b = pos(col)
        far = m4(a + 2)
        ag_wait(col, 2, at_ab(col, far, b, c, 0, T))
        ag_wait(col, 3, at_ab(col, far, b, c, T, T))
        second(col, 3, at_ab(col, far, b, c))
        across(col, 3, 0, at_ab(col, far, b, c))
    for i in range(4):
        for col in range(2):
            a, b = pos(col)
            a_ = m4(a + (0, -1, 1, 2)[i])
            prev, nxt = m4(b - 1), m4(b + 1)
            ag_wait(col, 4 + 4 * i, at_ab(col, a_, prev, c))
            ag_send(col, 4 + 4 * i + 2, at_ab(col, a_, prev, c, 0, T), dev_ab(col, a, nxt))
            across(col, i, 1, at_ab(col, a_, prev, c))
            ag_wait(col, 4 + 4 * i + 1, at_ab(col, a_, nxt, c))
            ag_send(col, 4 + 4 * i + 3, at_ab(col, a_, nxt, c, T, T), dev_ab(col, a, prev))
            across(col, i, 2, at_ab(col, a_, nxt, c))
    for i in range(4):
        for col in range(2):
            a, b = pos(col)
            a_ = m4(a + (0, -1, 1, 2)[i])
            far = m4(b + 2)
            ag_wait(col, 4 + 4 * i + 2, at_ab(col, a_, far, c, 0, T))
            ag_wait(col, 4 + 4 * i + 3, at_ab(col, a_, far, c, T, T))
            across(col, i, 3, at_ab(col, a_, far, c))
    for i in range(4):
        for j in range(4):
            for col in range(2):
                a, b = pos(col)
                a_ = m4(a + (0, -1, 1, 2)[i])
                b_ = m4(b + (0, -1, 1, 2)[j])
                ag_wait(col, 20 + i * 4 + j, at_ab(col, a_, b_, 1 - c))

    lane_t = lax.broadcasted_iota(jnp.int32, (T, 128), 1)
    acc = jnp.zeros((T, 128), F32)
    for g in range(2):
        for k in range(K):
            s = jnp.zeros((T, 128), F32)
            for q in range(4):
                prod = comp[pl.ds(g * R + k * T, T), pl.ds(q * 512, 512)].astype(F32) * wt[
                    pl.ds(g * T, T), pl.ds(q * 512, 512)
                ].astype(F32)
                for e in range(4):
                    s = s + prod[:, e * 128 : (e + 1) * 128]
            acc = jnp.where(lane_t == g * K + k, jnp.sum(s, axis=1, keepdims=True), acc)
    tl[0] = jnp.transpose(acc)[0:8]

    def tl_copy(o):
        return rc(tl.at[0], tl.at[o], tl_s.at[o], tl_r.at[o], mate(o))

    def tl_start(o, carry):
        tl_copy(o).start()
        return carry

    lax.fori_loop(1, 32, tl_start, 0)

    def flip(n, carry):
        cols = pl.ds(pl.multiple_of(n * U, U), U)
        for m in range(2):
            comp_t[cols, pl.ds(m * R, R)] = jnp.transpose(comp[pl.ds(m * R, R), cols])
        return carry

    lax.fori_loop(0, D // U, flip, 0)

    lane_w = lax.broadcasted_iota(jnp.int32, (2 * T, 128), 1).astype(F32)

    def chunk_logits(cc, m, put):
        rows = pl.ds(pl.multiple_of(m * 2 * T, 2 * T), 2 * T)
        logit = nn(comp[rows, :], w[:, pl.ds(pl.multiple_of(cc * C, C), C)])
        shift = jnp.asarray(cc * C, F32)
        lse_m, tgt_m = lsec[rows, :], tgtc[rows, :] - shift
        for e in range(C // 128):
            prob = jnp.exp(logit[:, e * 128 : (e + 1) * 128] - lse_m)
            hot = jnp.where(lane_w + float(e * 128) == tgt_m, 1.0, 0.0)
            put(rows, e, prob - hot)

    def hold(m, carry):
        def put(rows, e, val):
            pbuf[rows, pl.ds(e * 128, 128)] = val

        chunk_logits(0, m, put)
        return carry

    lax.fori_loop(0, 4, hold, 0)

    def tl_wait(o, carry):
        tl_copy(o).wait()
        return carry

    lax.fori_loop(1, 32, tl_wait, 0)
    target_logit = jnp.sum(tl[...], axis=0)
    coef_rows = []
    gml_rows = []
    for g in range(2):
        lse_g = info2[g, 0:4]
        lm_g = info2[g, 4:8]
        scale_g = info2[g, 8:9]
        weights = jnp.exp(lm_g + target_logit[g * K : (g + 1) * K] - lse_g)
        resp = weights / jnp.sum(weights, axis=0, keepdims=True)
        coef_rows.append(scale_g * resp)
        gml_rows.append(-scale_g * (resp - jnp.exp(lm_g)))
    table = jnp.concatenate(coef_rows + gml_rows + [jnp.zeros((112, 128), F32)], axis=0)
    cols = jnp.transpose(table)
    for g in range(2):
        for k in range(K):
            coefc[pl.ds(g * R + k * T, T), :] = jnp.broadcast_to(
                cols[:, g * K + k : g * K + k + 1], (T, 128)
            )
    gml = jnp.zeros((T, 128), F32)
    for k in range(K):
        mine = jnp.where(zl == 0, cols[:, 8 + k : 9 + k], cols[:, 12 + k : 13 + k])
        high = mine.astype(BF16).astype(F32)
        gml = jnp.where(lane_t == k, high, gml)
        gml = jnp.where(lane_t == K + k, mine - high, gml)
    gpx[4] = gml.astype(BF16)

    def ring(idx, n, piece, me, right, left, r1, rf, ss, rs):
        two, one, back = m4(me + 2), m4(me + 1), m4(me - 1)
        copies = (
            lambda: rc(piece(two, 0), r1(0), ss.at[idx], rs.at[idx], right),
            lambda: rc(piece(one, 1), rf(0, 1), ss.at[idx + 1], rs.at[idx + 1], right),
            lambda: rc(piece(two, 1), r1(1), ss.at[idx + 2], rs.at[idx + 2], left),
            lambda: rc(piece(back, 0), rf(1, 0), ss.at[idx + 3], rs.at[idx + 3], left),
            lambda: rc(piece(one, 0), rf(0, 0), ss.at[idx + 4], rs.at[idx + 4], right),
            lambda: rc(piece(back, 1), rf(1, 1), ss.at[idx + 5], rs.at[idx + 5], left),
        )

        def first(which=(0, 2, 1, 3)):
            for i in which:
                copies[i]().start()

        def add(ref, other):
            ref[...] = (ref[...].astype(F32) + other[...].astype(F32)).astype(BF16)

        def forward():
            copies[0]().wait_recv()
            add(piece(one, 0), r1(0))
            copies[4]().start()
            copies[2]().wait_recv()
            add(piece(back, 1), r1(1))
            copies[5]().start()

        def arrive():
            for i in (1, 3, 4, 5):
                copies[i]().wait_recv()

        def drain():
            for i in range(6):
                copies[i]().wait_send()

        return first, forward, arrive, drain

    x_right, x_left = dev(x_=m4(x + 1)), dev(x_=m4(x - 1))

    def x_ring(cc):
        return ring(
            cc * 6,
            6,
            lambda t, h: part.at[cc, t * 2 + h],
            x,
            x_right,
            x_left,
            lambda i: r1x.at[cc, i],
            lambda i, h: rfx.at[cc, i, h],
            x_s,
            x_r,
        )

    def chunk_out(cc):
        cols = pl.ds(pl.multiple_of(cc * C, C), C)
        for i in range(4):
            t = m4(x + (2, 1, -1, 0)[i])
            rows = pl.ds(pl.multiple_of(t * 512, 512), 512)
            res = nn(comp_t[rows, :], gl[:, cols]).astype(BF16)
            part[cc, t * 2] = res[0:256]
            part[cc, t * 2 + 1] = res[256:512]
            if i < 3:
                x_ring(cc)[0](((0, 2), (1,), (3,))[i])

    def scale_first(m, carry):
        rows = pl.ds(pl.multiple_of(m * 2 * T, 2 * T), 2 * T)
        coef_m = coefc[rows, :]
        for e in range(C // 128):
            gl[rows, pl.ds(e * 128, 128)] = (coef_m * pbuf[rows, pl.ds(e * 128, 128)]).astype(BF16)
        return carry

    lax.fori_loop(0, 4, scale_first, 0)
    chunk_out(0)

    def chunk(cc, carry):
        def rows_of(m, carry2):
            coef_m = coefc[pl.ds(pl.multiple_of(m * 2 * T, 2 * T), 2 * T), :]

            def put(rows, e, val):
                gl[rows, pl.ds(pl.multiple_of(cc * C + e * 128, 128), 128)] = (coef_m * val).astype(
                    BF16
                )

            chunk_logits(cc, m, put)
            return carry2

        lax.fori_loop(0, 4, rows_of, 0)
        chunk_out(cc)
        return carry

    lax.fori_loop(1, NC, chunk, 0)

    def comp_grad(col):
        def tile(i, carry):
            g, h, j = lax.div(i, 4), lax.rem(lax.div(i, 2), 2), lax.rem(i, 2)
            rows = pl.ds(pl.multiple_of(g * R + col * 2 * T, 2 * T), 2 * T)
            units = pl.ds(pl.multiple_of((h * 2 + j) * 512, 512), 512)
            res = nt(gl[rows, :], w[units, :])
            z_ = h * 2 + g
            for jj in range(4):
                y_ = j * 2 + jj // 2
                val = res[:, jj * 128 : (jj + 1) * 128].astype(BF16)
                if col == 0:
                    gcb[jj % 2, col, z_, y_] = val
                else:
                    gcb[jj % 2, col, y_, z_] = val
            return carry

        lax.fori_loop(0, 8, tile, 0)
        swap = rc(gcb.at[1 - c, col], rd.at[col], d_s.at[col], d_r.at[col], partner_c)
        swap.start()
        return swap

    def a_ring(col):
        me = z if col == 0 else y
        mk = (lambda p: dev(z_=p)) if col == 0 else (lambda p: dev(y_=p))
        return ring(
            col * 6,
            6,
            lambda t, h: gcb.at[c, col, t, pl.ds(2 * h, 2)],
            me,
            mk(m4(me + 1)),
            mk(m4(me - 1)),
            lambda i: r1a.at[col, i],
            lambda i, h: rfa.at[col, i, h],
            a_s,
            a_r,
        )

    def b_ring(col):
        first = z if col == 0 else y
        me = y if col == 0 else z
        mk = (lambda p: dev(y_=p)) if col == 0 else (lambda p: dev(z_=p))
        return ring(
            col * 6,
            6,
            lambda t, h: gcb.at[c, col, first, t, pl.ds(h * T, T)],
            me,
            mk(m4(me + 1)),
            mk(m4(me - 1)),
            lambda i: r1b.at[col, i],
            lambda i, h: rfb.at[col, i, h],
            b_s,
            b_r,
        )

    def merge(col, swap):
        swap.wait_recv()

        def add(i, carry):
            p, q = lax.div(i, 4), lax.rem(i, 4)
            gcb[c, col, p, q] = (gcb[c, col, p, q].astype(F32) + rd[col, p, q].astype(F32)).astype(
                BF16
            )
            return carry

        lax.fori_loop(0, 16, add, 0)

    def finish_a(col):
        me = z if col == 0 else y
        for h in range(2):
            for e in range(2):
                q = 2 * h + e
                gcb[c, col, me, q] = (
                    gcb[c, col, me, q].astype(F32)
                    + rfa[col, 0, h, e].astype(F32)
                    + rfa[col, 1, h, e].astype(F32)
                ).astype(BF16)

    def x_finish(cc):
        x_ring(cc)[2]()
        for h in range(2):
            part[cc, x * 2 + h] = (
                part[cc, x * 2 + h].astype(F32)
                + rfx[cc, 0, h].astype(F32)
                + rfx[cc, 1, h].astype(F32)
            ).astype(BF16)
        for cp in z_copies(cc):
            cp.start()

    def z_copies(cc):
        cols = pl.ds(pl.multiple_of(zl * VH + cc * C, C), C)
        dst = go_out.at[:, cols]
        return (
            rc(part.at[cc, x * 2 + 1 - zl], dst, zx_s.at[cc], zx_r.at[cc], partner_z),
            pltpu.make_async_copy(part.at[cc, x * 2 + zl], dst, zx_l.at[cc]),
        )

    for cc in range(4):
        x_ring(cc)[1]()
    swap0 = comp_grad(0)
    x_ring(4)[1]()
    swap1 = comp_grad(1)
    x_ring(5)[1]()
    merge(0, swap0)
    a_ring(0)[0]()
    merge(1, swap1)
    a_ring(1)[0]()
    a_ring(0)[1]()
    a_ring(1)[1]()
    for i in range(1, 4):
        hs_copy(i).wait()
    for i in range(4):
        hst[:, pl.ds(i * T, T)] = jnp.transpose(hs[i])
    x_ring(6)[1]()
    a_ring(0)[2]()
    finish_a(0)
    b_ring(0)[0]()
    a_ring(1)[2]()
    finish_a(1)
    b_ring(1)[0]()
    b_ring(0)[1]()
    b_ring(1)[1]()
    x_finish(0)

    for col in range(2):
        first = z if col == 0 else y
        me = y if col == 0 else z
        b_ring(col)[2]()
        for h in range(2):
            total = (
                gcb[c, col, first, me, pl.ds(h * T, T)].astype(F32)
                + rfb[col, 0, h].astype(F32)
                + rfb[col, 1, h].astype(F32)
            )
            k = 2 * col + h
            cf = comp[
                pl.ds(pl.multiple_of(own_rows + k * T, T), T), pl.ds(own_cols, U)
            ].astype(F32)
            gpx[k] = (total * (1.0 - cf * cf)).astype(BF16)

    def slot(i, r0=0, n=T):
        return gpall.at[:, pl.ds(i * T + r0, n)]

    g_copies = (
        rc(gpx, slot(1), g_s.at[0], g_r.at[0], x_right),
        rc(gpx, slot(2), g_s.at[1], g_r.at[1], x_left),
        rc(slot(1, 0, T // 2), slot(3, 0, T // 2), g_s.at[2], g_r.at[2], x_right),
        rc(slot(2, T // 2, T // 2), slot(3, T // 2, T // 2), g_s.at[3], g_r.at[3], x_left),
    )
    g_copies[0].start()
    g_copies[1].start()
    x_ring(7)[1]()

    def h_copy(o):
        p = lax.rem(v + o, 16)
        to = (x, zl, lax.div(p, 8), lax.rem(lax.div(p, 2), 4), lax.rem(p, 2))
        return rc(hts.at[o], hrecv.at[o], h_s.at[o], h_r.at[o], to)

    def h_tile(o):
        p = lax.rem(v + o, 16)
        rows = pl.ds(pl.multiple_of(p * U, U), U)
        acc = nt(gpx[0], proj[0, rows, :])
        for k in range(1, K):
            acc = acc + nt(gpx[k], proj[k, rows, :])
        return acc

    def h_step(o, carry):
        hts[o] = h_tile(o).astype(BF16)
        h_copy(o).start()
        return carry

    lax.fori_loop(1, 16, h_step, 0)
    hrecv[0] = h_tile(0).astype(BF16)
    gpall[:, pl.ds(0, T)] = gpx[...]
    x_finish(1)
    x_finish(2)
    x_finish(3)
    g_copies[0].wait_recv()
    g_copies[2].start()
    g_copies[1].wait_recv()
    g_copies[3].start()

    def h_wait(o, carry):
        h_copy(o).wait()
        return carry

    lax.fori_loop(1, 16, h_wait, 0)
    mw = jnp.concatenate(
        [mix_t[:, pl.ds(own_cols, U)].astype(F32)] * 2 + [jnp.zeros((120, U), F32)], axis=0
    ).astype(BF16)
    gh = nn(gpx[4], mw)
    for o in range(16):
        gh = gh + hrecv[o].astype(F32)
    gh_v[...] = gh.astype(BF16)
    out_copies = (
        pltpu.make_async_copy(gh_v, gh_out, sem_o.at[0]),
        pltpu.make_async_copy(gp_v, gp_out, sem_o.at[1]),
        pltpu.make_async_copy(gm_v, gm_out, sem_o.at[2]),
    )
    out_copies[0].start()
    x_finish(4)
    x_finish(5)

    g_copies[2].wait_recv()
    g_copies[3].wait_recv()

    def product(half, k):
        return nn(hst[pl.ds(pl.multiple_of(half * 256, 256), 256), :], gpall[k])

    def mix_product(half):
        res = lax.dot_general(
            gpall[4],
            hst[pl.ds(pl.multiple_of(half * 256, 256), 256), :],
            (((0,), (1,)), ((), ())),
            preferred_element_type=F32,
        )
        return res[0:4] + res[4:8]

    for k in range(K):
        prods[k] = product(1 - zl, k).astype(BF16)
    gms[...] = mix_product(1 - zl)
    p_copies = (
        rc(prods, prodr, p_s.at[0], p_r.at[0], partner_z),
        rc(gms, gmr, p_s.at[1], p_r.at[1], partner_z),
    )
    for cp in p_copies:
        cp.start()
    x_finish(6)
    x_finish(7)
    for cp in p_copies:
        cp.wait_recv()
    for k in range(K):
        gp_v[k] = (product(zl, k) + prodr[k].astype(F32)).astype(BF16)
    gm_v[...] = mix_product(zl) + gmr[...]
    out_copies[1].start()
    out_copies[2].start()

    for cp in ag_sent:
        cp.wait_send()
    for cp in (info_copy, swap0, swap1, *g_copies, *p_copies):
        cp.wait_send()
    for col in range(2):
        a_ring(col)[3]()
        b_ring(col)[3]()

    def x_drain(cc, carry):
        x_ring(cc)[3]()
        for cp in z_copies(cc):
            cp.wait()
        return carry

    lax.fori_loop(0, NC, x_drain, 0)
    for cp in out_copies:
        cp.wait()


def place(gh, gm, gp, go, gh_o, gm_o, gp_o, go_o, b_gh, b_gm, b_gp, b_go, s_in, s_out):
    pairs = [(gh, b_gh, gh_o), (gm, b_gm, gm_o), (gp, b_gp, gp_o)]
    for i in range(4):
        rows = pl.ds(i * 64, 64)
        pairs.append((go.at[rows], b_go.at[rows], go_o.at[rows]))
    loads = [pltpu.make_async_copy(s, b, s_in.at[i]) for i, (s, b, _) in enumerate(pairs)]
    stores = [pltpu.make_async_copy(b, t, s_out.at[i]) for i, (_, b, t) in enumerate(pairs)]
    for cp in reversed(loads):
        cp.start()
    for i in reversed(range(len(pairs))):
        loads[i].wait()
        stores[i].start()
    for cp in stores:
        cp.wait()


def shards(hidden, mix_weight, proj_weight, out_weight, saved_lse, targets, loss_scale):
    vm = pl.BlockSpec(memory_space=pltpu.VMEM)
    hbm = pl.BlockSpec(memory_space=pltpu.HBM)
    dma = pltpu.SemaphoreType.DMA
    outs = (
        jax.ShapeDtypeStruct((T, U), BF16),
        jax.ShapeDtypeStruct((K, 256), F32),
        jax.ShapeDtypeStruct((K, 256, U), BF16),
        jax.ShapeDtypeStruct((256, VL), BF16),
    )
    found = pl.pallas_call(
        kernel,
        out_shape=outs,
        in_specs=[vm, vm, vm, vm, hbm, hbm, hbm],
        out_specs=(hbm, hbm, hbm, hbm),
        scratch_shapes=[
            pltpu.VMEM((T, D), BF16),
            pltpu.VMEM((K, D, U), BF16),
            pltpu.VMEM((D, VH), BF16),
            pltpu.VMEM((2 * R, D), BF16),
            pltpu.VMEM((D, 2 * R), BF16),
            pltpu.VMEM((2 * R, VH), BF16),
            pltpu.VMEM((NC, 8, 256, C), BF16),
            pltpu.VMEM((NC, 2, 256, C), BF16),
            pltpu.VMEM((NC, 2, 2, 256, C), BF16),
            pltpu.VMEM((2, 2, 4, 4, 2 * T, U), BF16),
            pltpu.VMEM((2, 4, 4, 2 * T, U), BF16),
            pltpu.VMEM((2, 2, 2, 2 * T, U), BF16),
            pltpu.VMEM((2, 2, 2, 2, 2 * T, U), BF16),
            pltpu.VMEM((2, 2, T, U), BF16),
            pltpu.VMEM((2, 2, 2, T, U), BF16),
            pltpu.VMEM((2 * T, D), BF16),
            pltpu.VMEM((4, T, 512), BF16),
            pltpu.VMEM((512, 4 * T), BF16),
            pltpu.VMEM((5, T, U), BF16),
            pltpu.VMEM((5, 4 * T, U), BF16),
            pltpu.VMEM((K, 256, U), BF16),
            pltpu.VMEM((K, 256, U), BF16),
            pltpu.VMEM((K, 256), F32),
            pltpu.VMEM((K, 256), F32),
            pltpu.VMEM((16, T, U), BF16),
            pltpu.VMEM((16, T, U), BF16),
            pltpu.VMEM((2, 16, T), F32),
            pltpu.VMEM((2 * R, 128), F32),
            pltpu.VMEM((2 * R, 128), F32),
            pltpu.VMEM((2 * R, 128), F32),
            pltpu.VMEM((32, 8, T), F32),
            pltpu.VMEM((2 * R, C), F32),
            pltpu.VMEM((T, U), BF16),
            pltpu.VMEM((K, 256), F32),
            pltpu.VMEM((K, 256, U), BF16),
            dma((3,)),
            dma((2,)),
            dma((2,)),
            dma((2,)),
            dma((3,)),
            dma((72,)),
            dma((72,)),
            dma((4,)),
            dma((4,)),
            dma((32,)),
            dma((32,)),
            dma((6 * NC,)),
            dma((6 * NC,)),
            dma((NC,)),
            dma((NC,)),
            dma((NC,)),
            dma((2,)),
            dma((2,)),
            dma((12,)),
            dma((12,)),
            dma((12,)),
            dma((12,)),
            dma((16,)),
            dma((16,)),
            dma((4,)),
            dma((4,)),
        ],
        compiler_params=pltpu.CompilerParams(
            collective_id=0, has_side_effects=True, vmem_limit_bytes=67043328
        ),
    )(
        mix_weight.T,
        saved_lse.T,
        loss_scale[None, :],
        targets[None, :],
        hidden,
        proj_weight,
        out_weight,
    )
    gh, gm, gp, go = pl.pallas_call(
        place,
        out_shape=outs,
        in_specs=[hbm] * 4,
        out_specs=(hbm,) * 4,
        scratch_shapes=[pltpu.VMEM(o.shape, o.dtype) for o in outs] + [dma((7,)), dma((7,))],
    )(*found)
    return gh, gm.T, gp, go


def solution(mesh):
    finer = Mesh(mesh.devices.reshape(4, 2, 2, 4, 2), AXES)
    in_specs = (
        P(DP, None),
        P(),
        P(None, None, VOC),
        P(None, VOC),
        P(DP, None),
        P(DP),
        P(DP),
    )
    out_specs = (P(DP, VOC), P(DP, None), P(None, DP, VOC), P(DP, VOC))
    return jax.shard_map(
        shards, mesh=finer, in_specs=in_specs, out_specs=out_specs, check_vma=False
    )
```

```python
import functools

import jax
import jax.numpy as jnp
from jax import lax
from jax.experimental import pallas as pl
from jax.experimental.pallas import tpu as pltpu
from jax.sharding import Mesh
from jax.sharding import PartitionSpec as P

AXES = ("x", "zl", "zh", "y", "c")
DP = ("x", "zl")
VOC = ("zh", "y", "c")
MESH_ID = pl.DeviceIdType.MESH
F32 = jnp.float32
BF16 = jnp.bfloat16

T = 128
K = 4
R = T * K
U = 128
D = 2048
VL = 4096
VH = VL // 2
NC = 8
C = VH // NC
W2 = 2 * C


def nt(a, b):
    return lax.dot_general(a, b, (((1,), (1,)), ((), ())), preferred_element_type=F32)


def nn(a, b):
    return lax.dot_general(a, b, (((1,), (0,)), ((), ())), preferred_element_type=F32)


def kernel(
    mix_t,
    lse_t,
    scale,
    target,
    hidden_hbm,
    proj_hbm,
    w_hbm,
    gh_out,
    gm_out,
    gp_out,
    go_out,
    hidden,
    proj,
    w,
    comp,
    comp_t,
    gl,
    part,
    r1x,
    rfx,
    gcb,
    rd,
    r1a,
    rfa,
    r1b,
    rfb,
    wt,
    hs,
    hst,
    gpx,
    gpall,
    prods,
    prodr,
    gms,
    gmr,
    hts,
    hrecv,
    info2,
    lsec,
    coefc,
    tgtc,
    tl,
    pbuf,
    gh_v,
    gm_v,
    gp_v,
    sem_w,
    sem_i,
    p_s,
    p_r,
    sem_o,
    ag_s,
    ag_r,
    hs_s,
    hs_r,
    tl_s,
    tl_r,
    x_s,
    x_r,
    zx_s,
    zx_r,
    zx_l,
    d_s,
    d_r,
    a_s,
    a_r,
    b_s,
    b_r,
    h_s,
    h_r,
    g_s,
    g_r,
):
    x = lax.axis_index("x")
    zl = lax.axis_index("zl")
    zh = lax.axis_index("zh")
    y = lax.axis_index("y")
    c = lax.axis_index("c")
    z = zh * 2 + zl
    v = zh * 8 + y * 2 + c
    d = x * 2 + zl

    def m4(i):
        return lax.rem(i + 4, 4)

    def dev(x_=None, z_=None, y_=None, c_=None):
        zz = z if z_ is None else z_
        return (
            x if x_ is None else x_,
            lax.rem(zz, 2),
            lax.div(zz, 2),
            y if y_ is None else y_,
            c if c_ is None else c_,
        )

    def rc(src, dst, ss, rs, to):
        return pltpu.make_async_remote_copy(
            src_ref=src, dst_ref=dst, send_sem=ss, recv_sem=rs, device_id=to, device_id_type=MESH_ID
        )

    partner_c = dev(c_=1 - c)
    partner_z = (x, 1 - zl, zh, y, c)

    q32 = z * 8 + y * 2 + c

    def mate(o):
        p = lax.rem(q32 + o, 32)
        zz = lax.div(p, 8)
        return (x, lax.rem(zz, 2), lax.div(zz, 2), lax.rem(lax.div(p, 2), 4), lax.rem(p, 2))

    barrier = pltpu.get_barrier_semaphore()

    def greet(o, carry):
        pl.semaphore_signal(barrier, inc=1, device_id=mate(o), device_id_type=MESH_ID)
        return carry

    lax.fori_loop(1, 32, greet, 0)
    for o in range(1, 4):
        pl.semaphore_signal(barrier, inc=1, device_id=dev(x_=m4(x + o)), device_id_type=MESH_ID)

    hidden_copy = pltpu.make_async_copy(hidden_hbm, hidden, sem_w.at[0])
    proj_copy = pltpu.make_async_copy(proj_hbm, proj, sem_w.at[1])
    w_copy = pltpu.make_async_copy(
        w_hbm.at[:, pl.ds(pl.multiple_of(zl * VH, VH), VH)], w, sem_w.at[2]
    )
    hidden_copy.start()
    proj_copy.start()
    w_copy.start()
    hidden_copy.wait()
    mix_logits = nt(mix_t[...], hidden[...])
    info2[zl, 0:4] = lse_t[...]
    info2[zl, 4:8] = mix_logits - jnp.log(jnp.sum(jnp.exp(mix_logits), axis=0, keepdims=True))
    info2[zl, 8:9] = scale[...]
    info2[zl, 9:10] = target[...].astype(F32)
    info2[zl, 10:16] = jnp.zeros((6, T), F32)

    def row_columns(g):
        cols = jnp.transpose(jnp.concatenate([info2[g], jnp.zeros((112, T), F32)], axis=0))
        local = cols[:, 9:10] - (v * VL + zl * VH).astype(F32)
        for k in range(K):
            rows = pl.ds(pl.multiple_of(g * R + k * T, T), T)
            lsec[rows, :] = jnp.broadcast_to(cols[:, k : k + 1], (T, 128))
            tgtc[rows, :] = jnp.broadcast_to(local, (T, 128))

    row_columns(zl)
    info_copy = rc(info2.at[zl], info2.at[zl], sem_i.at[0], sem_i.at[1], partner_z)

    own_rows = pl.multiple_of(zl * R, R)
    own_cols = pl.multiple_of(v * U, U)

    def blk(col, z_, y_, c_, r0=0, n=2 * T):
        row = lax.rem(z_, 2) * R + col * 2 * T + r0
        lane = (lax.div(z_, 2) * 8 + y_ * 2 + c_) * U
        return comp.at[pl.ds(pl.multiple_of(row, T), n), pl.ds(pl.multiple_of(lane, U), U)]

    def pos(col):
        return (y, z) if col == 0 else (z, y)

    def at_ab(col, a_, b_, c_, r0=0, n=2 * T):
        return blk(col, b_, a_, c_, r0, n) if col == 0 else blk(col, a_, b_, c_, r0, n)

    def dev_ab(col, a_, b_):
        return dev(y_=a_, z_=b_) if col == 0 else dev(z_=a_, y_=b_)

    def ag_copy(col, i, ref, to):
        r = 30 + i if col is None else col * 15 + i
        return rc(ref, ref, ag_s, ag_r.at[r], to)

    def ag_send(col, i, ref, to):
        ag_copy(col, i, ref, to).start()

    def ag_wait(col, i, ref):
        ag_copy(col, i, ref, partner_c).wait_recv()

    def second(col, i, ref):
        a, b = pos(col)
        ag_send(col, 3 + 3 * i, ref, dev_ab(col, a, m4(b + 1)))
        ag_send(col, 3 + 3 * i + 1, ref, dev_ab(col, a, m4(b - 1)))

    def across(i, ref):
        ag_send(None, i, ref, partner_c)

    def flip(col, a_, b_, c_):
        z_, y_ = (b_, a_) if col == 0 else (a_, b_)
        row = pl.multiple_of(lax.rem(z_, 2) * R + col * 2 * T, 2 * T)
        lane = pl.multiple_of((lax.div(z_, 2) * 8 + y_ * 2 + c_) * U, U)
        comp_t[pl.ds(lane, U), pl.ds(row, 2 * T)] = jnp.transpose(
            comp[pl.ds(row, 2 * T), pl.ds(lane, U)]
        )

    proj_copy.wait()
    for k in range(K):
        pre = nn(hidden[...], proj[k])
        comp[pl.ds(pl.multiple_of(own_rows + k * T, T), T), pl.ds(own_cols, U)] = jnp.tanh(
            pre
        ).astype(BF16)
    pl.semaphore_wait(barrier, 34)
    for col in range(2):
        a, b = pos(col)
        own = at_ab(col, a, b, c)
        ag_send(col, 0, own, dev_ab(col, m4(a + 1), b))
        ag_send(col, 1, own, dev_ab(col, m4(a - 1), b))
    info_copy.start()
    for col in range(2):
        a, b = pos(col)
        own = at_ab(col, a, b, c)
        second(col, 0, own)
        across(0, own)

    def hs_copy(i):
        p = m4(x + (0, 1, -1, 2)[i])
        return rc(
            hidden.at[:, pl.ds(pl.multiple_of(p * 512, 512), 512)], hs.at[i], hs_s, hs_r, dev(x_=p)
        )

    for i in range(1, 4):
        hs_copy(i).start()
    hs[0] = hidden[:, pl.ds(pl.multiple_of(x * 512, 512), 512)]

    def pick(n, carry):
        rows = pl.ds(pl.multiple_of(n * 512, 512), 512)
        acc = jnp.zeros((2 * T, 512), F32)
        for q in range(4):
            lane = lax.broadcasted_iota(jnp.int32, (T, 512), 1).astype(F32) + float(q * 512)
            hot = jnp.concatenate(
                [
                    (lane == tgtc[pl.ds(g * R, T), :][:, 0:1]).astype(F32).astype(BF16)
                    for g in range(2)
                ],
                axis=0,
            )
            acc = acc + nt(hot, w[rows, pl.ds(q * 512, 512)])
        wt[:, rows] = acc.astype(BF16)
        return carry

    for col in range(2):
        a, b = pos(col)
        prev, nxt = m4(a - 1), m4(a + 1)
        ag_wait(col, 0, at_ab(col, prev, b, c))
        ag_send(col, 2, at_ab(col, prev, b, c, 0, T), dev_ab(col, nxt, b))
        second(col, 1, at_ab(col, prev, b, c))
        across(1, at_ab(col, prev, b, c))
        ag_wait(col, 1, at_ab(col, nxt, b, c))
        ag_send(col, 2, at_ab(col, nxt, b, c, T, T), dev_ab(col, prev, b))
        second(col, 2, at_ab(col, nxt, b, c))
        across(2, at_ab(col, nxt, b, c))
    info_in = rc(info2.at[1 - zl], info2.at[1 - zl], sem_i.at[0], sem_i.at[1], partner_z)
    info_in.wait_recv()
    row_columns(1 - zl)
    for col in range(2):
        a, b = pos(col)
        far = m4(a + 2)
        ag_wait(col, 2, at_ab(col, far, b, c))
        second(col, 3, at_ab(col, far, b, c))
        across(3, at_ab(col, far, b, c))
    w_copy.wait()
    lax.fori_loop(0, 4, pick, 0)
    for i in range(4):
        for col in range(2):
            a, b = pos(col)
            a_ = m4(a + (0, -1, 1, 2)[i])
            prev, nxt = m4(b - 1), m4(b + 1)
            ag_wait(col, 3 + 3 * i, at_ab(col, a_, prev, c))
            ag_send(col, 3 + 3 * i + 2, at_ab(col, a_, prev, c, 0, T), dev_ab(col, a, nxt))
            across(i, at_ab(col, a_, prev, c))
            ag_wait(col, 3 + 3 * i + 1, at_ab(col, a_, nxt, c))
            ag_send(col, 3 + 3 * i + 2, at_ab(col, a_, nxt, c, T, T), dev_ab(col, a, prev))
            across(i, at_ab(col, a_, nxt, c))
            for b_ in (b, prev, nxt):
                flip(col, a_, b_, c)
    for i in range(4):
        for col in range(2):
            a, b = pos(col)
            a_ = m4(a + (0, -1, 1, 2)[i])
            far = m4(b + 2)
            ag_wait(col, 3 + 3 * i + 2, at_ab(col, a_, far, c))
            across(i, at_ab(col, a_, far, c))
            flip(col, a_, far, c)
    for i in range(4):
        ag_wait(None, i, comp.at[pl.ds(0, T), :])
        for col in range(2):
            a, b = pos(col)
            a_ = m4(a + (0, -1, 1, 2)[i])

            def flip_step(b_, carry):
                flip(col, a_, b_, 1 - c)
                return carry

            lax.fori_loop(0, 4, flip_step, 0)

    lane_t = lax.broadcasted_iota(jnp.int32, (T, 128), 1)
    acc = jnp.zeros((T, 128), F32)
    for g in range(2):
        for k in range(K):
            s = jnp.zeros((T, 128), F32)
            for q in range(4):
                prod = comp[pl.ds(g * R + k * T, T), pl.ds(q * 512, 512)].astype(F32) * wt[
                    pl.ds(g * T, T), pl.ds(q * 512, 512)
                ].astype(F32)
                for e in range(4):
                    s = s + prod[:, e * 128 : (e + 1) * 128]
            acc = jnp.where(lane_t == g * K + k, jnp.sum(s, axis=1, keepdims=True), acc)
    tl[0] = jnp.transpose(acc)[0:8]

    def tl_copy(o):
        return rc(tl.at[0], tl.at[o], tl_s, tl_r, mate(o))

    def tl_start(o, carry):
        tl_copy(o).start()
        return carry

    lax.fori_loop(1, 32, tl_start, 0)

    lane_w = lax.broadcasted_iota(jnp.int32, (2 * T, 128), 1).astype(F32)

    def block_logits(p, m, put):
        rows = pl.ds(pl.multiple_of(m * 2 * T, 2 * T), 2 * T)
        logit = nn(comp[rows, :], w[:, pl.ds(pl.multiple_of(p * W2, W2), W2)])
        shift = jnp.asarray(p * W2, F32)
        lse_m, tgt_m = lsec[rows, :], tgtc[rows, :] - shift
        for e in range(W2 // 128):
            prob = jnp.exp(logit[:, e * 128 : (e + 1) * 128] - lse_m)
            hot = jnp.where(lane_w + float(e * 128) == tgt_m, 1.0, 0.0)
            put(rows, e, prob - hot)

    def hold(m, carry):
        def put(rows, e, val):
            pbuf[rows, pl.ds(e * 128, 128)] = val

        block_logits(0, m, put)
        return carry

    lax.fori_loop(0, 4, hold, 0)

    tl_all = rc(tl.at[pl.ds(1, 31)], tl.at[pl.ds(1, 31)], tl_s, tl_r, partner_c)
    tl_all.wait_recv()
    target_logit = jnp.sum(tl[...], axis=0)
    coef_rows = []
    gml_rows = []
    for g in range(2):
        lse_g = info2[g, 0:4]
        lm_g = info2[g, 4:8]
        scale_g = info2[g, 8:9]
        weights = jnp.exp(lm_g + target_logit[g * K : (g + 1) * K] - lse_g)
        resp = weights / jnp.sum(weights, axis=0, keepdims=True)
        coef_rows.append(scale_g * resp)
        gml_rows.append(-scale_g * (resp - jnp.exp(lm_g)))
    table = jnp.concatenate(coef_rows + gml_rows + [jnp.zeros((112, 128), F32)], axis=0)
    cols = jnp.transpose(table)
    for g in range(2):
        for k in range(K):
            coefc[pl.ds(g * R + k * T, T), :] = jnp.broadcast_to(
                cols[:, g * K + k : g * K + k + 1], (T, 128)
            )
    gml = jnp.zeros((T, 128), F32)
    for k in range(K):
        mine = jnp.where(zl == 0, cols[:, 8 + k : 9 + k], cols[:, 12 + k : 13 + k])
        high = mine.astype(BF16).astype(F32)
        gml = jnp.where(lane_t == k, high, gml)
        gml = jnp.where(lane_t == K + k, mine - high, gml)
    gpx[4] = gml.astype(BF16)

    def ring(piece, me, right, left, r1, rf, ss, r1_sem, rf_sem, r1_all, rf_all):
        two, one, back = m4(me + 2), m4(me + 1), m4(me - 1)
        copies = (
            lambda: rc(piece(two, 0), r1(0), ss, r1_sem, right),
            lambda: rc(piece(one, 1), rf(0, 1), ss, rf_sem, right),
            lambda: rc(piece(two, 1), r1(1), ss, r1_sem, left),
            lambda: rc(piece(back, 0), rf(1, 0), ss, rf_sem, left),
            lambda: rc(piece(one, 0), rf(0, 0), ss, rf_sem, right),
            lambda: rc(piece(back, 1), rf(1, 1), ss, rf_sem, left),
        )

        def first(which=(0, 2, 1, 3)):
            for i in which:
                copies[i]().start()

        def add(ref, other):
            ref[...] = (ref[...].astype(F32) + other[...].astype(F32)).astype(BF16)

        def forward():
            rc(r1_all, r1_all, ss, r1_sem, right).wait_recv()
            add(piece(one, 0), r1(0))
            copies[4]().start()
            add(piece(back, 1), r1(1))
            copies[5]().start()

        def arrive():
            rc(rf_all, rf_all, ss, rf_sem, right).wait_recv()

        return first, forward, arrive

    x_right, x_left = dev(x_=m4(x + 1)), dev(x_=m4(x - 1))

    def x_ring(cc):
        return ring(
            lambda t, h: part.at[cc, t * 2 + h],
            x,
            x_right,
            x_left,
            lambda i: r1x.at[cc, i],
            lambda i, h: rfx.at[cc, i, h],
            x_s,
            x_r.at[2 * cc],
            x_r.at[2 * cc + 1],
            r1x.at[cc],
            rfx.at[cc],
        )

    def grad_out(p):
        cols = pl.ds(p * W2, W2)
        order = ((2, 0), (2, 1), (1, 1), (-1, 0), (1, 0), (-1, 1), (0, 0), (0, 1))
        for i, (step, h) in enumerate(order):
            t = m4(x + step)
            rows = pl.ds(pl.multiple_of(t * 512 + h * 256, 256), 256)
            res = nn(comp_t[rows, :], gl[:, cols]).astype(BF16)
            for e in range(2):
                part[2 * p + e, t * 2 + h] = res[:, e * C : (e + 1) * C]
            if i < 4:
                for e in range(2):
                    x_ring(2 * p + e)[0](((0, 2, 1, 3)[i],))

    def scale_first(m, carry):
        rows = pl.ds(pl.multiple_of(m * 2 * T, 2 * T), 2 * T)
        coef_m = coefc[rows, :]
        for e in range(W2 // 128):
            gl[rows, pl.ds(e * 128, 128)] = (coef_m * pbuf[rows, pl.ds(e * 128, 128)]).astype(BF16)
        return carry

    lax.fori_loop(0, 4, scale_first, 0)

    def grad_logits(p):
        def rows_of(m, carry):
            coef_m = coefc[pl.ds(pl.multiple_of(m * 2 * T, 2 * T), 2 * T), :]

            def put(rows, e, val):
                gl[rows, pl.ds(pl.multiple_of(p * W2 + e * 128, 128), 128)] = (coef_m * val).astype(
                    BF16
                )

            block_logits(p, m, put)
            return carry

        lax.fori_loop(0, 4, rows_of, 0)

    def comp_grad(col):
        def tile(i, carry):
            g, h, j = lax.div(i, 4), lax.rem(lax.div(i, 2), 2), lax.rem(i, 2)
            rows = pl.ds(pl.multiple_of(g * R + col * 2 * T, 2 * T), 2 * T)
            units = pl.ds(pl.multiple_of((h * 2 + j) * 512, 512), 512)
            res = nt(gl[rows, :], w[units, :])
            z_ = h * 2 + g
            for jj in range(4):
                y_ = j * 2 + jj // 2
                val = res[:, jj * 128 : (jj + 1) * 128].astype(BF16)
                if col == 0:
                    gcb[jj % 2, col, z_, y_] = val
                else:
                    gcb[jj % 2, col, y_, z_] = val
            return carry

        lax.fori_loop(0, 8, tile, 0)
        swap = rc(gcb.at[1 - c, col], rd.at[col], d_s.at[col], d_r.at[col], partner_c)
        swap.start()
        return swap

    def a_ring(col):
        me = z if col == 0 else y
        mk = (lambda p: dev(z_=p)) if col == 0 else (lambda p: dev(y_=p))
        return ring(
            lambda t, h: gcb.at[c, col, t, pl.ds(2 * h, 2)],
            me,
            mk(m4(me + 1)),
            mk(m4(me - 1)),
            lambda i: r1a.at[col, i],
            lambda i, h: rfa.at[col, i, h],
            a_s,
            a_r.at[2 * col],
            a_r.at[2 * col + 1],
            r1a.at[col],
            rfa.at[col],
        )

    def b_ring(col):
        first = z if col == 0 else y
        me = y if col == 0 else z
        mk = (lambda p: dev(y_=p)) if col == 0 else (lambda p: dev(z_=p))
        return ring(
            lambda t, h: gcb.at[c, col, first, t, pl.ds(h * T, T)],
            me,
            mk(m4(me + 1)),
            mk(m4(me - 1)),
            lambda i: r1b.at[col, i],
            lambda i, h: rfb.at[col, i, h],
            b_s,
            b_r.at[2 * col],
            b_r.at[2 * col + 1],
            r1b.at[col],
            rfb.at[col],
        )

    def merge(col, swap):
        swap.wait_recv()

        def add(i, carry):
            p, q = lax.div(i, 4), lax.rem(i, 4)
            gcb[c, col, p, q] = (gcb[c, col, p, q].astype(F32) + rd[col, p, q].astype(F32)).astype(
                BF16
            )
            return carry

        lax.fori_loop(0, 16, add, 0)

    def finish_a(col):
        me = z if col == 0 else y
        for h in range(2):
            for e in range(2):
                q = 2 * h + e
                gcb[c, col, me, q] = (
                    gcb[c, col, me, q].astype(F32)
                    + rfa[col, 0, h, e].astype(F32)
                    + rfa[col, 1, h, e].astype(F32)
                ).astype(BF16)

    def x_finish(cc):
        x_ring(cc)[2]()
        for h in range(2):
            part[cc, x * 2 + h] = (
                part[cc, x * 2 + h].astype(F32)
                + rfx[cc, 0, h].astype(F32)
                + rfx[cc, 1, h].astype(F32)
            ).astype(BF16)
        for cp in z_copies(cc):
            cp.start()

    def z_copies(cc):
        cols = pl.ds(pl.multiple_of(zl * VH + cc * C, C), C)
        dst = go_out.at[:, cols]
        return (
            rc(part.at[cc, x * 2 + 1 - zl], dst, zx_s, zx_r, partner_z),
            pltpu.make_async_copy(part.at[cc, x * 2 + zl], dst, zx_l),
        )

    def finish_b(col):
        first = z if col == 0 else y
        me = y if col == 0 else z
        b_ring(col)[2]()
        for h in range(2):
            total = (
                gcb[c, col, first, me, pl.ds(h * T, T)].astype(F32)
                + rfb[col, 0, h].astype(F32)
                + rfb[col, 1, h].astype(F32)
            )
            k = 2 * col + h
            cf = comp[
                pl.ds(pl.multiple_of(own_rows + k * T, T), T), pl.ds(own_cols, U)
            ].astype(F32)
            gpx[k] = (total * (1.0 - cf * cf)).astype(BF16)

    grad_out(0)
    grad_logits(1)
    grad_out(1)
    x_ring(0)[1]()
    grad_logits(2)
    grad_logits(3)
    x_ring(1)[1]()
    swap0 = comp_grad(0)
    grad_out(2)
    merge(0, swap0)
    a_ring(0)[0]()
    x_ring(2)[1]()
    swap1 = comp_grad(1)
    a_ring(0)[1]()
    x_ring(3)[1]()
    grad_out(3)
    merge(1, swap1)
    a_ring(1)[0]()
    x_finish(0)
    a_ring(0)[2]()
    finish_a(0)
    b_ring(0)[0]()
    a_ring(1)[1]()
    hs_all = rc(hs.at[pl.ds(1, 3)], hs.at[pl.ds(1, 3)], hs_s, hs_r, partner_c)
    hs_all.wait_recv()
    for i in range(4):
        hst[:, pl.ds(i * T, T)] = jnp.transpose(hs[i])
    b_ring(0)[1]()
    x_finish(1)
    a_ring(1)[2]()
    finish_a(1)
    b_ring(1)[0]()
    finish_b(0)
    b_ring(1)[1]()
    finish_b(1)

    def slot(i, r0=0, n=T):
        return gpall.at[:, pl.ds(i * T + r0, n)]

    g_copies = (
        rc(gpx, slot(1), g_s, g_r.at[0], x_right),
        rc(gpx, slot(2), g_s, g_r.at[1], x_left),
        rc(slot(1, 0, T // 2), slot(3, 0, T // 2), g_s, g_r.at[2], x_right),
        rc(slot(2, T // 2, T // 2), slot(3, T // 2, T // 2), g_s, g_r.at[2], x_left),
    )
    g_copies[0].start()
    g_copies[1].start()
    x_ring(4)[1]()

    def h_copy(o):
        p = lax.rem(v + o, 16)
        to = (x, zl, lax.div(p, 8), lax.rem(lax.div(p, 2), 4), lax.rem(p, 2))
        return rc(hts.at[o], hrecv.at[o], h_s, h_r, to)

    def h_tile(o):
        p = lax.rem(v + o, 16)
        rows = pl.ds(pl.multiple_of(p * U, U), U)
        acc = nt(gpx[0], proj[0, rows, :])
        for k in range(1, K):
            acc = acc + nt(gpx[k], proj[k, rows, :])
        return acc

    def h_step(o, carry):
        hts[o] = h_tile(o).astype(BF16)
        h_copy(o).start()
        return carry

    lax.fori_loop(1, 16, h_step, 0)
    hrecv[0] = h_tile(0).astype(BF16)
    gpall[:, pl.ds(0, T)] = gpx[...]
    x_ring(5)[1]()
    x_finish(2)
    x_finish(3)
    h_all = rc(hts.at[pl.ds(1, 15)], hrecv.at[pl.ds(1, 15)], h_s, h_r, partner_c)
    h_all.wait_recv()
    mw = jnp.concatenate(
        [mix_t[:, pl.ds(own_cols, U)].astype(F32)] * 2 + [jnp.zeros((120, U), F32)], axis=0
    ).astype(BF16)
    gh = nn(gpx[4], mw)
    for o in range(16):
        gh = gh + hrecv[o].astype(F32)
    gh_v[...] = gh.astype(BF16)
    out_copies = (
        pltpu.make_async_copy(gh_v, gh_out, sem_o.at[0]),
        pltpu.make_async_copy(gp_v, gp_out, sem_o.at[1]),
        pltpu.make_async_copy(gm_v, gm_out, sem_o.at[2]),
    )
    out_copies[0].start()
    x_ring(6)[1]()
    g_copies[0].wait_recv()
    g_copies[2].start()
    g_copies[1].wait_recv()
    g_copies[3].start()
    x_ring(7)[1]()
    x_finish(4)
    x_finish(5)

    rc(slot(3), slot(3), g_s, g_r.at[2], x_right).wait_recv()

    def product(half, k):
        return nn(hst[pl.ds(pl.multiple_of(half * 256, 256), 256), :], gpall[k])

    def mix_product(half):
        res = lax.dot_general(
            gpall[4],
            hst[pl.ds(pl.multiple_of(half * 256, 256), 256), :],
            (((0,), (1,)), ((), ())),
            preferred_element_type=F32,
        )
        return res[0:4] + res[4:8]

    for k in range(K):
        prods[k] = product(1 - zl, k).astype(BF16)
    gms[...] = mix_product(1 - zl)
    p_copies = (
        rc(prods, prodr, p_s.at[0], p_r.at[0], partner_z),
        rc(gms, gmr, p_s.at[1], p_r.at[1], partner_z),
    )
    for cp in p_copies:
        cp.start()
    x_finish(6)
    x_finish(7)
    for cp in p_copies:
        cp.wait_recv()
    for k in range(K):
        gp_v[k] = (product(zl, k) + prodr[k].astype(F32)).astype(BF16)
    gm_v[...] = mix_product(zl) + gmr[...]
    out_copies[1].start()
    out_copies[2].start()

    for cp in (info_copy, swap0, swap1, *p_copies, tl_all, hs_all, h_all):
        cp.wait_send()
    for ref, sem in (
        (comp.at[pl.ds(0, 992), :], ag_s),
        (part.at[pl.ds(0, 6)], x_s),
        (part.at[0], zx_s),
        (gcb.at[0, :, pl.ds(0, 3)], a_s),
        (gcb.at[0, 0, pl.ds(0, 3), pl.ds(0, 2)], b_s),
        (gpall.at[:, pl.ds(0, 3 * T)], g_s),
    ):
        rc(ref, ref, sem, zx_r, partner_z).wait_send()
    half_out = go_out.at[:, pl.ds(0, VH)]
    rc(half_out, half_out, zx_s, zx_r, partner_z).wait_recv()
    pltpu.make_async_copy(part.at[0], part.at[0], zx_l).wait()
    for cp in out_copies:
        cp.wait()


def place(gh, gm, gp, go, gh_o, gm_o, gp_o, go_o, b_gh, b_gm, b_gp, b_go, s_in, s_out):
    pairs = [(gh, b_gh, gh_o), (gm, b_gm, gm_o), (gp, b_gp, gp_o)]
    for i in range(4):
        rows = pl.ds(i * 64, 64)
        pairs.append((go.at[rows], b_go.at[rows], go_o.at[rows]))
    loads = [pltpu.make_async_copy(s, b, s_in.at[i]) for i, (s, b, _) in enumerate(pairs)]
    stores = [pltpu.make_async_copy(b, t, s_out.at[i]) for i, (_, b, t) in enumerate(pairs)]
    for cp in reversed(loads):
        cp.start()
    for i in reversed(range(len(pairs))):
        loads[i].wait()
        stores[i].start()
    for cp in stores:
        cp.wait()


def shards(hidden, mix_weight, proj_weight, out_weight, saved_lse, targets, loss_scale):
    vm = pl.BlockSpec(memory_space=pltpu.VMEM)
    hbm = pl.BlockSpec(memory_space=pltpu.HBM)
    dma = pltpu.SemaphoreType.DMA
    outs = (
        jax.ShapeDtypeStruct((T, U), BF16),
        jax.ShapeDtypeStruct((K, 256), F32),
        jax.ShapeDtypeStruct((K, 256, U), BF16),
        jax.ShapeDtypeStruct((256, VL), BF16),
    )
    found = pl.pallas_call(
        kernel,
        out_shape=outs,
        in_specs=[vm, vm, vm, vm, hbm, hbm, hbm],
        out_specs=(hbm, hbm, hbm, hbm),
        scratch_shapes=[
            pltpu.VMEM((T, D), BF16),
            pltpu.VMEM((K, D, U), BF16),
            pltpu.VMEM((D, VH), BF16),
            pltpu.VMEM((2 * R, D), BF16),
            pltpu.VMEM((D, 2 * R), BF16),
            pltpu.VMEM((2 * R, VH), BF16),
            pltpu.VMEM((NC, 8, 256, C), BF16),
            pltpu.VMEM((NC, 2, 256, C), BF16),
            pltpu.VMEM((NC, 2, 2, 256, C), BF16),
            pltpu.VMEM((2, 2, 4, 4, 2 * T, U), BF16),
            pltpu.VMEM((2, 4, 4, 2 * T, U), BF16),
            pltpu.VMEM((2, 2, 2, 2 * T, U), BF16),
            pltpu.VMEM((2, 2, 2, 2, 2 * T, U), BF16),
            pltpu.VMEM((2, 2, T, U), BF16),
            pltpu.VMEM((2, 2, 2, T, U), BF16),
            pltpu.VMEM((2 * T, D), BF16),
            pltpu.VMEM((4, T, 512), BF16),
            pltpu.VMEM((512, 4 * T), BF16),
            pltpu.VMEM((5, T, U), BF16),
            pltpu.VMEM((5, 4 * T, U), BF16),
            pltpu.VMEM((K, 256, U), BF16),
            pltpu.VMEM((K, 256, U), BF16),
            pltpu.VMEM((K, 256), F32),
            pltpu.VMEM((K, 256), F32),
            pltpu.VMEM((16, T, U), BF16),
            pltpu.VMEM((16, T, U), BF16),
            pltpu.VMEM((2, 16, T), F32),
            pltpu.VMEM((2 * R, 128), F32),
            pltpu.VMEM((2 * R, 128), F32),
            pltpu.VMEM((2 * R, 128), F32),
            pltpu.VMEM((32, 8, T), F32),
            pltpu.VMEM((2 * R, W2), F32),
            pltpu.VMEM((T, U), BF16),
            pltpu.VMEM((K, 256), F32),
            pltpu.VMEM((K, 256, U), BF16),
            dma((3,)),
            dma((2,)),
            dma((2,)),
            dma((2,)),
            dma((3,)),
            dma,
            dma((34,)),
            dma,
            dma,
            dma,
            dma,
            dma,
            dma((16,)),
            dma,
            dma,
            dma,
            dma((2,)),
            dma((2,)),
            dma,
            dma((4,)),
            dma,
            dma((4,)),
            dma,
            dma,
            dma,
            dma((3,)),
        ],
        compiler_params=pltpu.CompilerParams(
            collective_id=0, has_side_effects=True, vmem_limit_bytes=67043328
        ),
    )(
        mix_weight.T,
        saved_lse.T,
        loss_scale[None, :],
        targets[None, :],
        hidden,
        proj_weight,
        out_weight,
    )
    gh, gm, gp, go = pl.pallas_call(
        place,
        out_shape=outs,
        in_specs=[hbm] * 4,
        out_specs=(hbm,) * 4,
        scratch_shapes=[pltpu.VMEM(o.shape, o.dtype) for o in outs] + [dma((7,)), dma((7,))],
    )(*found)
    return gh, gm.T, gp, go


def solution(mesh):
    finer = Mesh(mesh.devices.reshape(4, 2, 2, 4, 2), AXES)
    in_specs = (
        P(DP, None),
        P(),
        P(None, None, VOC),
        P(None, VOC),
        P(DP, None),
        P(DP),
        P(DP),
    )
    out_specs = (P(DP, VOC), P(DP, None), P(None, DP, VOC), P(DP, VOC))
    return jax.shard_map(
        shards, mesh=finer, in_specs=in_specs, out_specs=out_specs, check_vma=False
    )
```

```python
import functools

import jax
import jax.numpy as jnp
from jax import lax
from jax.experimental import pallas as pl
from jax.experimental.pallas import tpu as pltpu
from jax.sharding import Mesh
from jax.sharding import PartitionSpec as P

AXES = ("x", "zl", "zh", "y", "c")
DP = ("x", "zl")
VOC = ("zh", "y", "c")
MESH_ID = pl.DeviceIdType.MESH
F32 = jnp.float32
BF16 = jnp.bfloat16

T = 128
K = 4
R = T * K
U = 128
D = 2048
VL = 4096
VH = VL // 2
NC = 8
C = VH // NC
W2 = 2 * C


def nt(a, b):
    return lax.dot_general(a, b, (((1,), (1,)), ((), ())), preferred_element_type=F32)


def nn(a, b):
    return lax.dot_general(a, b, (((1,), (0,)), ((), ())), preferred_element_type=F32)


def kernel(
    mix_t,
    lse_t,
    scale,
    target,
    hidden_hbm,
    proj_hbm,
    w_hbm,
    gh_out,
    gm_out,
    gp_out,
    go_out,
    hidden,
    proj,
    w,
    comp,
    comp_t,
    gl,
    part,
    r1x,
    rfx,
    gcb,
    rd,
    r1a,
    rfa,
    rfb,
    wt,
    hs,
    hst,
    gpx,
    gpall,
    gmla,
    prods,
    prodr,
    gms,
    gmr,
    hts,
    hrecv,
    info2,
    lsec,
    coefc,
    tgtc,
    tl,
    pbuf,
    gh_v,
    gm_v,
    gp_v,
    sem_w,
    sem_i,
    p_s,
    p_r,
    sem_o,
    ag_s,
    ag_r,
    hs_s,
    hs_r,
    tl_s,
    tl_r,
    x_s,
    x_r,
    zx_s,
    zx_r,
    zx_l,
    d_s,
    d_r,
    a_s,
    a_r,
    b_s,
    b_r,
    h_s,
    h_r,
    g_s,
    g_r,
    gm_s,
    gm_r,
):
    x = lax.axis_index("x")
    zl = lax.axis_index("zl")
    zh = lax.axis_index("zh")
    y = lax.axis_index("y")
    c = lax.axis_index("c")
    z = zh * 2 + zl
    v = zh * 8 + y * 2 + c
    d = x * 2 + zl

    def m4(i):
        return lax.rem(i + 4, 4)

    def dev(x_=None, z_=None, y_=None, c_=None):
        zz = z if z_ is None else z_
        return (
            x if x_ is None else x_,
            lax.rem(zz, 2),
            lax.div(zz, 2),
            y if y_ is None else y_,
            c if c_ is None else c_,
        )

    def rc(src, dst, ss, rs, to):
        return pltpu.make_async_remote_copy(
            src_ref=src, dst_ref=dst, send_sem=ss, recv_sem=rs, device_id=to, device_id_type=MESH_ID
        )

    partner_c = dev(c_=1 - c)
    partner_z = (x, 1 - zl, zh, y, c)

    hidden_copy = pltpu.make_async_copy(hidden_hbm, hidden, sem_w.at[0])
    proj_copy = pltpu.make_async_copy(proj_hbm, proj, sem_w.at[1])
    w_copy = pltpu.make_async_copy(
        w_hbm.at[:, pl.ds(pl.multiple_of(zl * VH, VH), VH)], w, sem_w.at[2]
    )
    hidden_copy.start()
    proj_copy.start()
    w_copy.start()

    q32 = z * 8 + y * 2 + c

    def mate(o):
        p = lax.rem(q32 + o, 32)
        zz = lax.div(p, 8)
        return (x, lax.rem(zz, 2), lax.div(zz, 2), lax.rem(lax.div(p, 2), 4), lax.rem(p, 2))

    barrier = pltpu.get_barrier_semaphore()

    def greet(o, carry):
        pl.semaphore_signal(barrier, inc=1, device_id=mate(o), device_id_type=MESH_ID)
        return carry

    lax.fori_loop(1, 32, greet, 0)
    for o in range(1, 4):
        pl.semaphore_signal(barrier, inc=1, device_id=dev(x_=m4(x + o)), device_id_type=MESH_ID)

    own_rows = pl.multiple_of(zl * R, R)
    own_cols = pl.multiple_of(v * U, U)

    def blk(col, z_, y_, c_, r0=0, n=2 * T):
        row = lax.rem(z_, 2) * R + col * 2 * T + r0
        lane = (lax.div(z_, 2) * 8 + y_ * 2 + c_) * U
        return comp.at[pl.ds(pl.multiple_of(row, T), n), pl.ds(pl.multiple_of(lane, U), U)]

    def pos(col):
        return (y, z) if col == 0 else (z, y)

    def at_ab(col, a_, b_, c_, r0=0, n=2 * T):
        return blk(col, b_, a_, c_, r0, n) if col == 0 else blk(col, a_, b_, c_, r0, n)

    def dev_ab(col, a_, b_):
        return dev(y_=a_, z_=b_) if col == 0 else dev(z_=a_, y_=b_)

    def ag_copy(col, i, ref, to):
        r = 30 + i if col is None else col * 15 + i
        return rc(ref, ref, ag_s, ag_r.at[r], to)

    def ag_send(col, i, ref, to):
        ag_copy(col, i, ref, to).start()

    def ag_wait(col, i, ref):
        ag_copy(col, i, ref, partner_c).wait_recv()

    def second(col, i, ref):
        a, b = pos(col)
        ag_send(col, 3 + 3 * i, ref, dev_ab(col, a, m4(b + 1)))
        ag_send(col, 3 + 3 * i + 1, ref, dev_ab(col, a, m4(b - 1)))

    def across(i, ref):
        ag_send(None, i, ref, partner_c)

    def flip(col, a_, b_, c_):
        z_, y_ = (b_, a_) if col == 0 else (a_, b_)
        row = pl.multiple_of(lax.rem(z_, 2) * R + col * 2 * T, 2 * T)
        lane = pl.multiple_of((lax.div(z_, 2) * 8 + y_ * 2 + c_) * U, U)
        comp_t[pl.ds(lane, U), pl.ds(row, 2 * T)] = jnp.transpose(
            comp[pl.ds(row, 2 * T), pl.ds(lane, U)]
        )

    hidden_copy.wait()
    proj_copy.wait()
    for k in range(K):
        pre = nn(hidden[...], proj[k])
        comp[pl.ds(pl.multiple_of(own_rows + k * T, T), T), pl.ds(own_cols, U)] = jnp.tanh(
            pre
        ).astype(BF16)
    pl.semaphore_wait(barrier, 34)
    for col in range(2):
        a, b = pos(col)
        own = at_ab(col, a, b, c)
        ag_send(col, 0, own, dev_ab(col, m4(a + 1), b))
        ag_send(col, 1, own, dev_ab(col, m4(a - 1), b))
    for col in range(2):
        a, b = pos(col)
        own = at_ab(col, a, b, c)
        second(col, 0, own)
        across(0, own)

    mix_logits = nt(mix_t[...], hidden[...])
    info2[zl, 0:4] = lse_t[...]
    info2[zl, 4:8] = mix_logits - jnp.log(jnp.sum(jnp.exp(mix_logits), axis=0, keepdims=True))
    info2[zl, 8:9] = scale[...]
    info2[zl, 9:10] = target[...].astype(F32)
    info2[zl, 10:16] = jnp.zeros((6, T), F32)

    def row_columns(g):
        cols = jnp.transpose(jnp.concatenate([info2[g], jnp.zeros((112, T), F32)], axis=0))
        local = cols[:, 9:10] - (v * VL + zl * VH).astype(F32)
        for k in range(K):
            rows = pl.ds(pl.multiple_of(g * R + k * T, T), T)
            lsec[rows, :] = jnp.broadcast_to(cols[:, k : k + 1], (T, 128))
            tgtc[rows, :] = jnp.broadcast_to(local, (T, 128))

    row_columns(zl)
    info_copy = rc(info2.at[zl], info2.at[zl], sem_i.at[0], sem_i.at[1], partner_z)
    info_copy.start()

    def hs_copy(i):
        p = m4(x + (0, 1, -1, 2)[i])
        return rc(
            hidden.at[:, pl.ds(pl.multiple_of(p * 512, 512), 512)], hs.at[i], hs_s, hs_r, dev(x_=p)
        )

    for i in range(1, 4):
        hs_copy(i).start()
    hs[0] = hidden[:, pl.ds(pl.multiple_of(x * 512, 512), 512)]

    def pick(g):
        def step(n, carry):
            rows = pl.ds(pl.multiple_of(n * 512, 512), 512)
            acc = jnp.zeros((T, 512), F32)
            for q in range(4):
                lane = lax.broadcasted_iota(jnp.int32, (T, 512), 1).astype(F32) + float(q * 512)
                tgt = tgtc[pl.ds(pl.multiple_of(g * R, R), T), :][:, 0:1]
                hot = (lane == tgt).astype(F32).astype(BF16)
                acc = acc + nt(hot, w[rows, pl.ds(q * 512, 512)])
            wt[pl.ds(pl.multiple_of(g * T, T), T), rows] = acc.astype(BF16)
            return carry

        lax.fori_loop(0, 4, step, 0)

    w_copy.wait()
    pick(zl)

    for col in range(2):
        a, b = pos(col)
        prev, nxt = m4(a - 1), m4(a + 1)
        ag_wait(col, 0, at_ab(col, prev, b, c))
        ag_send(col, 2, at_ab(col, prev, b, c, 0, T), dev_ab(col, nxt, b))
        ag_wait(col, 1, at_ab(col, nxt, b, c))
        ag_send(col, 2, at_ab(col, nxt, b, c, T, T), dev_ab(col, prev, b))
    for i, step in ((1, -1), (2, 1)):
        for col in range(2):
            a, b = pos(col)
            second(col, i, at_ab(col, m4(a + step), b, c))
            across(i, at_ab(col, m4(a + step), b, c))

    def near(i):
        for col in range(2):
            a, b = pos(col)
            a_ = m4(a + (0, -1, 1, 2)[i])
            prev, nxt = m4(b - 1), m4(b + 1)
            ag_wait(col, 3 + 3 * i, at_ab(col, a_, prev, c))
            ag_send(col, 3 + 3 * i + 2, at_ab(col, a_, prev, c, 0, T), dev_ab(col, a, nxt))
            ag_wait(col, 3 + 3 * i + 1, at_ab(col, a_, nxt, c))
            ag_send(col, 3 + 3 * i + 2, at_ab(col, a_, nxt, c, T, T), dev_ab(col, a, prev))
            across(i, at_ab(col, a_, prev, c))
            across(i, at_ab(col, a_, nxt, c))

    def flip_near(i):
        for col in range(2):
            a, b = pos(col)
            a_ = m4(a + (0, -1, 1, 2)[i])
            for step in (0, -1, 1):
                flip(col, a_, m4(b + step), c)

    def far(i):
        for col in range(2):
            a, b = pos(col)
            a_ = m4(a + (0, -1, 1, 2)[i])
            b_ = m4(b + 2)
            ag_wait(col, 3 + 3 * i + 2, at_ab(col, a_, b_, c))
            across(i, at_ab(col, a_, b_, c))
            flip(col, a_, b_, c)

    def partner_wait(i):
        ag_wait(None, i, comp.at[pl.ds(0, T), :])

    def flip_partner(i):
        for col in range(2):
            a, b = pos(col)
            a_ = m4(a + (0, -1, 1, 2)[i])

            def flip_step(b_, carry):
                flip(col, a_, b_, 1 - c)
                return carry

            lax.fori_loop(0, 4, flip_step, 0)

    near(0)
    info_in = rc(info2.at[1 - zl], info2.at[1 - zl], sem_i.at[0], sem_i.at[1], partner_z)
    info_in.wait_recv()
    row_columns(1 - zl)
    pick(1 - zl)
    for col in range(2):
        a, b = pos(col)
        two = m4(a + 2)
        ag_wait(col, 2, at_ab(col, two, b, c))
        second(col, 3, at_ab(col, two, b, c))
        across(3, at_ab(col, two, b, c))
    near(1)
    near(2)
    for i in range(3):
        flip_near(i)
    far(0)
    near(3)
    partner_wait(0)
    flip_partner(0)
    far(1)
    far(2)
    flip_near(3)
    partner_wait(1)
    flip_partner(1)
    partner_wait(2)
    flip_partner(2)
    far(3)
    partner_wait(3)

    lane_t = lax.broadcasted_iota(jnp.int32, (T, 128), 1)
    acc = jnp.zeros((T, 128), F32)
    for g in range(2):
        for k in range(K):
            s = jnp.zeros((T, 128), F32)
            for q in range(4):
                prod = comp[pl.ds(g * R + k * T, T), pl.ds(q * 512, 512)].astype(F32) * wt[
                    pl.ds(g * T, T), pl.ds(q * 512, 512)
                ].astype(F32)
                for e in range(4):
                    s = s + prod[:, e * 128 : (e + 1) * 128]
            acc = jnp.where(lane_t == g * K + k, jnp.sum(s, axis=1, keepdims=True), acc)
    tl[0] = jnp.transpose(acc)[0:8]

    def tl_copy(o):
        return rc(tl.at[0], tl.at[o], tl_s, tl_r, mate(o))

    def tl_start(o, carry):
        tl_copy(o).start()
        return carry

    lax.fori_loop(1, 32, tl_start, 0)

    lane_w = lax.broadcasted_iota(jnp.int32, (2 * T, 128), 1).astype(F32)

    def block_logits(p, m, put):
        rows = pl.ds(pl.multiple_of(m * 2 * T, 2 * T), 2 * T)
        logit = nn(comp[rows, :], w[:, pl.ds(pl.multiple_of(p * W2, W2), W2)])
        shift = jnp.asarray(p * W2, F32)
        lse_m, tgt_m = lsec[rows, :], tgtc[rows, :] - shift
        for e in range(W2 // 128):
            prob = jnp.exp(logit[:, e * 128 : (e + 1) * 128] - lse_m)
            hot = jnp.where(lane_w + float(e * 128) == tgt_m, 1.0, 0.0)
            put(rows, e, prob - hot)

    def hold(m, carry):
        def put(rows, e, val):
            pbuf[rows, pl.ds(e * 128, 128)] = val

        block_logits(0, m, put)
        return carry

    lax.fori_loop(0, 4, hold, 0)
    flip_partner(3)

    tl_all = rc(tl.at[pl.ds(1, 31)], tl.at[pl.ds(1, 31)], tl_s, tl_r, partner_c)
    tl_all.wait_recv()
    target_logit = jnp.sum(tl[...], axis=0)
    coef_rows = []
    gml_rows = []
    for g in range(2):
        lse_g = info2[g, 0:4]
        lm_g = info2[g, 4:8]
        scale_g = info2[g, 8:9]
        weights = jnp.exp(lm_g + target_logit[g * K : (g + 1) * K] - lse_g)
        resp = weights / jnp.sum(weights, axis=0, keepdims=True)
        coef_rows.append(scale_g * resp)
        gml_rows.append(-scale_g * (resp - jnp.exp(lm_g)))
    table = jnp.concatenate(coef_rows + [jnp.zeros((120, 128), F32)], axis=0)
    cols = jnp.transpose(table)
    for g in range(2):
        for k in range(K):
            coefc[pl.ds(g * R + k * T, T), :] = jnp.broadcast_to(
                cols[:, g * K + k : g * K + k + 1], (T, 128)
            )
    mine = jnp.where(zl == 0, gml_rows[0], gml_rows[1])
    high = mine.astype(BF16).astype(F32)
    gmla[0] = jnp.concatenate([high, mine - high, jnp.zeros((8, T), F32)], axis=0).astype(BF16)
    for i in range(1, 4):
        rc(gmla.at[0], gmla.at[i], gm_s, gm_r, dev(x_=m4(x + (0, 1, -1, 2)[i]))).start()

    def ring(piece, me, right, left, r1, rf, ss, r1_sem, rf_sem, r1_all, rf_all):
        two, one, back = m4(me + 2), m4(me + 1), m4(me - 1)
        copies = (
            lambda: rc(piece(two, 0), r1(0), ss, r1_sem, right),
            lambda: rc(piece(one, 1), rf(0, 1), ss, rf_sem, right),
            lambda: rc(piece(two, 1), r1(1), ss, r1_sem, left),
            lambda: rc(piece(back, 0), rf(1, 0), ss, rf_sem, left),
            lambda: rc(piece(one, 0), rf(0, 0), ss, rf_sem, right),
            lambda: rc(piece(back, 1), rf(1, 1), ss, rf_sem, left),
        )

        def first(which=(0, 2, 1, 3)):
            for i in which:
                copies[i]().start()

        def add(ref, other):
            ref[...] = (ref[...].astype(F32) + other[...].astype(F32)).astype(BF16)

        def forward():
            rc(r1_all, r1_all, ss, r1_sem, right).wait_recv()
            add(piece(one, 0), r1(0))
            copies[4]().start()
            add(piece(back, 1), r1(1))
            copies[5]().start()

        def arrive():
            rc(rf_all, rf_all, ss, rf_sem, right).wait_recv()

        return first, forward, arrive

    x_right, x_left = dev(x_=m4(x + 1)), dev(x_=m4(x - 1))

    def x_ring(cc):
        return ring(
            lambda t, h: part.at[cc, t * 2 + h],
            x,
            x_right,
            x_left,
            lambda i: r1x.at[cc, i],
            lambda i, h: rfx.at[cc, i, h],
            x_s,
            x_r.at[2 * cc],
            x_r.at[2 * cc + 1],
            r1x.at[cc],
            rfx.at[cc],
        )

    def grad_out(p, tiles, send=True):
        cols = pl.ds(p * W2, W2)
        order = ((2, 0), (2, 1), (1, 1), (-1, 0), (1, 0), (-1, 1), (0, 0), (0, 1))
        for i in tiles:
            step, h = order[i]
            t = m4(x + step)
            rows = pl.ds(pl.multiple_of(t * 512 + h * 256, 256), 256)
            res = nn(comp_t[rows, :], gl[:, cols]).astype(BF16)
            for e in range(2):
                part[2 * p + e, t * 2 + h] = res[:, e * C : (e + 1) * C]
            if send and i < 4:
                for e in range(2):
                    x_ring(2 * p + e)[0](((0, 2, 1, 3)[i],))

    def scale_first(m, carry):
        rows = pl.ds(pl.multiple_of(m * 2 * T, 2 * T), 2 * T)
        coef_m = coefc[rows, :]
        for e in range(W2 // 128):
            gl[rows, pl.ds(e * 128, 128)] = (coef_m * pbuf[rows, pl.ds(e * 128, 128)]).astype(BF16)
        return carry

    lax.fori_loop(0, 4, scale_first, 0)

    def grad_logits(p):
        def rows_of(m, carry):
            coef_m = coefc[pl.ds(pl.multiple_of(m * 2 * T, 2 * T), 2 * T), :]

            def put(rows, e, val):
                gl[rows, pl.ds(pl.multiple_of(p * W2 + e * 128, 128), 128)] = (coef_m * val).astype(
                    BF16
                )

            block_logits(p, m, put)
            return carry

        lax.fori_loop(0, 4, rows_of, 0)

    def comp_grad(bat):
        def tile(i, carry):
            g, h, j = lax.div(i, 4), lax.rem(lax.div(i, 2), 2), lax.rem(i, 2)
            rows = pl.ds(pl.multiple_of(g * R + bat * 2 * T, 2 * T), 2 * T)
            units = pl.ds(pl.multiple_of((h * 2 + j) * 512, 512), 512)
            res = nt(gl[rows, :], w[units, :])
            z_ = h * 2 + g
            for jj in range(4):
                y_ = j * 2 + jj // 2
                val = res[:, jj * 128 : (jj + 1) * 128].astype(BF16)
                gcb[jj % 2, 2 * bat, z_, y_] = val[0:T]
                gcb[jj % 2, 2 * bat + 1, y_, z_] = val[T : 2 * T]
            return carry

        lax.fori_loop(0, 6, tile, 0)
        if bat == 1:
            x_finish(0)
        lax.fori_loop(6, 8, tile, 0)
        two = pl.ds(2 * bat, 2)
        swap = rc(gcb.at[1 - c, two], rd.at[two], d_s.at[bat], d_r.at[bat], partner_c)
        swap.start()
        return swap

    def a_ring(k):
        me = z if k % 2 == 0 else y
        mk = (lambda p: dev(z_=p)) if k % 2 == 0 else (lambda p: dev(y_=p))
        return ring(
            lambda t, h: gcb.at[c, k, t, pl.ds(2 * h, 2)],
            me,
            mk(m4(me + 1)),
            mk(m4(me - 1)),
            lambda i: r1a.at[k, i],
            lambda i, h: rfa.at[k, i, h],
            a_s,
            a_r.at[2 * k],
            a_r.at[2 * k + 1],
            r1a.at[k],
            rfa.at[k],
        )

    def b_copies(k):
        first, me = (z, y) if k % 2 == 0 else (y, z)
        mk = (lambda p: dev(y_=p)) if k % 2 == 0 else (lambda p: dev(z_=p))
        return [
            rc(gcb.at[c, k, first, t], rfb.at[k, o - 1], b_s, b_r.at[k], mk(t))
            for o in range(1, 4)
            for t in [m4(me + o)]
        ]

    def merge(bat, swap):
        swap.wait_recv()

        def add(i, carry):
            p, q = lax.div(i, 4), lax.rem(i, 4)
            for k in (2 * bat, 2 * bat + 1):
                gcb[c, k, p, q] = (
                    gcb[c, k, p, q].astype(F32) + rd[k, p, q].astype(F32)
                ).astype(BF16)
            return carry

        lax.fori_loop(0, 16, add, 0)
        for k in (2 * bat, 2 * bat + 1):
            a_ring(k)[0]()

    def forward_a(bat):
        for k in (2 * bat, 2 * bat + 1):
            a_ring(k)[1]()

    def finish_a(bat):
        for k in (2 * bat, 2 * bat + 1):
            a_ring(k)[2]()
            me = z if k % 2 == 0 else y
            for h in range(2):
                for e in range(2):
                    q = 2 * h + e
                    gcb[c, k, me, q] = (
                        gcb[c, k, me, q].astype(F32)
                        + rfa[k, 0, h, e].astype(F32)
                        + rfa[k, 1, h, e].astype(F32)
                    ).astype(BF16)
            for cp in b_copies(k):
                cp.start()

    def finish_b(bat):
        for k in (2 * bat, 2 * bat + 1):
            rc(rfb.at[k], rfb.at[k], b_s, b_r.at[k], partner_c).wait_recv()
            first, me = (z, y) if k % 2 == 0 else (y, z)
            total = gcb[c, k, first, me].astype(F32)
            for o in range(3):
                total = total + rfb[k, o].astype(F32)
            cf = comp[
                pl.ds(pl.multiple_of(own_rows + k * T, T), T), pl.ds(own_cols, U)
            ].astype(F32)
            gpx[k] = (total * (1.0 - cf * cf)).astype(BF16)

    def x_finish(cc):
        x_ring(cc)[2]()
        for h in range(2):
            part[cc, x * 2 + h] = (
                part[cc, x * 2 + h].astype(F32)
                + rfx[cc, 0, h].astype(F32)
                + rfx[cc, 1, h].astype(F32)
            ).astype(BF16)
        for cp in z_copies(cc):
            cp.start()

    def z_copies(cc):
        cols = pl.ds(pl.multiple_of(zl * VH + cc * C, C), C)
        dst = go_out.at[:, cols]
        return (
            rc(part.at[cc, x * 2 + 1 - zl], dst, zx_s, zx_r, partner_z),
            pltpu.make_async_copy(part.at[cc, x * 2 + zl], dst, zx_l),
        )

    first_half, second_half, every = range(4), range(4, 8), range(8)
    grad_out(0, every)
    grad_logits(1)
    grad_out(1, every)
    x_ring(0)[1]()
    grad_logits(2)
    grad_logits(3)
    x_ring(1)[1]()
    swap0 = comp_grad(0)
    x_ring(2)[1]()
    grad_out(2, first_half)
    merge(0, swap0)
    swap1 = comp_grad(1)
    forward_a(0)
    x_ring(3)[1]()
    x_finish(1)
    grad_out(2, second_half)
    merge(1, swap1)
    finish_a(0)
    hs_all = rc(hs.at[pl.ds(1, 3)], hs.at[pl.ds(1, 3)], hs_s, hs_r, partner_c)
    hs_all.wait_recv()
    for i in range(4):
        hst[:, pl.ds(i * T, T)] = jnp.transpose(hs[i])
    grad_out(3, first_half, False)
    forward_a(1)
    x_finish(2)
    grad_out(3, second_half, False)
    x_ring(4)[1]()
    finish_b(0)
    finish_a(1)
    finish_b(1)

    def slot(i, r0=0, n=T):
        return gpall.at[:, pl.ds(i * T + r0, n)]

    g_copies = (
        rc(gpx, slot(1), g_s, g_r.at[0], x_right),
        rc(gpx, slot(2), g_s, g_r.at[1], x_left),
        rc(slot(1, 0, T // 2), slot(3, 0, T // 2), g_s, g_r.at[2], x_right),
        rc(slot(2, T // 2, T // 2), slot(3, T // 2, T // 2), g_s, g_r.at[2], x_left),
    )
    g_copies[0].start()
    g_copies[1].start()
    x_ring(6)[0]()

    def h_copy(o):
        p = lax.rem(v + o, 16)
        to = (x, zl, lax.div(p, 8), lax.rem(lax.div(p, 2), 4), lax.rem(p, 2))
        return rc(hts.at[o], hrecv.at[o], h_s, h_r, to)

    def h_tile(o):
        p = lax.rem(v + o, 16)
        rows = pl.ds(pl.multiple_of(p * U, U), U)
        acc = nt(gpx[0], proj[0, rows, :])
        for k in range(1, K):
            acc = acc + nt(gpx[k], proj[k, rows, :])
        return acc

    def h_step(o, carry):
        hts[o] = h_tile(o).astype(BF16)
        h_copy(o).start()
        return carry

    lax.fori_loop(1, 16, h_step, 0)
    hrecv[0] = h_tile(0).astype(BF16)
    gpall[:, pl.ds(0, T)] = gpx[...]
    x_finish(3)
    x_finish(4)
    g_copies[0].wait_recv()
    g_copies[2].start()
    g_copies[1].wait_recv()
    g_copies[3].start()
    x_ring(5)[1]()
    x_ring(7)[0]()

    rc(slot(3), slot(3), g_s, g_r.at[2], x_right).wait_recv()

    def product(half, k):
        return nn(hst[pl.ds(pl.multiple_of(half * 256, 256), 256), :], gpall[k])

    def mix_product(half):
        rows = pl.ds(pl.multiple_of(half * 256, 256), 256)
        res = nt(gmla[0], hst[rows, pl.ds(0, T)])
        for i in range(1, 4):
            res = res + nt(gmla[i], hst[rows, pl.ds(i * T, T)])
        return res[0:4] + res[4:8]

    for k in range(K):
        prods[k] = product(1 - zl, k).astype(BF16)
    gm_all = rc(gmla.at[pl.ds(1, 3)], gmla.at[pl.ds(1, 3)], gm_s, gm_r, partner_c)
    gm_all.wait_recv()
    gms[...] = mix_product(1 - zl)
    p_copies = (
        rc(prods, prodr, p_s.at[0], p_r.at[0], partner_z),
        rc(gms, gmr, p_s.at[1], p_r.at[1], partner_z),
    )
    for cp in p_copies:
        cp.start()
    x_ring(6)[1]()
    x_finish(5)
    x_ring(7)[1]()
    x_finish(6)
    h_all = rc(hts.at[pl.ds(1, 15)], hrecv.at[pl.ds(1, 15)], h_s, h_r, partner_c)
    h_all.wait_recv()
    mw = jnp.concatenate(
        [mix_t[:, pl.ds(own_cols, U)].astype(F32)] * 2 + [jnp.zeros((8, U), F32)], axis=0
    ).astype(BF16)
    gh = lax.dot_general(gmla[0], mw, (((0,), (0,)), ((), ())), preferred_element_type=F32)
    for o in range(16):
        gh = gh + hrecv[o].astype(F32)
    gh_v[...] = gh.astype(BF16)
    out_copies = (
        pltpu.make_async_copy(gh_v, gh_out, sem_o.at[0]),
        pltpu.make_async_copy(gp_v, gp_out, sem_o.at[1]),
        pltpu.make_async_copy(gm_v, gm_out, sem_o.at[2]),
    )
    out_copies[0].start()
    x_finish(7)
    for cp in p_copies:
        cp.wait_recv()
    for k in range(K):
        gp_v[k] = (product(zl, k) + prodr[k].astype(F32)).astype(BF16)
    gm_v[...] = mix_product(zl) + gmr[...]
    out_copies[1].start()
    out_copies[2].start()

    for cp in (info_copy, swap0, swap1, *p_copies, tl_all, hs_all, h_all, gm_all):
        cp.wait_send()
    for ref, sem in (
        (comp.at[pl.ds(0, 992), :], ag_s),
        (part.at[pl.ds(0, 6)], x_s),
        (part.at[0], zx_s),
        (gcb.at[0, pl.ds(0, 3)], a_s),
        (gcb.at[0, 0, pl.ds(0, 3)], b_s),
        (gpall.at[:, pl.ds(0, 3 * T)], g_s),
    ):
        rc(ref, ref, sem, zx_r, partner_z).wait_send()
    half_out = go_out.at[:, pl.ds(0, VH)]
    rc(half_out, half_out, zx_s, zx_r, partner_z).wait_recv()
    pltpu.make_async_copy(part.at[0], part.at[0], zx_l).wait()
    for cp in out_copies:
        cp.wait()


def place(gh, gm, gp, go, gh_o, gm_o, gp_o, go_o, b_gh, b_gm, b_gp, b_go, s_in, s_out):
    pairs = [(gh, b_gh, gh_o), (gm, b_gm, gm_o), (gp, b_gp, gp_o)]
    for i in range(4):
        rows = pl.ds(i * 64, 64)
        pairs.append((go.at[rows], b_go.at[rows], go_o.at[rows]))
    loads = [pltpu.make_async_copy(s, b, s_in.at[i]) for i, (s, b, _) in enumerate(pairs)]
    stores = [pltpu.make_async_copy(b, t, s_out.at[i]) for i, (_, b, t) in enumerate(pairs)]
    for cp in reversed(loads):
        cp.start()
    for i in reversed(range(len(pairs))):
        loads[i].wait()
        stores[i].start()
    for cp in stores:
        cp.wait()


def shards(hidden, mix_weight, proj_weight, out_weight, saved_lse, targets, loss_scale):
    vm = pl.BlockSpec(memory_space=pltpu.VMEM)
    hbm = pl.BlockSpec(memory_space=pltpu.HBM)
    dma = pltpu.SemaphoreType.DMA
    outs = (
        jax.ShapeDtypeStruct((T, U), BF16),
        jax.ShapeDtypeStruct((K, 256), F32),
        jax.ShapeDtypeStruct((K, 256, U), BF16),
        jax.ShapeDtypeStruct((256, VL), BF16),
    )
    found = pl.pallas_call(
        kernel,
        out_shape=outs,
        in_specs=[vm, vm, vm, vm, hbm, hbm, hbm],
        out_specs=(hbm, hbm, hbm, hbm),
        scratch_shapes=[
            pltpu.VMEM((T, D), BF16),
            pltpu.VMEM((K, D, U), BF16),
            pltpu.VMEM((D, VH), BF16),
            pltpu.VMEM((2 * R, D), BF16),
            pltpu.VMEM((D, 2 * R), BF16),
            pltpu.VMEM((2 * R, VH), BF16),
            pltpu.VMEM((NC, 8, 256, C), BF16),
            pltpu.VMEM((NC, 2, 256, C), BF16),
            pltpu.VMEM((NC, 2, 2, 256, C), BF16),
            pltpu.VMEM((2, 4, 4, 4, T, U), BF16),
            pltpu.VMEM((4, 4, 4, T, U), BF16),
            pltpu.VMEM((4, 2, 2, T, U), BF16),
            pltpu.VMEM((4, 2, 2, 2, T, U), BF16),
            pltpu.VMEM((4, 3, T, U), BF16),
            pltpu.VMEM((2 * T, D), BF16),
            pltpu.VMEM((4, T, 512), BF16),
            pltpu.VMEM((512, 4 * T), BF16),
            pltpu.VMEM((K, T, U), BF16),
            pltpu.VMEM((K, 4 * T, U), BF16),
            pltpu.VMEM((4, 16, T), BF16),
            pltpu.VMEM((K, 256, U), BF16),
            pltpu.VMEM((K, 256, U), BF16),
            pltpu.VMEM((K, 256), F32),
            pltpu.VMEM((K, 256), F32),
            pltpu.VMEM((16, T, U), BF16),
            pltpu.VMEM((16, T, U), BF16),
            pltpu.VMEM((2, 16, T), F32),
            pltpu.VMEM((2 * R, 128), F32),
            pltpu.VMEM((2 * R, 128), F32),
            pltpu.VMEM((2 * R, 128), F32),
            pltpu.VMEM((32, 8, T), F32),
            pltpu.VMEM((2 * R, W2), F32),
            pltpu.VMEM((T, U), BF16),
            pltpu.VMEM((K, 256), F32),
            pltpu.VMEM((K, 256, U), BF16),
            dma((3,)),
            dma((2,)),
            dma((2,)),
            dma((2,)),
            dma((3,)),
            dma,
            dma((34,)),
            dma,
            dma,
            dma,
            dma,
            dma,
            dma((16,)),
            dma,
            dma,
            dma,
            dma((2,)),
            dma((2,)),
            dma,
            dma((8,)),
            dma,
            dma((4,)),
            dma,
            dma,
            dma,
            dma((3,)),
            dma,
            dma,
        ],
        compiler_params=pltpu.CompilerParams(
            collective_id=0, has_side_effects=True, vmem_limit_bytes=67043328
        ),
    )(
        mix_weight.T,
        saved_lse.T,
        loss_scale[None, :],
        targets[None, :],
        hidden,
        proj_weight,
        out_weight,
    )
    gh, gm, gp, go = pl.pallas_call(
        place,
        out_shape=outs,
        in_specs=[hbm] * 4,
        out_specs=(hbm,) * 4,
        scratch_shapes=[pltpu.VMEM(o.shape, o.dtype) for o in outs] + [dma((7,)), dma((7,))],
    )(*found)
    return gh, gm.T, gp, go


def solution(mesh):
    finer = Mesh(mesh.devices.reshape(4, 2, 2, 4, 2), AXES)
    in_specs = (
        P(DP, None),
        P(),
        P(None, None, VOC),
        P(None, VOC),
        P(DP, None),
        P(DP),
        P(DP),
    )
    out_specs = (P(DP, VOC), P(DP, None), P(None, DP, VOC), P(DP, VOC))
    return jax.shard_map(
        shards, mesh=finer, in_specs=in_specs, out_specs=out_specs, check_vma=False
    )
```

```python
import functools

import jax
import jax.numpy as jnp
from jax import lax
from jax.experimental import pallas as pl
from jax.experimental.pallas import tpu as pltpu
from jax.sharding import Mesh
from jax.sharding import PartitionSpec as P

AXES = ("x", "zl", "zh", "y", "c")
DP = ("x", "zl")
VOC = ("zh", "y", "c")
MESH_ID = pl.DeviceIdType.MESH
F32 = jnp.float32
BF16 = jnp.bfloat16

T = 128
K = 4
R = T * K
U = 128
D = 2048
VL = 4096
VH = VL // 2
NC = 8
C = VH // NC
W2 = 2 * C


def nt(a, b):
    return lax.dot_general(a, b, (((1,), (1,)), ((), ())), preferred_element_type=F32)


def nn(a, b):
    return lax.dot_general(a, b, (((1,), (0,)), ((), ())), preferred_element_type=F32)


def kernel(
    mix_t,
    lse_t,
    scale,
    target,
    hidden_hbm,
    proj_hbm,
    w_hbm,
    gh_out,
    gm_out,
    gp_out,
    go_out,
    hidden,
    proj,
    w,
    comp,
    comp_t,
    gl,
    part,
    r1x,
    rfx,
    gcb,
    rd,
    r1a,
    rfa,
    rfb,
    wt,
    hs,
    hst,
    gpx,
    gpall,
    gmla,
    prods,
    prodr,
    gms,
    gmr,
    hts,
    hrecv,
    info2,
    lsec,
    coefc,
    tgtc,
    tl,
    tacc,
    pbuf,
    gh_v,
    gm_v,
    gp_v,
    sem_w,
    sem_i,
    p_s,
    p_r,
    sem_o,
    ag_s,
    ag_r,
    hs_s,
    hs_r,
    tl_s,
    tl_r,
    x_s,
    x_r,
    zx_s,
    zx_r,
    zx_l,
    d_s,
    d_r,
    a_s,
    a_r,
    b_s,
    b_r,
    h_s,
    h_r,
    g_s,
    g_r,
    gm_s,
    gm_r,
):
    x = lax.axis_index("x")
    zl = lax.axis_index("zl")
    zh = lax.axis_index("zh")
    y = lax.axis_index("y")
    c = lax.axis_index("c")
    z = zh * 2 + zl
    v = zh * 8 + y * 2 + c
    d = x * 2 + zl

    def m4(i):
        return lax.rem(i + 4, 4)

    def dev(x_=None, z_=None, y_=None, c_=None):
        zz = z if z_ is None else z_
        return (
            x if x_ is None else x_,
            lax.rem(zz, 2),
            lax.div(zz, 2),
            y if y_ is None else y_,
            c if c_ is None else c_,
        )

    def rc(src, dst, ss, rs, to):
        return pltpu.make_async_remote_copy(
            src_ref=src, dst_ref=dst, send_sem=ss, recv_sem=rs, device_id=to, device_id_type=MESH_ID
        )

    partner_c = dev(c_=1 - c)
    partner_z = (x, 1 - zl, zh, y, c)

    hidden_copy = pltpu.make_async_copy(hidden_hbm, hidden, sem_w.at[0])
    proj_copy = pltpu.make_async_copy(proj_hbm, proj, sem_w.at[1])
    w_copy = pltpu.make_async_copy(
        w_hbm.at[:, pl.ds(pl.multiple_of(zl * VH, VH), VH)], w, sem_w.at[2]
    )
    hidden_copy.start()
    proj_copy.start()
    w_copy.start()

    q32 = z * 8 + y * 2 + c

    def mate(o):
        p = lax.rem(q32 + o, 32)
        zz = lax.div(p, 8)
        return (x, lax.rem(zz, 2), lax.div(zz, 2), lax.rem(lax.div(p, 2), 4), lax.rem(p, 2))

    barrier = pltpu.get_barrier_semaphore()

    def greet(o, carry):
        pl.semaphore_signal(barrier, inc=1, device_id=mate(o), device_id_type=MESH_ID)
        return carry

    lax.fori_loop(1, 32, greet, 0)
    for o in range(1, 4):
        pl.semaphore_signal(barrier, inc=1, device_id=dev(x_=m4(x + o)), device_id_type=MESH_ID)

    own_cols = pl.multiple_of(v * U, U)

    def blk(col, z_, y_, c_, r0=0, n=2 * T):
        block = lax.rem(z_, 2) * 16 + lax.div(z_, 2) * 8 + y_ * 2 + c_
        return comp.at[block, pl.ds(col * 2 * T + r0, n)]

    def pos(col):
        return (y, z) if col == 0 else (z, y)

    def at_ab(col, a_, b_, c_, r0=0, n=2 * T):
        return blk(col, b_, a_, c_, r0, n) if col == 0 else blk(col, a_, b_, c_, r0, n)

    def dev_ab(col, a_, b_):
        return dev(y_=a_, z_=b_) if col == 0 else dev(z_=a_, y_=b_)

    def ag_copy(col, i, ref, to):
        r = 30 + i if col is None else col * 15 + i
        return rc(ref, ref, ag_s, ag_r.at[r], to)

    def ag_send(col, i, ref, to):
        ag_copy(col, i, ref, to).start()

    def ag_wait(col, i, ref):
        ag_copy(col, i, ref, partner_c).wait_recv()

    def second(col, i, ref):
        a, b = pos(col)
        ag_send(col, 3 + 3 * i, ref, dev_ab(col, a, m4(b + 1)))
        ag_send(col, 3 + 3 * i + 1, ref, dev_ab(col, a, m4(b - 1)))

    def across(i, ref):
        ag_send(None, i, ref, partner_c)

    def flip(col, a_, b_, c_):
        z_, y_ = (b_, a_) if col == 0 else (a_, b_)
        row = pl.multiple_of(lax.rem(z_, 2) * R + col * 2 * T, 2 * T)
        unit = lax.div(z_, 2) * 8 + y_ * 2 + c_
        comp_t[pl.ds(pl.multiple_of(unit * U, U), U), pl.ds(row, 2 * T)] = jnp.transpose(
            comp[lax.rem(z_, 2) * 16 + unit, pl.ds(col * 2 * T, 2 * T)]
        )

    def gauge(col, a_, b_, c_):
        z_, y_ = (b_, a_) if col == 0 else (a_, b_)
        g = lax.rem(z_, 2)
        unit = lax.div(z_, 2) * 8 + y_ * 2 + c_
        weight = wt[
            pl.ds(pl.multiple_of(g * T, T), T), pl.ds(pl.multiple_of(unit * U, U), U)
        ].astype(F32)
        for k in (2 * col, 2 * col + 1):
            tacc[g * K + k] += comp[g * 16 + unit, pl.ds(k * T, T)].astype(F32) * weight

    hidden_copy.wait()
    proj_copy.wait()
    for k in range(K):
        pre = nn(hidden[...], proj[k])
        comp[zl * 16 + v, pl.ds(k * T, T)] = jnp.tanh(pre).astype(BF16)
    pl.semaphore_wait(barrier, 34)
    for col in range(2):
        a, b = pos(col)
        own = at_ab(col, a, b, c)
        ag_send(col, 0, own, dev_ab(col, m4(a + 1), b))
        ag_send(col, 1, own, dev_ab(col, m4(a - 1), b))

    mix_logits = nt(mix_t[...], hidden[...])
    info2[zl, 0:4] = lse_t[...]
    info2[zl, 4:8] = mix_logits - jnp.log(jnp.sum(jnp.exp(mix_logits), axis=0, keepdims=True))
    info2[zl, 8:9] = scale[...]
    info2[zl, 9:10] = target[...].astype(F32)
    info2[zl, 10:16] = jnp.zeros((6, T), F32)

    def row_columns(g):
        cols = jnp.transpose(jnp.concatenate([info2[g], jnp.zeros((112, T), F32)], axis=0))
        local = cols[:, 9:10] - (v * VL + zl * VH).astype(F32)
        for k in range(K):
            rows = pl.ds(pl.multiple_of(g * R + k * T, T), T)
            lsec[rows, :] = jnp.broadcast_to(cols[:, k : k + 1], (T, 128))
            tgtc[rows, :] = jnp.broadcast_to(local, (T, 128))

    row_columns(zl)
    info_copy = rc(info2.at[zl], info2.at[zl], sem_i.at[0], sem_i.at[1], partner_z)
    info_copy.start()

    for col in range(2):
        a, b = pos(col)
        own = at_ab(col, a, b, c)
        second(col, 0, own)
        across(0, own)

    def hs_copy(i):
        p = m4(x + (0, 1, -1, 2)[i])
        return rc(
            hidden.at[:, pl.ds(pl.multiple_of(p * 512, 512), 512)], hs.at[i], hs_s, hs_r, dev(x_=p)
        )

    for i in range(1, 4):
        hs_copy(i).start()
    hs[0] = hidden[:, pl.ds(pl.multiple_of(x * 512, 512), 512)]

    def pick(n, carry):
        rows = pl.ds(pl.multiple_of(n * 512, 512), 512)
        acc = jnp.zeros((2 * T, 512), F32)
        for q in range(4):
            lane = lax.broadcasted_iota(jnp.int32, (T, 512), 1).astype(F32) + float(q * 512)
            hot = jnp.concatenate(
                [
                    (lane == tgtc[pl.ds(g * R, T), :][:, 0:1]).astype(F32).astype(BF16)
                    for g in range(2)
                ],
                axis=0,
            )
            acc = acc + nt(hot, w[rows, pl.ds(q * 512, 512)])
        wt[:, rows] = acc.astype(BF16)
        return carry

    for col in range(2):
        a, b = pos(col)
        prev, nxt = m4(a - 1), m4(a + 1)
        ag_wait(col, 0, at_ab(col, prev, b, c))
        ag_send(col, 2, at_ab(col, prev, b, c, 0, T), dev_ab(col, nxt, b))
        ag_wait(col, 1, at_ab(col, nxt, b, c))
        ag_send(col, 2, at_ab(col, nxt, b, c, T, T), dev_ab(col, prev, b))
    for i, step in ((1, -1), (2, 1)):
        for col in range(2):
            a, b = pos(col)
            second(col, i, at_ab(col, m4(a + step), b, c))
            across(i, at_ab(col, m4(a + step), b, c))

    def near(i):
        for col in range(2):
            a, b = pos(col)
            a_ = m4(a + (0, -1, 1, 2)[i])
            prev, nxt = m4(b - 1), m4(b + 1)
            ag_wait(col, 3 + 3 * i, at_ab(col, a_, prev, c))
            ag_send(col, 3 + 3 * i + 2, at_ab(col, a_, prev, c, 0, T), dev_ab(col, a, nxt))
            ag_wait(col, 3 + 3 * i + 1, at_ab(col, a_, nxt, c))
            ag_send(col, 3 + 3 * i + 2, at_ab(col, a_, nxt, c, T, T), dev_ab(col, a, prev))
            across(i, at_ab(col, a_, prev, c))
            across(i, at_ab(col, a_, nxt, c))

    def flip_near(i):
        for col in range(2):
            a, b = pos(col)
            a_ = m4(a + (0, -1, 1, 2)[i])
            for step in (0, -1, 1):
                flip(col, a_, m4(b + step), c)
                gauge(col, a_, m4(b + step), c)

    def far(i):
        for col in range(2):
            a, b = pos(col)
            a_ = m4(a + (0, -1, 1, 2)[i])
            b_ = m4(b + 2)
            ag_wait(col, 3 + 3 * i + 2, at_ab(col, a_, b_, c))
            across(i, at_ab(col, a_, b_, c))
            flip(col, a_, b_, c)
            gauge(col, a_, b_, c)

    def partner_wait(i):
        ag_wait(None, i, comp.at[pl.ds(0, 4)])

    def on_partner(i, act):
        for col in range(2):
            a, b = pos(col)
            a_ = m4(a + (0, -1, 1, 2)[i])

            def step(b_, carry):
                act(col, a_, b_, 1 - c)
                return carry

            lax.fori_loop(0, 4, step, 0)

    def both(*where):
        flip(*where)
        gauge(*where)

    tacc[...] = jnp.zeros_like(tacc)
    near(0)
    info_in = rc(info2.at[1 - zl], info2.at[1 - zl], sem_i.at[0], sem_i.at[1], partner_z)
    info_in.wait_recv()
    row_columns(1 - zl)
    w_copy.wait()
    lax.fori_loop(0, 2, pick, 0)
    for col in range(2):
        a, b = pos(col)
        two = m4(a + 2)
        ag_wait(col, 2, at_ab(col, two, b, c))
        second(col, 3, at_ab(col, two, b, c))
        across(3, at_ab(col, two, b, c))
    lax.fori_loop(2, 4, pick, 0)
    near(1)
    near(2)
    for i in range(3):
        flip_near(i)
    far(0)
    near(3)
    partner_wait(0)
    on_partner(0, both)
    far(1)
    far(2)
    flip_near(3)
    partner_wait(1)
    on_partner(1, both)
    partner_wait(2)
    on_partner(2, both)
    far(3)
    partner_wait(3)
    on_partner(3, gauge)

    lane_t = lax.broadcasted_iota(jnp.int32, (T, 128), 1)
    acc = jnp.zeros((T, 128), F32)
    for g in range(2):
        for k in range(K):
            acc = jnp.where(lane_t == g * K + k, jnp.sum(tacc[g * K + k], axis=1, keepdims=True), acc)
    tl[0] = jnp.transpose(acc)[0:8]

    def tl_copy(o):
        return rc(tl.at[0], tl.at[o], tl_s, tl_r, mate(o))

    def tl_start(o, carry):
        tl_copy(o).start()
        return carry

    lax.fori_loop(1, 32, tl_start, 0)

    lane_w = lax.broadcasted_iota(jnp.int32, (2 * T, 128), 1).astype(F32)

    def block_logits(p, m, put):
        rows = pl.ds(pl.multiple_of(m * 2 * T, 2 * T), 2 * T)
        g, part_rows = lax.div(m, 2), pl.ds(pl.multiple_of(lax.rem(m, 2) * 2 * T, 2 * T), 2 * T)
        vectors = jnp.concatenate([comp[g * 16 + u, part_rows] for u in range(16)], axis=1)
        logit = nn(vectors, w[:, pl.ds(pl.multiple_of(p * W2, W2), W2)])
        shift = jnp.asarray(p * W2, F32)
        lse_m, tgt_m = lsec[rows, :], tgtc[rows, :] - shift
        for e in range(W2 // 128):
            prob = jnp.exp(logit[:, e * 128 : (e + 1) * 128] - lse_m)
            hot = jnp.where(lane_w + float(e * 128) == tgt_m, 1.0, 0.0)
            put(rows, e, prob - hot)

    def hold(m, carry):
        def put(rows, e, val):
            pbuf[rows, pl.ds(e * 128, 128)] = val

        block_logits(0, m, put)
        return carry

    lax.fori_loop(0, 4, hold, 0)
    on_partner(3, flip)

    tl_all = rc(tl.at[pl.ds(1, 31)], tl.at[pl.ds(1, 31)], tl_s, tl_r, partner_c)
    tl_all.wait_recv()
    target_logit = jnp.sum(tl[...], axis=0)
    coef_rows = []
    gml_rows = []
    for g in range(2):
        lse_g = info2[g, 0:4]
        lm_g = info2[g, 4:8]
        scale_g = info2[g, 8:9]
        weights = jnp.exp(lm_g + target_logit[g * K : (g + 1) * K] - lse_g)
        resp = weights / jnp.sum(weights, axis=0, keepdims=True)
        coef_rows.append(scale_g * resp)
        gml_rows.append(-scale_g * (resp - jnp.exp(lm_g)))
    table = jnp.concatenate(coef_rows + [jnp.zeros((120, 128), F32)], axis=0)
    cols = jnp.transpose(table)
    for g in range(2):
        for k in range(K):
            coefc[pl.ds(g * R + k * T, T), :] = jnp.broadcast_to(
                cols[:, g * K + k : g * K + k + 1], (T, 128)
            )
    mine = jnp.where(zl == 0, gml_rows[0], gml_rows[1])
    high = mine.astype(BF16).astype(F32)
    gmla[0] = jnp.concatenate([high, mine - high, jnp.zeros((8, T), F32)], axis=0).astype(BF16)
    for i in range(1, 4):
        rc(gmla.at[0], gmla.at[i], gm_s, gm_r, dev(x_=m4(x + (0, 1, -1, 2)[i]))).start()

    def ring(piece, me, right, left, r1, rf, ss, r1_sem, rf_sem, r1_all, rf_all):
        two, one, back = m4(me + 2), m4(me + 1), m4(me - 1)
        copies = (
            lambda: rc(piece(two, 0), r1(0), ss, r1_sem, right),
            lambda: rc(piece(one, 1), rf(0, 1), ss, rf_sem, right),
            lambda: rc(piece(two, 1), r1(1), ss, r1_sem, left),
            lambda: rc(piece(back, 0), rf(1, 0), ss, rf_sem, left),
            lambda: rc(piece(one, 0), rf(0, 0), ss, rf_sem, right),
            lambda: rc(piece(back, 1), rf(1, 1), ss, rf_sem, left),
        )

        def first(which=(0, 2, 1, 3)):
            for i in which:
                copies[i]().start()

        def add(ref, other):
            ref[...] = (ref[...].astype(F32) + other[...].astype(F32)).astype(BF16)

        def forward():
            rc(r1_all, r1_all, ss, r1_sem, right).wait_recv()
            add(piece(one, 0), r1(0))
            copies[4]().start()
            add(piece(back, 1), r1(1))
            copies[5]().start()

        def arrive():
            rc(rf_all, rf_all, ss, rf_sem, right).wait_recv()

        return first, forward, arrive

    x_right, x_left = dev(x_=m4(x + 1)), dev(x_=m4(x - 1))

    def x_ring(cc, e=None):
        lanes = pl.ds(0, C) if e is None else pl.ds(e * 128, 128)
        sem = 2 * cc if e is None else 2 * NC + 2 * (2 * (cc - 6) + e)
        return ring(
            lambda t, h: part.at[cc, t * 2 + h, :, lanes],
            x,
            x_right,
            x_left,
            lambda i: r1x.at[cc, i, :, lanes],
            lambda i, h: rfx.at[cc, i, h, :, lanes],
            x_s,
            x_r.at[sem],
            x_r.at[sem + 1],
            r1x.at[cc, :, :, lanes],
            rfx.at[cc, :, :, :, lanes],
        )

    def grad_out(p, tiles, send=True):
        cols = pl.ds(p * W2, W2)
        order = ((2, 0), (2, 1), (1, 1), (-1, 0), (1, 0), (-1, 1), (0, 0), (0, 1))
        for i in tiles:
            step, h = order[i]
            t = m4(x + step)
            rows = pl.ds(pl.multiple_of(t * 512 + h * 256, 256), 256)
            res = nn(comp_t[rows, :], gl[:, cols]).astype(BF16)
            for e in range(2):
                part[2 * p + e, t * 2 + h] = res[:, e * C : (e + 1) * C]
            if send and i < 4:
                for e in range(2):
                    x_ring(2 * p + e)[0](((0, 2, 1, 3)[i],))

    def scale_first(m, carry):
        rows = pl.ds(pl.multiple_of(m * 2 * T, 2 * T), 2 * T)
        coef_m = coefc[rows, :]
        for e in range(W2 // 128):
            gl[rows, pl.ds(e * 128, 128)] = (coef_m * pbuf[rows, pl.ds(e * 128, 128)]).astype(BF16)
        return carry

    lax.fori_loop(0, 4, scale_first, 0)

    def grad_logits(p):
        def rows_of(m, carry):
            coef_m = coefc[pl.ds(pl.multiple_of(m * 2 * T, 2 * T), 2 * T), :]

            def put(rows, e, val):
                gl[rows, pl.ds(pl.multiple_of(p * W2 + e * 128, 128), 128)] = (coef_m * val).astype(
                    BF16
                )

            block_logits(p, m, put)
            return carry

        lax.fori_loop(0, 4, rows_of, 0)

    def comp_grad(bat):
        def tile(i, carry):
            g, h, j = lax.div(i, 4), lax.rem(lax.div(i, 2), 2), lax.rem(i, 2)
            rows = pl.ds(pl.multiple_of(g * R + bat * 2 * T, 2 * T), 2 * T)
            units = pl.ds(pl.multiple_of((h * 2 + j) * 512, 512), 512)
            res = nt(gl[rows, :], w[units, :])
            z_ = h * 2 + g
            for jj in range(4):
                y_ = j * 2 + jj // 2
                val = res[:, jj * 128 : (jj + 1) * 128].astype(BF16)
                gcb[jj % 2, 2 * bat, z_, y_] = val[0:T]
                gcb[jj % 2, 2 * bat + 1, y_, z_] = val[T : 2 * T]
            return carry

        lax.fori_loop(0, 8, tile, 0)
        two = pl.ds(2 * bat, 2)
        swap = rc(gcb.at[1 - c, two], rd.at[two], d_s.at[bat], d_r.at[bat], partner_c)
        swap.start()
        return swap

    def a_ring(k):
        me = z if k % 2 == 0 else y
        mk = (lambda p: dev(z_=p)) if k % 2 == 0 else (lambda p: dev(y_=p))
        return ring(
            lambda t, h: gcb.at[c, k, t, pl.ds(2 * h, 2)],
            me,
            mk(m4(me + 1)),
            mk(m4(me - 1)),
            lambda i: r1a.at[k, i],
            lambda i, h: rfa.at[k, i, h],
            a_s,
            a_r.at[2 * k],
            a_r.at[2 * k + 1],
            r1a.at[k],
            rfa.at[k],
        )

    def b_copies(k):
        first, me = (z, y) if k % 2 == 0 else (y, z)
        mk = (lambda p: dev(y_=p)) if k % 2 == 0 else (lambda p: dev(z_=p))
        return [
            rc(gcb.at[c, k, first, t], rfb.at[k, o - 1], b_s, b_r.at[k], mk(t))
            for o in range(1, 4)
            for t in [m4(me + o)]
        ]

    def merge(bat, swap):
        swap.wait_recv()

        def add(i, carry):
            p, q = lax.div(i, 4), lax.rem(i, 4)
            for k in (2 * bat, 2 * bat + 1):
                gcb[c, k, p, q] = (
                    gcb[c, k, p, q].astype(F32) + rd[k, p, q].astype(F32)
                ).astype(BF16)
            return carry

        lax.fori_loop(0, 16, add, 0)
        for k in (2 * bat, 2 * bat + 1):
            a_ring(k)[0]()

    def forward_a(bat):
        for k in (2 * bat, 2 * bat + 1):
            a_ring(k)[1]()

    def finish_a(bat):
        for k in (2 * bat, 2 * bat + 1):
            a_ring(k)[2]()
            me = z if k % 2 == 0 else y
            for h in range(2):
                for e in range(2):
                    q = 2 * h + e
                    gcb[c, k, me, q] = (
                        gcb[c, k, me, q].astype(F32)
                        + rfa[k, 0, h, e].astype(F32)
                        + rfa[k, 1, h, e].astype(F32)
                    ).astype(BF16)
            for cp in b_copies(k):
                cp.start()

    def finish_b(bat):
        for k in (2 * bat, 2 * bat + 1):
            rc(rfb.at[k], rfb.at[k], b_s, b_r.at[k], partner_c).wait_recv()
            first, me = (z, y) if k % 2 == 0 else (y, z)
            total = gcb[c, k, first, me].astype(F32)
            for o in range(3):
                total = total + rfb[k, o].astype(F32)
            cf = comp[zl * 16 + v, pl.ds(k * T, T)].astype(F32)
            gpx[k] = (total * (1.0 - cf * cf)).astype(BF16)

    def x_finish(cc, e=None):
        lanes = pl.ds(0, C) if e is None else pl.ds(e * 128, 128)
        x_ring(cc, e)[2]()
        for h in range(2):
            part[cc, x * 2 + h, :, lanes] = (
                part[cc, x * 2 + h, :, lanes].astype(F32)
                + rfx[cc, 0, h, :, lanes].astype(F32)
                + rfx[cc, 1, h, :, lanes].astype(F32)
            ).astype(BF16)
        if e is None:
            cols = pl.ds(pl.multiple_of(zl * VH + cc * C, C), C)
        else:
            cols = pl.ds(pl.multiple_of(zl * VH + cc * C + e * 128, 128), 128)
        dst = go_out.at[:, cols]
        rc(part.at[cc, x * 2 + 1 - zl, :, lanes], dst, zx_s, zx_r, partner_z).start()
        pltpu.make_async_copy(part.at[cc, x * 2 + zl, :, lanes], dst, zx_l).start()

    first_half, second_half, every = range(4), range(4, 8), range(8)
    grad_out(0, every)
    grad_logits(1)
    grad_out(1, every)
    x_ring(0)[1]()
    grad_logits(2)
    grad_logits(3)
    x_ring(1)[1]()
    swap0 = comp_grad(0)
    x_ring(2)[1]()
    grad_out(2, first_half)
    merge(0, swap0)
    swap1 = comp_grad(1)
    forward_a(0)
    x_ring(3)[1]()
    grad_out(2, second_half)
    merge(1, swap1)
    finish_a(0)
    hs_all = rc(hs.at[pl.ds(1, 3)], hs.at[pl.ds(1, 3)], hs_s, hs_r, partner_c)
    hs_all.wait_recv()
    for i in range(4):
        hst[:, pl.ds(i * T, T)] = jnp.transpose(hs[i])
    grad_out(3, first_half, False)
    forward_a(1)
    grad_out(3, second_half, False)
    x_ring(4)[1]()
    finish_b(0)
    finish_a(1)
    x_finish(0)
    x_finish(1)
    x_finish(2)
    finish_b(1)

    def slot(i, r0=0, n=T):
        return gpall.at[:, pl.ds(i * T + r0, n)]

    g_copies = (
        rc(gpx, slot(1), g_s, g_r.at[0], x_right),
        rc(gpx, slot(2), g_s, g_r.at[1], x_left),
        rc(slot(1, 0, T // 2), slot(3, 0, T // 2), g_s, g_r.at[2], x_right),
        rc(slot(2, T // 2, T // 2), slot(3, T // 2, T // 2), g_s, g_r.at[2], x_left),
    )
    g_copies[0].start()
    g_copies[1].start()
    x_ring(6, 0)[0]()

    def h_copy(o):
        p = lax.rem(v + o, 16)
        to = (x, zl, lax.div(p, 8), lax.rem(lax.div(p, 2), 4), lax.rem(p, 2))
        return rc(hts.at[o], hrecv.at[o], h_s, h_r, to)

    def h_tile(o):
        p = lax.rem(v + o, 16)
        rows = pl.ds(pl.multiple_of(p * U, U), U)
        acc = nt(gpx[0], proj[0, rows, :])
        for k in range(1, K):
            acc = acc + nt(gpx[k], proj[k, rows, :])
        return acc

    def h_step(o, carry):
        hts[o] = h_tile(o).astype(BF16)
        h_copy(o).start()
        return carry

    lax.fori_loop(1, 9, h_step, 0)
    x_ring(6, 1)[0]()
    lax.fori_loop(9, 16, h_step, 0)
    hrecv[0] = h_tile(0).astype(BF16)
    gpall[:, pl.ds(0, T)] = gpx[...]
    x_finish(3)
    x_finish(4)
    g_copies[0].wait_recv()
    g_copies[2].start()
    g_copies[1].wait_recv()
    g_copies[3].start()
    x_ring(5)[1]()
    x_ring(7, 0)[0]()

    rc(slot(3), slot(3), g_s, g_r.at[2], x_right).wait_recv()
    x_ring(7, 1)[0]()

    def product(half, k):
        return nn(hst[pl.ds(pl.multiple_of(half * 256, 256), 256), :], gpall[k])

    def mix_product(half):
        rows = pl.ds(pl.multiple_of(half * 256, 256), 256)
        res = nt(gmla[0], hst[rows, pl.ds(0, T)])
        for i in range(1, 4):
            res = res + nt(gmla[i], hst[rows, pl.ds(i * T, T)])
        return res[0:4] + res[4:8]

    for k in range(K):
        prods[k] = product(1 - zl, k).astype(BF16)
    gm_all = rc(gmla.at[pl.ds(1, 3)], gmla.at[pl.ds(1, 3)], gm_s, gm_r, partner_c)
    gm_all.wait_recv()
    gms[...] = mix_product(1 - zl)
    p_copies = (
        rc(prods, prodr, p_s.at[0], p_r.at[0], partner_z),
        rc(gms, gmr, p_s.at[1], p_r.at[1], partner_z),
    )
    for cp in p_copies:
        cp.start()
    x_ring(6, 0)[1]()
    x_ring(6, 1)[1]()
    x_finish(5)
    x_ring(7, 0)[1]()
    x_finish(6, 0)
    x_ring(7, 1)[1]()
    x_finish(6, 1)
    x_finish(7, 0)
    h_all = rc(hts.at[pl.ds(1, 15)], hrecv.at[pl.ds(1, 15)], h_s, h_r, partner_c)
    h_all.wait_recv()
    mw = jnp.concatenate(
        [mix_t[:, pl.ds(own_cols, U)].astype(F32)] * 2 + [jnp.zeros((8, U), F32)], axis=0
    ).astype(BF16)
    gh = lax.dot_general(gmla[0], mw, (((0,), (0,)), ((), ())), preferred_element_type=F32)
    for o in range(16):
        gh = gh + hrecv[o].astype(F32)
    gh_v[...] = gh.astype(BF16)
    out_copies = (
        pltpu.make_async_copy(gh_v, gh_out, sem_o.at[0]),
        pltpu.make_async_copy(gp_v, gp_out, sem_o.at[1]),
        pltpu.make_async_copy(gm_v, gm_out, sem_o.at[2]),
    )
    out_copies[0].start()
    x_finish(7, 1)
    for cp in p_copies:
        cp.wait_recv()
    for k in range(K):
        gp_v[k] = (product(zl, k) + prodr[k].astype(F32)).astype(BF16)
    gm_v[...] = mix_product(zl) + gmr[...]
    out_copies[1].start()
    out_copies[2].start()

    for cp in (info_copy, swap0, swap1, *p_copies, tl_all, hs_all, h_all, gm_all):
        cp.wait_send()
    for ref, sem in (
        (comp.at[pl.ds(0, 31)], ag_s),
        (part.at[pl.ds(0, 6)], x_s),
        (part.at[0], zx_s),
        (gcb.at[0, pl.ds(0, 3)], a_s),
        (gcb.at[0, 0, pl.ds(0, 3)], b_s),
        (gpall.at[:, pl.ds(0, 3 * T)], g_s),
    ):
        rc(ref, ref, sem, zx_r, partner_z).wait_send()
    half_out = go_out.at[:, pl.ds(0, VH)]
    rc(half_out, half_out, zx_s, zx_r, partner_z).wait_recv()
    pltpu.make_async_copy(part.at[0], part.at[0], zx_l).wait()
    for cp in out_copies:
        cp.wait()


def place(gh, gm, gp, go, gh_o, gm_o, gp_o, go_o, b_gh, b_gm, b_gp, b_go, s_in, s_out):
    pairs = [(gh, b_gh, gh_o), (gm, b_gm, gm_o), (gp, b_gp, gp_o)]
    for i in range(4):
        rows = pl.ds(i * 64, 64)
        pairs.append((go.at[rows], b_go.at[rows], go_o.at[rows]))
    loads = [pltpu.make_async_copy(s, b, s_in.at[i]) for i, (s, b, _) in enumerate(pairs)]
    stores = [pltpu.make_async_copy(b, t, s_out.at[i]) for i, (_, b, t) in enumerate(pairs)]
    for cp in reversed(loads):
        cp.start()
    for i in reversed(range(len(pairs))):
        loads[i].wait()
        stores[i].start()
    for cp in stores:
        cp.wait()


def shards(hidden, mix_weight, proj_weight, out_weight, saved_lse, targets, loss_scale):
    vm = pl.BlockSpec(memory_space=pltpu.VMEM)
    hbm = pl.BlockSpec(memory_space=pltpu.HBM)
    dma = pltpu.SemaphoreType.DMA
    outs = (
        jax.ShapeDtypeStruct((T, U), BF16),
        jax.ShapeDtypeStruct((K, 256), F32),
        jax.ShapeDtypeStruct((K, 256, U), BF16),
        jax.ShapeDtypeStruct((256, VL), BF16),
    )
    found = pl.pallas_call(
        kernel,
        out_shape=outs,
        in_specs=[vm, vm, vm, vm, hbm, hbm, hbm],
        out_specs=(hbm, hbm, hbm, hbm),
        scratch_shapes=[
            pltpu.VMEM((T, D), BF16),
            pltpu.VMEM((K, D, U), BF16),
            pltpu.VMEM((D, VH), BF16),
            pltpu.VMEM((32, R, U), BF16),
            pltpu.VMEM((D, 2 * R), BF16),
            pltpu.VMEM((2 * R, VH), BF16),
            pltpu.VMEM((NC, 8, 256, C), BF16),
            pltpu.VMEM((NC, 2, 256, C), BF16),
            pltpu.VMEM((NC, 2, 2, 256, C), BF16),
            pltpu.VMEM((2, 4, 4, 4, T, U), BF16),
            pltpu.VMEM((4, 4, 4, T, U), BF16),
            pltpu.VMEM((4, 2, 2, T, U), BF16),
            pltpu.VMEM((4, 2, 2, 2, T, U), BF16),
            pltpu.VMEM((4, 3, T, U), BF16),
            pltpu.VMEM((2 * T, D), BF16),
            pltpu.VMEM((4, T, 512), BF16),
            pltpu.VMEM((512, 4 * T), BF16),
            pltpu.VMEM((K, T, U), BF16),
            pltpu.VMEM((K, 4 * T, U), BF16),
            pltpu.VMEM((4, 16, T), BF16),
            pltpu.VMEM((K, 256, U), BF16),
            pltpu.VMEM((K, 256, U), BF16),
            pltpu.VMEM((K, 256), F32),
            pltpu.VMEM((K, 256), F32),
            pltpu.VMEM((16, T, U), BF16),
            pltpu.VMEM((16, T, U), BF16),
            pltpu.VMEM((2, 16, T), F32),
            pltpu.VMEM((2 * R, 128), F32),
            pltpu.VMEM((2 * R, 128), F32),
            pltpu.VMEM((2 * R, 128), F32),
            pltpu.VMEM((32, 8, T), F32),
            pltpu.VMEM((2 * K, T, U), F32),
            pltpu.VMEM((2 * R, W2), F32),
            pltpu.VMEM((T, U), BF16),
            pltpu.VMEM((K, 256), F32),
            pltpu.VMEM((K, 256, U), BF16),
            dma((3,)),
            dma((2,)),
            dma((2,)),
            dma((2,)),
            dma((3,)),
            dma,
            dma((34,)),
            dma,
            dma,
            dma,
            dma,
            dma,
            dma((24,)),
            dma,
            dma,
            dma,
            dma((2,)),
            dma((2,)),
            dma,
            dma((8,)),
            dma,
            dma((4,)),
            dma,
            dma,
            dma,
            dma((3,)),
            dma,
            dma,
        ],
        compiler_params=pltpu.CompilerParams(
            collective_id=0, has_side_effects=True, vmem_limit_bytes=67043328
        ),
    )(
        mix_weight.T,
        saved_lse.T,
        loss_scale[None, :],
        targets[None, :],
        hidden,
        proj_weight,
        out_weight,
    )
    gh, gm, gp, go = pl.pallas_call(
        place,
        out_shape=outs,
        in_specs=[hbm] * 4,
        out_specs=(hbm,) * 4,
        scratch_shapes=[pltpu.VMEM(o.shape, o.dtype) for o in outs] + [dma((7,)), dma((7,))],
    )(*found)
    return gh, gm.T, gp, go


def solution(mesh):
    finer = Mesh(mesh.devices.reshape(4, 2, 2, 4, 2), AXES)
    in_specs = (
        P(DP, None),
        P(),
        P(None, None, VOC),
        P(None, VOC),
        P(DP, None),
        P(DP),
        P(DP),
    )
    out_specs = (P(DP, VOC), P(DP, None), P(None, DP, VOC), P(DP, VOC))
    return jax.shard_map(
        shards, mesh=finer, in_specs=in_specs, out_specs=out_specs, check_vma=False
    )
```

```python
import functools

import jax
import jax.numpy as jnp
from jax import lax
from jax.experimental import pallas as pl
from jax.experimental.pallas import tpu as pltpu
from jax.sharding import Mesh
from jax.sharding import PartitionSpec as P

AXES = ("x", "zl", "zh", "y", "c")
DP = ("x", "zl")
VOC = ("zh", "y", "c")
MESH_ID = pl.DeviceIdType.MESH
F32 = jnp.float32
BF16 = jnp.bfloat16

T = 128
K = 4
R = T * K
U = 128
D = 2048
VL = 4096
VH = VL // 2
NC = 8
C = VH // NC
W2 = 2 * C


def nt(a, b):
    return lax.dot_general(a, b, (((1,), (1,)), ((), ())), preferred_element_type=F32)


def nn(a, b):
    return lax.dot_general(a, b, (((1,), (0,)), ((), ())), preferred_element_type=F32)


def kernel(
    mix_hbm,
    lse_hbm,
    scale_hbm,
    target_hbm,
    hidden_hbm,
    proj_hbm,
    w_hbm,
    gh_out,
    gm_out,
    gp_out,
    go_out,
    mix_t,
    lse_t,
    scale,
    target,
    hidden,
    proj,
    w,
    comp,
    comp_t,
    gl,
    part,
    r1x,
    rfx,
    gcb,
    rd,
    r1a,
    rfa,
    rfb,
    wt,
    hs,
    hst,
    gpx,
    gpall,
    gmla,
    prods,
    prodr,
    gms,
    gmr,
    hts,
    hrecv,
    info2,
    lsec,
    coefc,
    tgtc,
    tl,
    tacc,
    pbuf,
    gh_v,
    gm_v,
    gp_v,
    sem_w,
    sem_i,
    p_s,
    p_r,
    sem_o,
    ag_s,
    ag_r,
    hs_s,
    hs_r,
    tl_s,
    tl_r,
    x_s,
    x_r,
    zx_s,
    zx_r,
    zx_l,
    d_s,
    d_r,
    a_s,
    a_r,
    b_s,
    b_r,
    h_s,
    h_r,
    g_s,
    g_r,
    gm_s,
    gm_r,
):
    x = lax.axis_index("x")
    zl = lax.axis_index("zl")
    zh = lax.axis_index("zh")
    y = lax.axis_index("y")
    c = lax.axis_index("c")
    z = zh * 2 + zl
    v = zh * 8 + y * 2 + c
    d = x * 2 + zl

    def m4(i):
        return lax.rem(i + 4, 4)

    def dev(x_=None, z_=None, y_=None, c_=None):
        zz = z if z_ is None else z_
        return (
            x if x_ is None else x_,
            lax.rem(zz, 2),
            lax.div(zz, 2),
            y if y_ is None else y_,
            c if c_ is None else c_,
        )

    def rc(src, dst, ss, rs, to):
        return pltpu.make_async_remote_copy(
            src_ref=src, dst_ref=dst, send_sem=ss, recv_sem=rs, device_id=to, device_id_type=MESH_ID
        )

    partner_c = dev(c_=1 - c)
    partner_z = (x, 1 - zl, zh, y, c)

    hidden_copy = pltpu.make_async_copy(hidden_hbm, hidden, sem_w.at[0])
    proj_copy = pltpu.make_async_copy(proj_hbm, proj, sem_w.at[1])
    w_copy = pltpu.make_async_copy(
        w_hbm.at[:, pl.ds(pl.multiple_of(zl * VH, VH), VH)], w, sem_w.at[2]
    )
    small_copies = [
        pltpu.make_async_copy(src, dst, sem_w.at[3 + i])
        for i, (src, dst) in enumerate(
            ((mix_hbm, mix_t), (lse_hbm, lse_t), (scale_hbm, scale), (target_hbm, target))
        )
    ]
    hidden_copy.start()
    proj_copy.start()

    q32 = z * 8 + y * 2 + c

    def mate(o):
        p = lax.rem(q32 + o, 32)
        zz = lax.div(p, 8)
        return (x, lax.rem(zz, 2), lax.div(zz, 2), lax.rem(lax.div(p, 2), 4), lax.rem(p, 2))

    barrier = pltpu.get_barrier_semaphore()

    def greet(o, carry):
        pl.semaphore_signal(barrier, inc=1, device_id=mate(o), device_id_type=MESH_ID)
        return carry

    lax.fori_loop(1, 32, greet, 0)
    for o in range(1, 4):
        pl.semaphore_signal(barrier, inc=1, device_id=dev(x_=m4(x + o)), device_id_type=MESH_ID)

    own_cols = pl.multiple_of(v * U, U)

    def blk(col, z_, y_, c_, r0=0, n=2 * T):
        block = lax.rem(z_, 2) * 16 + lax.div(z_, 2) * 8 + y_ * 2 + c_
        return comp.at[block, pl.ds(col * 2 * T + r0, n)]

    def pos(col):
        return (y, z) if col == 0 else (z, y)

    def at_ab(col, a_, b_, c_, r0=0, n=2 * T):
        return blk(col, b_, a_, c_, r0, n) if col == 0 else blk(col, a_, b_, c_, r0, n)

    def dev_ab(col, a_, b_):
        return dev(y_=a_, z_=b_) if col == 0 else dev(z_=a_, y_=b_)

    def ag_copy(col, i, ref, to):
        r = 30 + i if col is None else col * 15 + i
        return rc(ref, ref, ag_s, ag_r.at[r], to)

    def ag_send(col, i, ref, to):
        ag_copy(col, i, ref, to).start()

    def ag_wait(col, i, ref):
        ag_copy(col, i, ref, partner_c).wait_recv()

    def second(col, i, ref):
        a, b = pos(col)
        ag_send(col, 3 + 3 * i, ref, dev_ab(col, a, m4(b + 1)))
        ag_send(col, 3 + 3 * i + 1, ref, dev_ab(col, a, m4(b - 1)))

    def across(i, ref):
        ag_send(None, i, ref, partner_c)

    def flip(col, a_, b_, c_):
        z_, y_ = (b_, a_) if col == 0 else (a_, b_)
        row = pl.multiple_of(lax.rem(z_, 2) * R + col * 2 * T, 2 * T)
        unit = lax.div(z_, 2) * 8 + y_ * 2 + c_
        comp_t[pl.ds(pl.multiple_of(unit * U, U), U), pl.ds(row, 2 * T)] = jnp.transpose(
            comp[lax.rem(z_, 2) * 16 + unit, pl.ds(col * 2 * T, 2 * T)]
        )

    def gauge(col, a_, b_, c_):
        z_, y_ = (b_, a_) if col == 0 else (a_, b_)
        g = lax.rem(z_, 2)
        unit = lax.div(z_, 2) * 8 + y_ * 2 + c_
        weight = wt[
            pl.ds(pl.multiple_of(g * T, T), T), pl.ds(pl.multiple_of(unit * U, U), U)
        ].astype(F32)
        for k in (2 * col, 2 * col + 1):
            tacc[g * K + k] += comp[g * 16 + unit, pl.ds(k * T, T)].astype(F32) * weight

    hidden_copy.wait()
    proj_copy.wait()
    for cp in small_copies:
        cp.start()
    w_copy.start()
    pre = jnp.tanh(nn(hidden[...], jnp.concatenate([proj[k] for k in range(K)], axis=1)))
    for k in range(K):
        comp[zl * 16 + v, pl.ds(k * T, T)] = pre[:, k * U : (k + 1) * U].astype(BF16)
    pl.semaphore_wait(barrier, 34)
    for col in range(2):
        a, b = pos(col)
        own = at_ab(col, a, b, c)
        ag_send(col, 0, own, dev_ab(col, m4(a + 1), b))
        ag_send(col, 1, own, dev_ab(col, m4(a - 1), b))

    for cp in small_copies:
        cp.wait()
    mix_logits = nt(mix_t[...], hidden[...])
    info2[zl, 0:4] = lse_t[...]
    info2[zl, 4:8] = mix_logits - jnp.log(jnp.sum(jnp.exp(mix_logits), axis=0, keepdims=True))
    info2[zl, 8:9] = scale[...]
    info2[zl, 9:10] = target[...].astype(F32)
    info2[zl, 10:16] = jnp.zeros((6, T), F32)

    def row_columns(g):
        cols = jnp.transpose(jnp.concatenate([info2[g], jnp.zeros((112, T), F32)], axis=0))
        local = cols[:, 9:10] - (v * VL + zl * VH).astype(F32)
        for k in range(K):
            rows = pl.ds(pl.multiple_of(g * R + k * T, T), T)
            lsec[rows, :] = jnp.broadcast_to(cols[:, k : k + 1], (T, 128))
            tgtc[rows, :] = jnp.broadcast_to(local, (T, 128))

    row_columns(zl)
    info_copy = rc(info2.at[zl], info2.at[zl], sem_i.at[0], sem_i.at[1], partner_z)
    info_copy.start()

    for col in range(2):
        a, b = pos(col)
        own = at_ab(col, a, b, c)
        second(col, 0, own)
        across(0, own)

    def hs_copy(i):
        p = m4(x + (0, 1, -1, 2)[i])
        return rc(
            hidden.at[:, pl.ds(pl.multiple_of(p * 512, 512), 512)], hs.at[i], hs_s, hs_r, dev(x_=p)
        )

    for i in range(1, 4):
        hs_copy(i).start()
    hs[0] = hidden[:, pl.ds(pl.multiple_of(x * 512, 512), 512)]

    def pick(n, carry):
        rows = pl.ds(pl.multiple_of(n * 512, 512), 512)
        acc = jnp.zeros((2 * T, 512), F32)
        for q in range(4):
            lane = lax.broadcasted_iota(jnp.int32, (T, 512), 1).astype(F32) + float(q * 512)
            hot = jnp.concatenate(
                [
                    (lane == tgtc[pl.ds(g * R, T), :][:, 0:1]).astype(F32).astype(BF16)
                    for g in range(2)
                ],
                axis=0,
            )
            acc = acc + nt(hot, w[rows, pl.ds(q * 512, 512)])
        wt[:, rows] = acc.astype(BF16)
        return carry

    for col in range(2):
        a, b = pos(col)
        prev, nxt = m4(a - 1), m4(a + 1)
        ag_wait(col, 0, at_ab(col, prev, b, c))
        ag_send(col, 2, at_ab(col, prev, b, c, 0, T), dev_ab(col, nxt, b))
        ag_wait(col, 1, at_ab(col, nxt, b, c))
        ag_send(col, 2, at_ab(col, nxt, b, c, T, T), dev_ab(col, prev, b))
    for i, step in ((1, -1), (2, 1)):
        for col in range(2):
            a, b = pos(col)
            second(col, i, at_ab(col, m4(a + step), b, c))
            across(i, at_ab(col, m4(a + step), b, c))

    def near(i):
        for col in range(2):
            a, b = pos(col)
            a_ = m4(a + (0, -1, 1, 2)[i])
            prev, nxt = m4(b - 1), m4(b + 1)
            ag_wait(col, 3 + 3 * i, at_ab(col, a_, prev, c))
            ag_send(col, 3 + 3 * i + 2, at_ab(col, a_, prev, c, 0, T), dev_ab(col, a, nxt))
            ag_wait(col, 3 + 3 * i + 1, at_ab(col, a_, nxt, c))
            ag_send(col, 3 + 3 * i + 2, at_ab(col, a_, nxt, c, T, T), dev_ab(col, a, prev))
            across(i, at_ab(col, a_, prev, c))
            across(i, at_ab(col, a_, nxt, c))

    def flip_near(i):
        for col in range(2):
            a, b = pos(col)
            a_ = m4(a + (0, -1, 1, 2)[i])
            for step in (0, -1, 1):
                flip(col, a_, m4(b + step), c)
                gauge(col, a_, m4(b + step), c)

    def far(i):
        for col in range(2):
            a, b = pos(col)
            a_ = m4(a + (0, -1, 1, 2)[i])
            b_ = m4(b + 2)
            ag_wait(col, 3 + 3 * i + 2, at_ab(col, a_, b_, c))
            across(i, at_ab(col, a_, b_, c))
            flip(col, a_, b_, c)
            gauge(col, a_, b_, c)

    def partner_wait(i):
        ag_wait(None, i, comp.at[pl.ds(0, 4)])

    def on_partner(i, act):
        for col in range(2):
            a, b = pos(col)
            a_ = m4(a + (0, -1, 1, 2)[i])

            def step(b_, carry):
                act(col, a_, b_, 1 - c)
                return carry

            lax.fori_loop(0, 4, step, 0)

    def both(*where):
        flip(*where)
        gauge(*where)

    tacc[...] = jnp.zeros_like(tacc)
    near(0)
    info_in = rc(info2.at[1 - zl], info2.at[1 - zl], sem_i.at[0], sem_i.at[1], partner_z)
    info_in.wait_recv()
    row_columns(1 - zl)
    w_copy.wait()
    lax.fori_loop(0, 2, pick, 0)
    for col in range(2):
        a, b = pos(col)
        two = m4(a + 2)
        ag_wait(col, 2, at_ab(col, two, b, c))
        second(col, 3, at_ab(col, two, b, c))
        across(3, at_ab(col, two, b, c))
    lax.fori_loop(2, 4, pick, 0)
    near(1)
    near(2)
    for i in range(3):
        flip_near(i)
    far(0)
    near(3)
    partner_wait(0)
    on_partner(0, both)
    far(1)
    far(2)
    flip_near(3)
    partner_wait(1)
    on_partner(1, both)
    partner_wait(2)
    on_partner(2, both)
    far(3)
    partner_wait(3)
    on_partner(3, gauge)

    lane_t = lax.broadcasted_iota(jnp.int32, (T, 128), 1)
    acc = jnp.zeros((T, 128), F32)
    for g in range(2):
        for k in range(K):
            acc = jnp.where(lane_t == g * K + k, jnp.sum(tacc[g * K + k], axis=1, keepdims=True), acc)
    tl[0] = jnp.transpose(acc)[0:8]

    def tl_copy(o):
        return rc(tl.at[0], tl.at[o], tl_s, tl_r, mate(o))

    def tl_start(o, carry):
        tl_copy(o).start()
        return carry

    lax.fori_loop(1, 32, tl_start, 0)

    lane_w = lax.broadcasted_iota(jnp.int32, (2 * T, 128), 1).astype(F32)

    def block_logits(p, m, put):
        rows = pl.ds(pl.multiple_of(m * 2 * T, 2 * T), 2 * T)
        g, part_rows = lax.div(m, 2), pl.ds(pl.multiple_of(lax.rem(m, 2) * 2 * T, 2 * T), 2 * T)
        vectors = jnp.concatenate([comp[g * 16 + u, part_rows] for u in range(16)], axis=1)
        logit = nn(vectors, w[:, pl.ds(pl.multiple_of(p * W2, W2), W2)])
        shift = jnp.asarray(p * W2, F32)
        lse_m, tgt_m = lsec[rows, :], tgtc[rows, :] - shift
        for e in range(W2 // 128):
            prob = jnp.exp(logit[:, e * 128 : (e + 1) * 128] - lse_m)
            hot = jnp.where(lane_w + float(e * 128) == tgt_m, 1.0, 0.0)
            put(rows, e, prob - hot)

    def hold(m, carry):
        def put(rows, e, val):
            pbuf[rows, pl.ds(e * 128, 128)] = val

        block_logits(0, m, put)
        return carry

    lax.fori_loop(0, 4, hold, 0)
    on_partner(3, flip)

    tl_all = rc(tl.at[pl.ds(1, 31)], tl.at[pl.ds(1, 31)], tl_s, tl_r, partner_c)
    tl_all.wait_recv()
    target_logit = jnp.sum(tl[...], axis=0)
    coef_rows = []
    gml_rows = []
    for g in range(2):
        lse_g = info2[g, 0:4]
        lm_g = info2[g, 4:8]
        scale_g = info2[g, 8:9]
        weights = jnp.exp(lm_g + target_logit[g * K : (g + 1) * K] - lse_g)
        resp = weights / jnp.sum(weights, axis=0, keepdims=True)
        coef_rows.append(scale_g * resp)
        gml_rows.append(-scale_g * (resp - jnp.exp(lm_g)))
    table = jnp.concatenate(coef_rows + [jnp.zeros((120, 128), F32)], axis=0)
    cols = jnp.transpose(table)
    for g in range(2):
        for k in range(K):
            coefc[pl.ds(g * R + k * T, T), :] = jnp.broadcast_to(
                cols[:, g * K + k : g * K + k + 1], (T, 128)
            )
    mine = jnp.where(zl == 0, gml_rows[0], gml_rows[1])
    high = mine.astype(BF16).astype(F32)
    gmla[0] = jnp.concatenate([high, mine - high, jnp.zeros((8, T), F32)], axis=0).astype(BF16)
    for i in range(1, 4):
        rc(gmla.at[0], gmla.at[i], gm_s, gm_r, dev(x_=m4(x + (0, 1, -1, 2)[i]))).start()

    def ring(piece, me, right, left, r1, rf, ss, r1_sem, rf_sem, r1_all, rf_all):
        two, one, back = m4(me + 2), m4(me + 1), m4(me - 1)
        copies = (
            lambda: rc(piece(two, 0), r1(0), ss, r1_sem, right),
            lambda: rc(piece(one, 1), rf(0, 1), ss, rf_sem, right),
            lambda: rc(piece(two, 1), r1(1), ss, r1_sem, left),
            lambda: rc(piece(back, 0), rf(1, 0), ss, rf_sem, left),
            lambda: rc(piece(one, 0), rf(0, 0), ss, rf_sem, right),
            lambda: rc(piece(back, 1), rf(1, 1), ss, rf_sem, left),
        )

        def first(which=(0, 2, 1, 3)):
            for i in which:
                copies[i]().start()

        def add(ref, other):
            ref[...] = (ref[...].astype(F32) + other[...].astype(F32)).astype(BF16)

        def forward():
            rc(r1_all, r1_all, ss, r1_sem, right).wait_recv()
            add(piece(one, 0), r1(0))
            copies[4]().start()
            add(piece(back, 1), r1(1))
            copies[5]().start()

        def arrive():
            rc(rf_all, rf_all, ss, rf_sem, right).wait_recv()

        return first, forward, arrive

    x_right, x_left = dev(x_=m4(x + 1)), dev(x_=m4(x - 1))

    def x_ring(cc, e=None):
        lanes = pl.ds(0, C) if e is None else pl.ds(e * 128, 128)
        sem = 2 * cc if e is None else 2 * NC + 2 * (2 * (cc - 6) + e)
        return ring(
            lambda t, h: part.at[cc, t * 2 + h, :, lanes],
            x,
            x_right,
            x_left,
            lambda i: r1x.at[cc, i, :, lanes],
            lambda i, h: rfx.at[cc, i, h, :, lanes],
            x_s,
            x_r.at[sem],
            x_r.at[sem + 1],
            r1x.at[cc, :, :, lanes],
            rfx.at[cc, :, :, :, lanes],
        )

    def grad_out(p, tiles, send=True):
        cols = pl.ds(p * W2, W2)
        order = ((2, 0), (2, 1), (1, 1), (-1, 0), (1, 0), (-1, 1), (0, 0), (0, 1))
        for i in tiles:
            step, h = order[i]
            t = m4(x + step)
            rows = pl.ds(pl.multiple_of(t * 512 + h * 256, 256), 256)
            res = nn(comp_t[rows, :], gl[:, cols]).astype(BF16)
            for e in range(2):
                part[2 * p + e, t * 2 + h] = res[:, e * C : (e + 1) * C]
            if send and i < 4:
                for e in range(2):
                    x_ring(2 * p + e)[0](((0, 2, 1, 3)[i],))

    def scale_first(m, carry):
        rows = pl.ds(pl.multiple_of(m * 2 * T, 2 * T), 2 * T)
        coef_m = coefc[rows, :]
        for e in range(W2 // 128):
            gl[rows, pl.ds(e * 128, 128)] = (coef_m * pbuf[rows, pl.ds(e * 128, 128)]).astype(BF16)
        return carry

    lax.fori_loop(0, 4, scale_first, 0)

    def grad_logits(p):
        def rows_of(m, carry):
            coef_m = coefc[pl.ds(pl.multiple_of(m * 2 * T, 2 * T), 2 * T), :]

            def put(rows, e, val):
                gl[rows, pl.ds(pl.multiple_of(p * W2 + e * 128, 128), 128)] = (coef_m * val).astype(
                    BF16
                )

            block_logits(p, m, put)
            return carry

        lax.fori_loop(0, 4, rows_of, 0)

    def comp_grad(bat):
        def tile(i, carry):
            g, h, j = lax.div(i, 4), lax.rem(lax.div(i, 2), 2), lax.rem(i, 2)
            rows = pl.ds(pl.multiple_of(g * R + bat * 2 * T, 2 * T), 2 * T)
            units = pl.ds(pl.multiple_of((h * 2 + j) * 512, 512), 512)
            res = nt(gl[rows, :], w[units, :])
            z_ = h * 2 + g
            for jj in range(4):
                y_ = j * 2 + jj // 2
                val = res[:, jj * 128 : (jj + 1) * 128].astype(BF16)
                gcb[jj % 2, 2 * bat, z_, y_] = val[0:T]
                gcb[jj % 2, 2 * bat + 1, y_, z_] = val[T : 2 * T]
            return carry

        lax.fori_loop(0, 8, tile, 0)
        two = pl.ds(2 * bat, 2)
        swap = rc(gcb.at[1 - c, two], rd.at[two], d_s.at[bat], d_r.at[bat], partner_c)
        swap.start()
        return swap

    def a_ring(k):
        me = z if k % 2 == 0 else y
        mk = (lambda p: dev(z_=p)) if k % 2 == 0 else (lambda p: dev(y_=p))
        return ring(
            lambda t, h: gcb.at[c, k, t, pl.ds(2 * h, 2)],
            me,
            mk(m4(me + 1)),
            mk(m4(me - 1)),
            lambda i: r1a.at[k, i],
            lambda i, h: rfa.at[k, i, h],
            a_s,
            a_r.at[2 * k],
            a_r.at[2 * k + 1],
            r1a.at[k],
            rfa.at[k],
        )

    def b_copies(k):
        first, me = (z, y) if k % 2 == 0 else (y, z)
        mk = (lambda p: dev(y_=p)) if k % 2 == 0 else (lambda p: dev(z_=p))
        return [
            rc(gcb.at[c, k, first, t], rfb.at[k, o - 1], b_s, b_r.at[k], mk(t))
            for o in range(1, 4)
            for t in [m4(me + o)]
        ]

    def merge(bat, swap):
        swap.wait_recv()

        def add(i, carry):
            p, q = lax.div(i, 4), lax.rem(i, 4)
            for k in (2 * bat, 2 * bat + 1):
                gcb[c, k, p, q] = (
                    gcb[c, k, p, q].astype(F32) + rd[k, p, q].astype(F32)
                ).astype(BF16)
            return carry

        lax.fori_loop(0, 16, add, 0)
        for k in (2 * bat, 2 * bat + 1):
            a_ring(k)[0]()

    def forward_a(bat):
        for k in (2 * bat, 2 * bat + 1):
            a_ring(k)[1]()

    def finish_a(bat):
        for k in (2 * bat, 2 * bat + 1):
            a_ring(k)[2]()
            me = z if k % 2 == 0 else y
            for h in range(2):
                for e in range(2):
                    q = 2 * h + e
                    gcb[c, k, me, q] = (
                        gcb[c, k, me, q].astype(F32)
                        + rfa[k, 0, h, e].astype(F32)
                        + rfa[k, 1, h, e].astype(F32)
                    ).astype(BF16)
            for cp in b_copies(k):
                cp.start()

    def finish_b(bat):
        for k in (2 * bat, 2 * bat + 1):
            rc(rfb.at[k], rfb.at[k], b_s, b_r.at[k], partner_c).wait_recv()
            first, me = (z, y) if k % 2 == 0 else (y, z)
            total = gcb[c, k, first, me].astype(F32)
            for o in range(3):
                total = total + rfb[k, o].astype(F32)
            cf = comp[zl * 16 + v, pl.ds(k * T, T)].astype(F32)
            gpx[k] = (total * (1.0 - cf * cf)).astype(BF16)

    def x_finish(cc, e=None):
        lanes = pl.ds(0, C) if e is None else pl.ds(e * 128, 128)
        x_ring(cc, e)[2]()
        for h in range(2):
            part[cc, x * 2 + h, :, lanes] = (
                part[cc, x * 2 + h, :, lanes].astype(F32)
                + rfx[cc, 0, h, :, lanes].astype(F32)
                + rfx[cc, 1, h, :, lanes].astype(F32)
            ).astype(BF16)
        if e is None:
            cols = pl.ds(pl.multiple_of(zl * VH + cc * C, C), C)
        else:
            cols = pl.ds(pl.multiple_of(zl * VH + cc * C + e * 128, 128), 128)
        dst = go_out.at[:, cols]
        rc(part.at[cc, x * 2 + 1 - zl, :, lanes], dst, zx_s, zx_r, partner_z).start()
        pltpu.make_async_copy(part.at[cc, x * 2 + zl, :, lanes], dst, zx_l).start()

    first_half, second_half, every = range(4), range(4, 8), range(8)
    grad_out(0, every)
    grad_logits(1)
    grad_out(1, every)
    x_ring(0)[1]()
    grad_logits(2)
    grad_logits(3)
    x_ring(1)[1]()
    swap0 = comp_grad(0)
    x_ring(2)[1]()
    grad_out(2, first_half)
    merge(0, swap0)
    swap1 = comp_grad(1)
    forward_a(0)
    x_ring(3)[1]()
    grad_out(2, second_half)
    merge(1, swap1)
    finish_a(0)
    hs_all = rc(hs.at[pl.ds(1, 3)], hs.at[pl.ds(1, 3)], hs_s, hs_r, partner_c)
    hs_all.wait_recv()
    for i in range(4):
        hst[:, pl.ds(i * T, T)] = jnp.transpose(hs[i])
    grad_out(3, first_half, False)
    forward_a(1)
    grad_out(3, second_half, False)
    x_ring(4)[1]()
    finish_b(0)
    finish_a(1)
    x_finish(0)
    x_finish(1)
    x_finish(2)
    finish_b(1)

    def slot(i, r0=0, n=T):
        return gpall.at[:, pl.ds(i * T + r0, n)]

    g_copies = (
        rc(gpx, slot(1), g_s, g_r.at[0], x_right),
        rc(gpx, slot(2), g_s, g_r.at[1], x_left),
        rc(slot(1, 0, T // 2), slot(3, 0, T // 2), g_s, g_r.at[2], x_right),
        rc(slot(2, T // 2, T // 2), slot(3, T // 2, T // 2), g_s, g_r.at[2], x_left),
    )
    g_copies[0].start()
    g_copies[1].start()
    x_ring(6, 0)[0]()

    def h_copy(o):
        p = lax.rem(v + o, 16)
        to = (x, zl, lax.div(p, 8), lax.rem(lax.div(p, 2), 4), lax.rem(p, 2))
        return rc(hts.at[o], hrecv.at[o], h_s, h_r, to)

    def h_tile(o):
        p = lax.rem(v + o, 16)
        rows = pl.ds(pl.multiple_of(p * U, U), U)
        acc = nt(gpx[0], proj[0, rows, :])
        for k in range(1, K):
            acc = acc + nt(gpx[k], proj[k, rows, :])
        return acc

    def h_step(o, carry):
        hts[o] = h_tile(o).astype(BF16)
        h_copy(o).start()
        return carry

    lax.fori_loop(1, 9, h_step, 0)
    x_ring(6, 1)[0]()
    lax.fori_loop(9, 16, h_step, 0)
    hrecv[0] = h_tile(0).astype(BF16)
    gpall[:, pl.ds(0, T)] = gpx[...]
    x_finish(3)
    x_finish(4)
    g_copies[0].wait_recv()
    g_copies[2].start()
    g_copies[1].wait_recv()
    g_copies[3].start()
    x_ring(5)[1]()
    x_ring(7, 0)[0]()

    rc(slot(3), slot(3), g_s, g_r.at[2], x_right).wait_recv()
    x_ring(7, 1)[0]()

    def product(half, k):
        return nn(hst[pl.ds(pl.multiple_of(half * 256, 256), 256), :], gpall[k])

    def mix_product(half):
        rows = pl.ds(pl.multiple_of(half * 256, 256), 256)
        res = nt(gmla[0], hst[rows, pl.ds(0, T)])
        for i in range(1, 4):
            res = res + nt(gmla[i], hst[rows, pl.ds(i * T, T)])
        return res[0:4] + res[4:8]

    for k in range(K):
        prods[k] = product(1 - zl, k).astype(BF16)
    gm_all = rc(gmla.at[pl.ds(1, 3)], gmla.at[pl.ds(1, 3)], gm_s, gm_r, partner_c)
    gm_all.wait_recv()
    gms[...] = mix_product(1 - zl)
    p_copies = (
        rc(prods, prodr, p_s.at[0], p_r.at[0], partner_z),
        rc(gms, gmr, p_s.at[1], p_r.at[1], partner_z),
    )
    for cp in p_copies:
        cp.start()
    x_ring(6, 0)[1]()
    x_ring(6, 1)[1]()
    x_finish(5)
    x_ring(7, 0)[1]()
    x_ring(7, 1)[1]()
    x_finish(6, 0)
    x_finish(6, 1)
    x_finish(7, 0)
    h_all = rc(hts.at[pl.ds(1, 15)], hrecv.at[pl.ds(1, 15)], h_s, h_r, partner_c)
    h_all.wait_recv()
    mw = jnp.concatenate(
        [mix_t[:, pl.ds(own_cols, U)].astype(F32)] * 2 + [jnp.zeros((8, U), F32)], axis=0
    ).astype(BF16)
    gh = lax.dot_general(gmla[0], mw, (((0,), (0,)), ((), ())), preferred_element_type=F32)
    for o in range(16):
        gh = gh + hrecv[o].astype(F32)
    gh_v[...] = gh.astype(BF16)
    out_copies = (
        pltpu.make_async_copy(gh_v, gh_out, sem_o.at[0]),
        pltpu.make_async_copy(gp_v, gp_out, sem_o.at[1]),
        pltpu.make_async_copy(gm_v, gm_out, sem_o.at[2]),
    )
    out_copies[0].start()
    x_finish(7, 1)
    for cp in p_copies:
        cp.wait_recv()
    for k in range(K):
        gp_v[k] = (product(zl, k) + prodr[k].astype(F32)).astype(BF16)
    gm_v[...] = mix_product(zl) + gmr[...]
    out_copies[1].start()
    out_copies[2].start()

    for cp in (info_copy, swap0, swap1, *p_copies, tl_all, hs_all, h_all, gm_all):
        cp.wait_send()
    for ref, sem in (
        (comp.at[pl.ds(0, 31)], ag_s),
        (part.at[pl.ds(0, 6)], x_s),
        (part.at[0], zx_s),
        (gcb.at[0, pl.ds(0, 3)], a_s),
        (gcb.at[0, 0, pl.ds(0, 3)], b_s),
        (gpall.at[:, pl.ds(0, 3 * T)], g_s),
    ):
        rc(ref, ref, sem, zx_r, partner_z).wait_send()
    half_out = go_out.at[:, pl.ds(0, VH)]
    rc(half_out, half_out, zx_s, zx_r, partner_z).wait_recv()
    pltpu.make_async_copy(part.at[0], part.at[0], zx_l).wait()
    for cp in out_copies:
        cp.wait()


def place(gh, gm, gp, go, gh_o, gm_o, gp_o, go_o, b_gh, b_gm, b_gp, b_go, s_in, s_out):
    pairs = [(gh, b_gh, gh_o), (gm, b_gm, gm_o), (gp, b_gp, gp_o)]
    for i in range(8):
        rows = pl.ds(i * 32, 32)
        pairs.append((go.at[rows], b_go.at[rows], go_o.at[rows]))
    loads = [pltpu.make_async_copy(s, b, s_in.at[i]) for i, (s, b, _) in enumerate(pairs)]
    stores = [pltpu.make_async_copy(b, t, s_out.at[i]) for i, (_, b, t) in enumerate(pairs)]
    for cp in reversed(loads):
        cp.start()
    for i in reversed(range(len(pairs))):
        loads[i].wait()
        stores[i].start()
    for cp in stores:
        cp.wait()


def shards(hidden, mix_weight, proj_weight, out_weight, saved_lse, targets, loss_scale):
    hbm = pl.BlockSpec(memory_space=pltpu.HBM)
    dma = pltpu.SemaphoreType.DMA
    outs = (
        jax.ShapeDtypeStruct((T, U), BF16),
        jax.ShapeDtypeStruct((K, 256), F32),
        jax.ShapeDtypeStruct((K, 256, U), BF16),
        jax.ShapeDtypeStruct((256, VL), BF16),
    )
    found = pl.pallas_call(
        kernel,
        out_shape=outs,
        in_specs=[hbm] * 7,
        out_specs=(hbm, hbm, hbm, hbm),
        scratch_shapes=[
            pltpu.VMEM((K, D), BF16),
            pltpu.VMEM((K, T), F32),
            pltpu.VMEM((1, T), F32),
            pltpu.VMEM((1, T), jnp.int32),
            pltpu.VMEM((T, D), BF16),
            pltpu.VMEM((K, D, U), BF16),
            pltpu.VMEM((D, VH), BF16),
            pltpu.VMEM((32, R, U), BF16),
            pltpu.VMEM((D, 2 * R), BF16),
            pltpu.VMEM((2 * R, VH), BF16),
            pltpu.VMEM((NC, 8, 256, C), BF16),
            pltpu.VMEM((NC, 2, 256, C), BF16),
            pltpu.VMEM((NC, 2, 2, 256, C), BF16),
            pltpu.VMEM((2, 4, 4, 4, T, U), BF16),
            pltpu.VMEM((4, 4, 4, T, U), BF16),
            pltpu.VMEM((4, 2, 2, T, U), BF16),
            pltpu.VMEM((4, 2, 2, 2, T, U), BF16),
            pltpu.VMEM((4, 3, T, U), BF16),
            pltpu.VMEM((2 * T, D), BF16),
            pltpu.VMEM((4, T, 512), BF16),
            pltpu.VMEM((512, 4 * T), BF16),
            pltpu.VMEM((K, T, U), BF16),
            pltpu.VMEM((K, 4 * T, U), BF16),
            pltpu.VMEM((4, 16, T), BF16),
            pltpu.VMEM((K, 256, U), BF16),
            pltpu.VMEM((K, 256, U), BF16),
            pltpu.VMEM((K, 256), F32),
            pltpu.VMEM((K, 256), F32),
            pltpu.VMEM((16, T, U), BF16),
            pltpu.VMEM((16, T, U), BF16),
            pltpu.VMEM((2, 16, T), F32),
            pltpu.VMEM((2 * R, 128), F32),
            pltpu.VMEM((2 * R, 128), F32),
            pltpu.VMEM((2 * R, 128), F32),
            pltpu.VMEM((32, 8, T), F32),
            pltpu.VMEM((2 * K, T, U), F32),
            pltpu.VMEM((2 * R, W2), F32),
            pltpu.VMEM((T, U), BF16),
            pltpu.VMEM((K, 256), F32),
            pltpu.VMEM((K, 256, U), BF16),
            dma((7,)),
            dma((2,)),
            dma((2,)),
            dma((2,)),
            dma((3,)),
            dma,
            dma((34,)),
            dma,
            dma,
            dma,
            dma,
            dma,
            dma((24,)),
            dma,
            dma,
            dma,
            dma((2,)),
            dma((2,)),
            dma,
            dma((8,)),
            dma,
            dma((4,)),
            dma,
            dma,
            dma,
            dma((3,)),
            dma,
            dma,
        ],
        compiler_params=pltpu.CompilerParams(
            collective_id=0, has_side_effects=True, vmem_limit_bytes=67043328
        ),
    )(
        mix_weight.T,
        saved_lse.T,
        loss_scale[None, :],
        targets[None, :],
        hidden,
        proj_weight,
        out_weight,
    )
    gh, gm, gp, go = pl.pallas_call(
        place,
        out_shape=outs,
        in_specs=[hbm] * 4,
        out_specs=(hbm,) * 4,
        scratch_shapes=[pltpu.VMEM(o.shape, o.dtype) for o in outs] + [dma((11,)), dma((11,))],
    )(*found)
    return gh, gm.T, gp, go


def solution(mesh):
    finer = Mesh(mesh.devices.reshape(4, 2, 2, 4, 2), AXES)
    in_specs = (
        P(DP, None),
        P(),
        P(None, None, VOC),
        P(None, VOC),
        P(DP, None),
        P(DP),
        P(DP),
    )
    out_specs = (P(DP, VOC), P(DP, None), P(None, DP, VOC), P(DP, VOC))
    return jax.shard_map(
        shards, mesh=finer, in_specs=in_specs, out_specs=out_specs, check_vma=False
    )
```

```python
import functools

import jax
import jax.numpy as jnp
from jax import lax
from jax.experimental import pallas as pl
from jax.experimental.pallas import tpu as pltpu
from jax.sharding import Mesh
from jax.sharding import PartitionSpec as P

AXES = ("x", "zl", "zh", "y", "c")
DP = ("x", "zl")
VOC = ("zh", "y", "c")
MESH_ID = pl.DeviceIdType.MESH
F32 = jnp.float32
BF16 = jnp.bfloat16

T = 128
K = 4
R = T * K
U = 128
D = 2048
VL = 4096
VH = VL // 2
NC = 8
C = VH // NC
W2 = 2 * C


def nt(a, b):
    return lax.dot_general(a, b, (((1,), (1,)), ((), ())), preferred_element_type=F32)


def nn(a, b):
    return lax.dot_general(a, b, (((1,), (0,)), ((), ())), preferred_element_type=F32)


def kernel(
    mix_hbm,
    lse_hbm,
    scale_hbm,
    target_hbm,
    hidden_hbm,
    proj_hbm,
    w_hbm,
    gh_out,
    gm_out,
    gp_out,
    go_out,
    mix_t,
    lse_t,
    scale,
    target,
    hidden,
    proj,
    w,
    comp,
    comp_t,
    gl,
    part,
    r1x,
    rfx,
    gcb,
    rd,
    r1a,
    rfa,
    rfb,
    wt,
    hs,
    hst,
    gpx,
    gpall,
    gmla,
    prods,
    prodr,
    gms,
    gmr,
    hts,
    hrecv,
    info2,
    lsec,
    coefc,
    tgtc,
    tl,
    tacc,
    pbuf,
    gh_v,
    gm_v,
    gp_v,
    sem_w,
    sem_i,
    p_s,
    p_r,
    sem_o,
    ag_s,
    ag_r,
    hs_s,
    hs_r,
    tl_s,
    tl_r,
    x_s,
    x_r,
    x_h,
    zx_s,
    zx_r,
    zx_l,
    d_s,
    d_r,
    a_s,
    a_r,
    b_s,
    b_r,
    h_s,
    h_r,
    g_s,
    g_r,
    gm_s,
    gm_r,
):
    x = lax.axis_index("x")
    zl = lax.axis_index("zl")
    zh = lax.axis_index("zh")
    y = lax.axis_index("y")
    c = lax.axis_index("c")
    z = zh * 2 + zl
    v = zh * 8 + y * 2 + c
    d = x * 2 + zl

    def m4(i):
        return lax.rem(i + 4, 4)

    def dev(x_=None, z_=None, y_=None, c_=None):
        zz = z if z_ is None else z_
        return (
            x if x_ is None else x_,
            lax.rem(zz, 2),
            lax.div(zz, 2),
            y if y_ is None else y_,
            c if c_ is None else c_,
        )

    def rc(src, dst, ss, rs, to):
        return pltpu.make_async_remote_copy(
            src_ref=src, dst_ref=dst, send_sem=ss, recv_sem=rs, device_id=to, device_id_type=MESH_ID
        )

    partner_c = dev(c_=1 - c)
    partner_z = (x, 1 - zl, zh, y, c)

    hidden_copy = pltpu.make_async_copy(hidden_hbm, hidden, sem_w.at[0])
    proj_copy = pltpu.make_async_copy(proj_hbm, proj, sem_w.at[1])
    w_copy = pltpu.make_async_copy(
        w_hbm.at[:, pl.ds(pl.multiple_of(zl * VH, VH), VH)], w, sem_w.at[2]
    )
    small_copies = [
        pltpu.make_async_copy(src, dst, sem_w.at[3 + i])
        for i, (src, dst) in enumerate(
            ((mix_hbm, mix_t), (lse_hbm, lse_t), (scale_hbm, scale), (target_hbm, target))
        )
    ]
    hidden_copy.start()
    proj_copy.start()

    q32 = z * 8 + y * 2 + c

    def mate(o):
        p = lax.rem(q32 + o, 32)
        zz = lax.div(p, 8)
        return (x, lax.rem(zz, 2), lax.div(zz, 2), lax.rem(lax.div(p, 2), 4), lax.rem(p, 2))

    barrier = pltpu.get_barrier_semaphore()

    def greet(o, carry):
        pl.semaphore_signal(barrier, inc=1, device_id=mate(o), device_id_type=MESH_ID)
        return carry

    lax.fori_loop(1, 32, greet, 0)
    for o in range(1, 4):
        pl.semaphore_signal(barrier, inc=1, device_id=dev(x_=m4(x + o)), device_id_type=MESH_ID)

    own_cols = pl.multiple_of(v * U, U)

    def blk(col, z_, y_, c_, r0=0, n=2 * T):
        block = lax.rem(z_, 2) * 16 + lax.div(z_, 2) * 8 + y_ * 2 + c_
        return comp.at[block, pl.ds(col * 2 * T + r0, n)]

    def pos(col):
        return (y, z) if col == 0 else (z, y)

    def at_ab(col, a_, b_, c_, r0=0, n=2 * T):
        return blk(col, b_, a_, c_, r0, n) if col == 0 else blk(col, a_, b_, c_, r0, n)

    def dev_ab(col, a_, b_):
        return dev(y_=a_, z_=b_) if col == 0 else dev(z_=a_, y_=b_)

    def ag_copy(col, i, ref, to):
        r = 30 + i if col is None else col * 15 + i
        return rc(ref, ref, ag_s, ag_r.at[r], to)

    def ag_send(col, i, ref, to):
        ag_copy(col, i, ref, to).start()

    def ag_wait(col, i, ref):
        ag_copy(col, i, ref, partner_c).wait_recv()

    def second(col, i, ref):
        a, b = pos(col)
        ag_send(col, 3 + 3 * i, ref, dev_ab(col, a, m4(b + 1)))
        ag_send(col, 3 + 3 * i + 1, ref, dev_ab(col, a, m4(b - 1)))

    def across(i, ref):
        ag_send(None, i, ref, partner_c)

    def flip(col, a_, b_, c_):
        z_, y_ = (b_, a_) if col == 0 else (a_, b_)
        row = pl.multiple_of(lax.rem(z_, 2) * R + col * 2 * T, 2 * T)
        unit = lax.div(z_, 2) * 8 + y_ * 2 + c_
        comp_t[pl.ds(pl.multiple_of(unit * U, U), U), pl.ds(row, 2 * T)] = jnp.transpose(
            comp[lax.rem(z_, 2) * 16 + unit, pl.ds(col * 2 * T, 2 * T)]
        )

    def gauge(col, a_, b_, c_):
        z_, y_ = (b_, a_) if col == 0 else (a_, b_)
        g = lax.rem(z_, 2)
        unit = lax.div(z_, 2) * 8 + y_ * 2 + c_
        weight = wt[
            pl.ds(pl.multiple_of(g * T, T), T), pl.ds(pl.multiple_of(unit * U, U), U)
        ].astype(F32)
        for k in (2 * col, 2 * col + 1):
            tacc[g * K + k] += comp[g * 16 + unit, pl.ds(k * T, T)].astype(F32) * weight

    hidden_copy.wait()
    proj_copy.wait()
    for cp in small_copies:
        cp.start()
    w_copy.start()
    pre = jnp.tanh(nn(hidden[...], jnp.concatenate([proj[k] for k in range(K)], axis=1)))
    for k in range(K):
        comp[zl * 16 + v, pl.ds(k * T, T)] = pre[:, k * U : (k + 1) * U].astype(BF16)
    pl.semaphore_wait(barrier, 34)
    for col in range(2):
        a, b = pos(col)
        own = at_ab(col, a, b, c)
        ag_send(col, 0, own, dev_ab(col, m4(a + 1), b))
        ag_send(col, 1, own, dev_ab(col, m4(a - 1), b))

    for cp in small_copies:
        cp.wait()
    mix_logits = nt(mix_t[...], hidden[...])
    info2[zl, 0:4] = lse_t[...]
    info2[zl, 4:8] = mix_logits - jnp.log(jnp.sum(jnp.exp(mix_logits), axis=0, keepdims=True))
    info2[zl, 8:9] = scale[...]
    info2[zl, 9:10] = target[...].astype(F32)
    info2[zl, 10:16] = jnp.zeros((6, T), F32)

    def row_columns(g):
        cols = jnp.transpose(jnp.concatenate([info2[g], jnp.zeros((112, T), F32)], axis=0))
        local = cols[:, 9:10] - (v * VL + zl * VH).astype(F32)
        for k in range(K):
            rows = pl.ds(pl.multiple_of(g * R + k * T, T), T)
            lsec[rows, :] = jnp.broadcast_to(cols[:, k : k + 1], (T, 128))
            tgtc[rows, :] = jnp.broadcast_to(local, (T, 128))

    row_columns(zl)
    info_copy = rc(info2.at[zl], info2.at[zl], sem_i.at[0], sem_i.at[1], partner_z)
    info_copy.start()

    for col in range(2):
        a, b = pos(col)
        own = at_ab(col, a, b, c)
        second(col, 0, own)
        across(0, own)

    def hs_copy(i):
        p = m4(x + (0, 1, -1, 2)[i])
        return rc(
            hidden.at[:, pl.ds(pl.multiple_of(p * 512, 512), 512)], hs.at[i], hs_s, hs_r, dev(x_=p)
        )

    for i in range(1, 4):
        hs_copy(i).start()
    hs[0] = hidden[:, pl.ds(pl.multiple_of(x * 512, 512), 512)]

    def pick(n, carry):
        rows = pl.ds(pl.multiple_of(n * 512, 512), 512)
        acc = jnp.zeros((2 * T, 512), F32)
        for q in range(4):
            lane = lax.broadcasted_iota(jnp.int32, (T, 512), 1).astype(F32) + float(q * 512)
            hot = jnp.concatenate(
                [
                    (lane == tgtc[pl.ds(g * R, T), :][:, 0:1]).astype(F32).astype(BF16)
                    for g in range(2)
                ],
                axis=0,
            )
            acc = acc + nt(hot, w[rows, pl.ds(q * 512, 512)])
        wt[:, rows] = acc.astype(BF16)
        return carry

    for col in range(2):
        a, b = pos(col)
        prev, nxt = m4(a - 1), m4(a + 1)
        ag_wait(col, 0, at_ab(col, prev, b, c))
        ag_send(col, 2, at_ab(col, prev, b, c, 0, T), dev_ab(col, nxt, b))
        ag_wait(col, 1, at_ab(col, nxt, b, c))
        ag_send(col, 2, at_ab(col, nxt, b, c, T, T), dev_ab(col, prev, b))
    for i, step in ((1, -1), (2, 1)):
        for col in range(2):
            a, b = pos(col)
            second(col, i, at_ab(col, m4(a + step), b, c))
            across(i, at_ab(col, m4(a + step), b, c))

    def near(i):
        for col in range(2):
            a, b = pos(col)
            a_ = m4(a + (0, -1, 1, 2)[i])
            prev, nxt = m4(b - 1), m4(b + 1)
            ag_wait(col, 3 + 3 * i, at_ab(col, a_, prev, c))
            ag_send(col, 3 + 3 * i + 2, at_ab(col, a_, prev, c, 0, T), dev_ab(col, a, nxt))
            ag_wait(col, 3 + 3 * i + 1, at_ab(col, a_, nxt, c))
            ag_send(col, 3 + 3 * i + 2, at_ab(col, a_, nxt, c, T, T), dev_ab(col, a, prev))
            across(i, at_ab(col, a_, prev, c))
            across(i, at_ab(col, a_, nxt, c))

    def flip_near(i):
        for col in range(2):
            a, b = pos(col)
            a_ = m4(a + (0, -1, 1, 2)[i])
            for step in (0, -1, 1):
                flip(col, a_, m4(b + step), c)
                gauge(col, a_, m4(b + step), c)

    def far(i):
        for col in range(2):
            a, b = pos(col)
            a_ = m4(a + (0, -1, 1, 2)[i])
            b_ = m4(b + 2)
            ag_wait(col, 3 + 3 * i + 2, at_ab(col, a_, b_, c))
            across(i, at_ab(col, a_, b_, c))
            flip(col, a_, b_, c)
            gauge(col, a_, b_, c)

    def partner_wait(i):
        ag_wait(None, i, comp.at[pl.ds(0, 4)])

    def on_partner(i, act):
        for col in range(2):
            a, b = pos(col)
            a_ = m4(a + (0, -1, 1, 2)[i])

            def step(b_, carry):
                act(col, a_, b_, 1 - c)
                return carry

            lax.fori_loop(0, 4, step, 0)

    def both(*where):
        flip(*where)
        gauge(*where)

    tacc[...] = jnp.zeros_like(tacc)
    near(0)
    info_in = rc(info2.at[1 - zl], info2.at[1 - zl], sem_i.at[0], sem_i.at[1], partner_z)
    info_in.wait_recv()
    row_columns(1 - zl)
    w_copy.wait()
    lax.fori_loop(0, 2, pick, 0)
    for col in range(2):
        a, b = pos(col)
        two = m4(a + 2)
        ag_wait(col, 2, at_ab(col, two, b, c))
        second(col, 3, at_ab(col, two, b, c))
        across(3, at_ab(col, two, b, c))
    lax.fori_loop(2, 4, pick, 0)
    near(1)
    near(2)
    for i in range(3):
        flip_near(i)
    far(0)
    near(3)
    partner_wait(0)
    on_partner(0, both)
    far(1)
    far(2)
    flip_near(3)
    partner_wait(1)
    on_partner(1, both)
    partner_wait(2)
    on_partner(2, both)
    far(3)
    partner_wait(3)
    on_partner(3, gauge)

    lane_t = lax.broadcasted_iota(jnp.int32, (T, 128), 1)
    acc = jnp.zeros((T, 128), F32)
    for g in range(2):
        for k in range(K):
            acc = jnp.where(lane_t == g * K + k, jnp.sum(tacc[g * K + k], axis=1, keepdims=True), acc)
    tl[0] = jnp.transpose(acc)[0:8]

    def tl_copy(o):
        return rc(tl.at[0], tl.at[o], tl_s, tl_r, mate(o))

    def tl_start(o, carry):
        tl_copy(o).start()
        return carry

    lax.fori_loop(1, 32, tl_start, 0)

    lane_w = lax.broadcasted_iota(jnp.int32, (2 * T, 128), 1).astype(F32)

    def block_logits(p, m, put):
        rows = pl.ds(pl.multiple_of(m * 2 * T, 2 * T), 2 * T)
        g, part_rows = lax.div(m, 2), pl.ds(pl.multiple_of(lax.rem(m, 2) * 2 * T, 2 * T), 2 * T)
        vectors = jnp.concatenate([comp[g * 16 + u, part_rows] for u in range(16)], axis=1)
        logit = nn(vectors, w[:, pl.ds(pl.multiple_of(p * W2, W2), W2)])
        shift = jnp.asarray(p * W2, F32)
        lse_m, tgt_m = lsec[rows, :], tgtc[rows, :] - shift
        for e in range(W2 // 128):
            prob = jnp.exp(logit[:, e * 128 : (e + 1) * 128] - lse_m)
            hot = jnp.where(lane_w + float(e * 128) == tgt_m, 1.0, 0.0)
            put(rows, e, prob - hot)

    def hold(m, carry):
        def put(rows, e, val):
            pbuf[rows, pl.ds(e * 128, 128)] = val

        block_logits(0, m, put)
        return carry

    lax.fori_loop(0, 4, hold, 0)
    on_partner(3, flip)

    tl_all = rc(tl.at[pl.ds(1, 31)], tl.at[pl.ds(1, 31)], tl_s, tl_r, partner_c)
    tl_all.wait_recv()
    target_logit = jnp.sum(tl[...], axis=0)
    coef_rows = []
    gml_rows = []
    for g in range(2):
        lse_g = info2[g, 0:4]
        lm_g = info2[g, 4:8]
        scale_g = info2[g, 8:9]
        weights = jnp.exp(lm_g + target_logit[g * K : (g + 1) * K] - lse_g)
        resp = weights / jnp.sum(weights, axis=0, keepdims=True)
        coef_rows.append(scale_g * resp)
        gml_rows.append(-scale_g * (resp - jnp.exp(lm_g)))
    table = jnp.concatenate(coef_rows + [jnp.zeros((120, 128), F32)], axis=0)
    cols = jnp.transpose(table)
    for g in range(2):
        for k in range(K):
            coefc[pl.ds(g * R + k * T, T), :] = jnp.broadcast_to(
                cols[:, g * K + k : g * K + k + 1], (T, 128)
            )
    mine = jnp.where(zl == 0, gml_rows[0], gml_rows[1])
    high = mine.astype(BF16).astype(F32)
    gmla[0] = jnp.concatenate([high, mine - high, jnp.zeros((8, T), F32)], axis=0).astype(BF16)
    for i in range(1, 4):
        rc(gmla.at[0], gmla.at[i], gm_s, gm_r, dev(x_=m4(x + (0, 1, -1, 2)[i]))).start()

    def ring(piece, me, right, left, r1, rf, ss, r1_sem, rf_sem, r1_all, rf_all):
        two, one, back = m4(me + 2), m4(me + 1), m4(me - 1)
        copies = (
            lambda: rc(piece(two, 0), r1(0), ss, r1_sem, right),
            lambda: rc(piece(one, 1), rf(0, 1), ss, rf_sem, right),
            lambda: rc(piece(two, 1), r1(1), ss, r1_sem, left),
            lambda: rc(piece(back, 0), rf(1, 0), ss, rf_sem, left),
            lambda: rc(piece(one, 0), rf(0, 0), ss, rf_sem, right),
            lambda: rc(piece(back, 1), rf(1, 1), ss, rf_sem, left),
        )

        def first(which=(0, 2, 1, 3)):
            for i in which:
                copies[i]().start()

        def add(ref, other):
            ref[...] = (ref[...].astype(F32) + other[...].astype(F32)).astype(BF16)

        def forward():
            rc(r1_all, r1_all, ss, r1_sem, right).wait_recv()
            add(piece(one, 0), r1(0))
            copies[4]().start()
            add(piece(back, 1), r1(1))
            copies[5]().start()

        def arrive():
            rc(rf_all, rf_all, ss, rf_sem, right).wait_recv()

        return first, forward, arrive

    x_right, x_left = dev(x_=m4(x + 1)), dev(x_=m4(x - 1))

    def x_ring(cc, e=None):
        lanes = pl.ds(0, C) if e is None else pl.ds(e * 128, 128)
        sem = 2 * cc if e is None else 2 * NC + 2 + 2 * e
        return ring(
            lambda t, h: part.at[cc, t * 2 + h, :, lanes],
            x,
            x_right,
            x_left,
            lambda i: r1x.at[cc, i, :, lanes],
            lambda i, h: rfx.at[cc, i, h, :, lanes],
            x_s,
            x_r.at[sem],
            x_r.at[sem + 1],
            r1x.at[cc, :, :, lanes],
            rfx.at[cc, :, :, :, lanes],
        )

    def grad_out(p, tiles, send=True):
        cols = pl.ds(p * W2, W2)
        order = ((2, 0), (2, 1), (1, 1), (-1, 0), (1, 0), (-1, 1), (0, 0), (0, 1))
        for i in tiles:
            step, h = order[i]
            t = m4(x + step)
            rows = pl.ds(pl.multiple_of(t * 512 + h * 256, 256), 256)
            res = nn(comp_t[rows, :], gl[:, cols]).astype(BF16)
            for e in range(2):
                part[2 * p + e, t * 2 + h] = res[:, e * C : (e + 1) * C]
            if send and i < 4:
                for e in range(2):
                    x_ring(2 * p + e)[0](((0, 2, 1, 3)[i],))

    def scale_first(m, carry):
        rows = pl.ds(pl.multiple_of(m * 2 * T, 2 * T), 2 * T)
        coef_m = coefc[rows, :]
        for e in range(W2 // 128):
            gl[rows, pl.ds(e * 128, 128)] = (coef_m * pbuf[rows, pl.ds(e * 128, 128)]).astype(BF16)
        return carry

    lax.fori_loop(0, 4, scale_first, 0)

    def grad_logits(p):
        def rows_of(m, carry):
            coef_m = coefc[pl.ds(pl.multiple_of(m * 2 * T, 2 * T), 2 * T), :]

            def put(rows, e, val):
                gl[rows, pl.ds(pl.multiple_of(p * W2 + e * 128, 128), 128)] = (coef_m * val).astype(
                    BF16
                )

            block_logits(p, m, put)
            return carry

        lax.fori_loop(0, 4, rows_of, 0)

    def comp_grad(bat):
        def tile(i, carry):
            g, h, j = lax.div(i, 4), lax.rem(lax.div(i, 2), 2), lax.rem(i, 2)
            rows = pl.ds(pl.multiple_of(g * R + bat * 2 * T, 2 * T), 2 * T)
            units = pl.ds(pl.multiple_of((h * 2 + j) * 512, 512), 512)
            res = nt(gl[rows, :], w[units, :])
            z_ = h * 2 + g
            for jj in range(4):
                y_ = j * 2 + jj // 2
                val = res[:, jj * 128 : (jj + 1) * 128].astype(BF16)
                gcb[jj % 2, 2 * bat, z_, y_] = val[0:T]
                gcb[jj % 2, 2 * bat + 1, y_, z_] = val[T : 2 * T]
            return carry

        lax.fori_loop(0, 8, tile, 0)
        two = pl.ds(2 * bat, 2)
        swap = rc(gcb.at[1 - c, two], rd.at[two], d_s.at[bat], d_r.at[bat], partner_c)
        swap.start()
        return swap

    def a_ring(k):
        me = z if k % 2 == 0 else y
        mk = (lambda p: dev(z_=p)) if k % 2 == 0 else (lambda p: dev(y_=p))
        return ring(
            lambda t, h: gcb.at[c, k, t, pl.ds(2 * h, 2)],
            me,
            mk(m4(me + 1)),
            mk(m4(me - 1)),
            lambda i: r1a.at[k, i],
            lambda i, h: rfa.at[k, i, h],
            a_s,
            a_r.at[2 * k],
            a_r.at[2 * k + 1],
            r1a.at[k],
            rfa.at[k],
        )

    def b_copies(k):
        first, me = (z, y) if k % 2 == 0 else (y, z)
        mk = (lambda p: dev(y_=p)) if k % 2 == 0 else (lambda p: dev(z_=p))
        return [
            rc(gcb.at[c, k, first, t], rfb.at[k, o - 1], b_s, b_r.at[k], mk(t))
            for o in range(1, 4)
            for t in [m4(me + o)]
        ]

    def merge(bat, swap):
        swap.wait_recv()

        def add(i, carry):
            p, q = lax.div(i, 4), lax.rem(i, 4)
            for k in (2 * bat, 2 * bat + 1):
                gcb[c, k, p, q] = (
                    gcb[c, k, p, q].astype(F32) + rd[k, p, q].astype(F32)
                ).astype(BF16)
            return carry

        lax.fori_loop(0, 16, add, 0)
        for k in (2 * bat, 2 * bat + 1):
            a_ring(k)[0]()

    def forward_a(bat):
        for k in (2 * bat, 2 * bat + 1):
            a_ring(k)[1]()

    def finish_a(bat):
        for k in (2 * bat, 2 * bat + 1):
            a_ring(k)[2]()
            me = z if k % 2 == 0 else y
            for h in range(2):
                for e in range(2):
                    q = 2 * h + e
                    gcb[c, k, me, q] = (
                        gcb[c, k, me, q].astype(F32)
                        + rfa[k, 0, h, e].astype(F32)
                        + rfa[k, 1, h, e].astype(F32)
                    ).astype(BF16)
            for cp in b_copies(k):
                cp.start()

    def finish_b(bat):
        for k in (2 * bat, 2 * bat + 1):
            rc(rfb.at[k], rfb.at[k], b_s, b_r.at[k], partner_c).wait_recv()
            first, me = (z, y) if k % 2 == 0 else (y, z)
            total = gcb[c, k, first, me].astype(F32)
            for o in range(3):
                total = total + rfb[k, o].astype(F32)
            cf = comp[zl * 16 + v, pl.ds(k * T, T)].astype(F32)
            gpx[k] = (total * (1.0 - cf * cf)).astype(BF16)

    def x_finish(cc, e=None):
        lanes = pl.ds(0, C) if e is None else pl.ds(e * 128, 128)
        x_ring(cc, e)[2]()
        for h in range(2):
            part[cc, x * 2 + h, :, lanes] = (
                part[cc, x * 2 + h, :, lanes].astype(F32)
                + rfx[cc, 0, h, :, lanes].astype(F32)
                + rfx[cc, 1, h, :, lanes].astype(F32)
            ).astype(BF16)
        if e is None:
            cols = pl.ds(pl.multiple_of(zl * VH + cc * C, C), C)
        else:
            cols = pl.ds(pl.multiple_of(zl * VH + cc * C + e * 128, 128), 128)
        dst = go_out.at[:, cols]
        rc(part.at[cc, x * 2 + 1 - zl, :, lanes], dst, zx_s, zx_r, partner_z).start()
        pltpu.make_async_copy(part.at[cc, x * 2 + zl, :, lanes], dst, zx_l).start()

    def last_ring(e):
        lanes = pl.ds(e * 128, 128)
        cc = NC - 1

        def piece(t, h):
            return part.at[cc, t * 2 + h, :, lanes]

        def rf(i, h):
            return rfx.at[cc, i, h, :, lanes]

        def r1(i):
            return r1x.at[cc, i, :, lanes]

        def half(h):
            return x_h.at[2 * e + h]

        two, one, back = m4(x + 2), m4(x + 1), m4(x - 1)
        leave, stay = m4(x + 1 - 2 * zl), m4(x - 1 + 2 * zl)
        r1_all = r1x.at[cc, :, :, lanes]

        def first():
            rc(piece(two, 0), r1(0), x_s, x_r.at[2 * NC + e], x_right).start()
            rc(piece(two, 1), r1(1), x_s, x_r.at[2 * NC + e], x_left).start()
            rc(
                piece(leave, 1 - zl), rf(zl, 1 - zl), x_s, half(1 - zl), dev(x_=leave)
            ).start()

        def forward():
            rc(r1_all, r1_all, x_s, x_r.at[2 * NC + e], x_right).wait_recv()
            for t, h in ((one, 0), (back, 1)):
                ref = piece(t, h)
                ref[...] = (ref[...].astype(F32) + r1(h)[...].astype(F32)).astype(BF16)
                rc(ref, rf(h, h), x_s, half(h), dev(x_=t)).start()

        def last():
            rc(piece(stay, zl), rf(1 - zl, zl), x_s, half(zl), dev(x_=stay)).start()

        def finish(h):
            got = rfx.at[cc, :, h, :, lanes]
            rc(got, got, x_s, half(h), x_right).wait_recv()
            ref = piece(x, h)
            ref[...] = (
                ref[...].astype(F32) + rf(0, h)[...].astype(F32) + rf(1, h)[...].astype(F32)
            ).astype(BF16)
            return ref, go_out.at[:, pl.ds(pl.multiple_of(zl * VH + cc * C + e * 128, 128), 128)]

        def cross():
            ref, dst = finish(1 - zl)
            rc(ref, dst, zx_s, zx_r, partner_z).start()

        def keep():
            ref, dst = finish(zl)
            pltpu.make_async_copy(ref, dst, zx_l).start()

        return first, forward, last, cross, keep

    first_half, second_half, every = range(4), range(4, 8), range(8)
    grad_out(0, every)
    grad_logits(1)
    grad_out(1, every)
    x_ring(0)[1]()
    grad_logits(2)
    grad_logits(3)
    x_ring(1)[1]()
    swap0 = comp_grad(0)
    x_ring(2)[1]()
    grad_out(2, first_half)
    merge(0, swap0)
    swap1 = comp_grad(1)
    forward_a(0)
    x_ring(3)[1]()
    grad_out(2, second_half)
    merge(1, swap1)
    finish_a(0)
    hs_all = rc(hs.at[pl.ds(1, 3)], hs.at[pl.ds(1, 3)], hs_s, hs_r, partner_c)
    hs_all.wait_recv()
    for i in range(4):
        hst[:, pl.ds(i * T, T)] = jnp.transpose(hs[i])
    grad_out(3, first_half, False)
    forward_a(1)
    grad_out(3, second_half, False)
    x_ring(4)[1]()
    finish_b(0)
    finish_a(1)
    x_finish(0)
    x_finish(1)
    x_finish(2)
    finish_b(1)

    def slot(i, r0=0, n=T):
        return gpall.at[:, pl.ds(i * T + r0, n)]

    g_copies = (
        rc(gpx, slot(1), g_s, g_r.at[0], x_right),
        rc(gpx, slot(2), g_s, g_r.at[1], x_left),
        rc(slot(1, 0, T // 2), slot(3, 0, T // 2), g_s, g_r.at[2], x_right),
        rc(slot(2, T // 2, T // 2), slot(3, T // 2, T // 2), g_s, g_r.at[2], x_left),
    )
    g_copies[0].start()
    g_copies[1].start()
    x_ring(6, 0)[0]()

    def h_copy(o):
        p = lax.rem(v + o, 16)
        to = (x, zl, lax.div(p, 8), lax.rem(lax.div(p, 2), 4), lax.rem(p, 2))
        return rc(hts.at[o], hrecv.at[o], h_s, h_r, to)

    def h_tile(o):
        p = lax.rem(v + o, 16)
        rows = pl.ds(pl.multiple_of(p * U, U), U)
        acc = nt(gpx[0], proj[0, rows, :])
        for k in range(1, K):
            acc = acc + nt(gpx[k], proj[k, rows, :])
        return acc

    def h_step(o, carry):
        hts[o] = h_tile(o).astype(BF16)
        h_copy(o).start()
        return carry

    lax.fori_loop(1, 9, h_step, 0)
    x_ring(6, 1)[0]()
    lax.fori_loop(9, 16, h_step, 0)
    hrecv[0] = h_tile(0).astype(BF16)
    gpall[:, pl.ds(0, T)] = gpx[...]
    x_finish(3)
    x_finish(4)
    g_copies[0].wait_recv()
    g_copies[2].start()
    g_copies[1].wait_recv()
    g_copies[3].start()
    x_ring(5)[1]()
    last_ring(0)[0]()

    rc(slot(3), slot(3), g_s, g_r.at[2], x_right).wait_recv()
    last_ring(1)[0]()

    def product(half, k):
        return nn(hst[pl.ds(pl.multiple_of(half * 256, 256), 256), :], gpall[k])

    def mix_product(half):
        rows = pl.ds(pl.multiple_of(half * 256, 256), 256)
        res = nt(gmla[0], hst[rows, pl.ds(0, T)])
        for i in range(1, 4):
            res = res + nt(gmla[i], hst[rows, pl.ds(i * T, T)])
        return res[0:4] + res[4:8]

    for k in range(K):
        prods[k] = product(1 - zl, k).astype(BF16)
    gm_all = rc(gmla.at[pl.ds(1, 3)], gmla.at[pl.ds(1, 3)], gm_s, gm_r, partner_c)
    gm_all.wait_recv()
    gms[...] = mix_product(1 - zl)
    p_copies = (
        rc(prods, prodr, p_s.at[0], p_r.at[0], partner_z),
        rc(gms, gmr, p_s.at[1], p_r.at[1], partner_z),
    )
    for cp in p_copies:
        cp.start()
    x_ring(6, 0)[1]()
    x_ring(6, 1)[1]()
    x_finish(5)
    last_ring(0)[1]()
    last_ring(1)[1]()
    last_ring(0)[2]()
    last_ring(1)[2]()
    x_finish(6, 0)
    x_finish(6, 1)
    last_ring(0)[3]()
    last_ring(1)[3]()
    h_all = rc(hts.at[pl.ds(1, 15)], hrecv.at[pl.ds(1, 15)], h_s, h_r, partner_c)
    h_all.wait_recv()
    mw = jnp.concatenate(
        [mix_t[:, pl.ds(own_cols, U)].astype(F32)] * 2 + [jnp.zeros((8, U), F32)], axis=0
    ).astype(BF16)
    gh = lax.dot_general(gmla[0], mw, (((0,), (0,)), ((), ())), preferred_element_type=F32)
    for o in range(16):
        gh = gh + hrecv[o].astype(F32)
    gh_v[...] = gh.astype(BF16)
    out_copies = (
        pltpu.make_async_copy(gh_v, gh_out, sem_o.at[0]),
        pltpu.make_async_copy(gp_v, gp_out, sem_o.at[1]),
        pltpu.make_async_copy(gm_v, gm_out, sem_o.at[2]),
    )
    out_copies[0].start()
    last_ring(0)[4]()
    last_ring(1)[4]()
    for cp in p_copies:
        cp.wait_recv()
    for k in range(K):
        gp_v[k] = (product(zl, k) + prodr[k].astype(F32)).astype(BF16)
    gm_v[...] = mix_product(zl) + gmr[...]
    out_copies[1].start()
    out_copies[2].start()

    for cp in (info_copy, swap0, swap1, *p_copies, tl_all, hs_all, h_all, gm_all):
        cp.wait_send()
    for ref, sem in (
        (comp.at[pl.ds(0, 31)], ag_s),
        (part.at[pl.ds(0, 6)], x_s),
        (part.at[0], zx_s),
        (gcb.at[0, pl.ds(0, 3)], a_s),
        (gcb.at[0, 0, pl.ds(0, 3)], b_s),
        (gpall.at[:, pl.ds(0, 3 * T)], g_s),
    ):
        rc(ref, ref, sem, zx_r, partner_z).wait_send()
    half_out = go_out.at[:, pl.ds(0, VH)]
    rc(half_out, half_out, zx_s, zx_r, partner_z).wait_recv()
    pltpu.make_async_copy(part.at[0], part.at[0], zx_l).wait()
    for cp in out_copies:
        cp.wait()


def place(gh, gm, gp, go, gh_o, gm_o, gp_o, go_o, b_gh, b_gm, b_gp, b_go, s_in, s_out):
    pairs = [(gh, b_gh, gh_o), (gm, b_gm, gm_o), (gp, b_gp, gp_o)]
    for i in range(8):
        rows = pl.ds(i * 32, 32)
        pairs.append((go.at[rows], b_go.at[rows], go_o.at[rows]))
    loads = [pltpu.make_async_copy(s, b, s_in.at[i]) for i, (s, b, _) in enumerate(pairs)]
    stores = [pltpu.make_async_copy(b, t, s_out.at[i]) for i, (_, b, t) in enumerate(pairs)]
    for cp in reversed(loads):
        cp.start()
    for i in reversed(range(len(pairs))):
        loads[i].wait()
        stores[i].start()
    for cp in stores:
        cp.wait()


def shards(hidden, mix_weight, proj_weight, out_weight, saved_lse, targets, loss_scale):
    hbm = pl.BlockSpec(memory_space=pltpu.HBM)
    dma = pltpu.SemaphoreType.DMA
    outs = (
        jax.ShapeDtypeStruct((T, U), BF16),
        jax.ShapeDtypeStruct((K, 256), F32),
        jax.ShapeDtypeStruct((K, 256, U), BF16),
        jax.ShapeDtypeStruct((256, VL), BF16),
    )
    found = pl.pallas_call(
        kernel,
        out_shape=outs,
        in_specs=[hbm] * 7,
        out_specs=(hbm, hbm, hbm, hbm),
        scratch_shapes=[
            pltpu.VMEM((K, D), BF16),
            pltpu.VMEM((K, T), F32),
            pltpu.VMEM((1, T), F32),
            pltpu.VMEM((1, T), jnp.int32),
            pltpu.VMEM((T, D), BF16),
            pltpu.VMEM((K, D, U), BF16),
            pltpu.VMEM((D, VH), BF16),
            pltpu.VMEM((32, R, U), BF16),
            pltpu.VMEM((D, 2 * R), BF16),
            pltpu.VMEM((2 * R, VH), BF16),
            pltpu.VMEM((NC, 8, 256, C), BF16),
            pltpu.VMEM((NC, 2, 256, C), BF16),
            pltpu.VMEM((NC, 2, 2, 256, C), BF16),
            pltpu.VMEM((2, 4, 4, 4, T, U), BF16),
            pltpu.VMEM((4, 4, 4, T, U), BF16),
            pltpu.VMEM((4, 2, 2, T, U), BF16),
            pltpu.VMEM((4, 2, 2, 2, T, U), BF16),
            pltpu.VMEM((4, 3, T, U), BF16),
            pltpu.VMEM((2 * T, D), BF16),
            pltpu.VMEM((4, T, 512), BF16),
            pltpu.VMEM((512, 4 * T), BF16),
            pltpu.VMEM((K, T, U), BF16),
            pltpu.VMEM((K, 4 * T, U), BF16),
            pltpu.VMEM((4, 16, T), BF16),
            pltpu.VMEM((K, 256, U), BF16),
            pltpu.VMEM((K, 256, U), BF16),
            pltpu.VMEM((K, 256), F32),
            pltpu.VMEM((K, 256), F32),
            pltpu.VMEM((16, T, U), BF16),
            pltpu.VMEM((16, T, U), BF16),
            pltpu.VMEM((2, 16, T), F32),
            pltpu.VMEM((2 * R, 128), F32),
            pltpu.VMEM((2 * R, 128), F32),
            pltpu.VMEM((2 * R, 128), F32),
            pltpu.VMEM((32, 8, T), F32),
            pltpu.VMEM((2 * K, T, U), F32),
            pltpu.VMEM((2 * R, W2), F32),
            pltpu.VMEM((T, U), BF16),
            pltpu.VMEM((K, 256), F32),
            pltpu.VMEM((K, 256, U), BF16),
            dma((7,)),
            dma((2,)),
            dma((2,)),
            dma((2,)),
            dma((3,)),
            dma,
            dma((34,)),
            dma,
            dma,
            dma,
            dma,
            dma,
            dma((22,)),
            dma((4,)),
            dma,
            dma,
            dma,
            dma((2,)),
            dma((2,)),
            dma,
            dma((8,)),
            dma,
            dma((4,)),
            dma,
            dma,
            dma,
            dma((3,)),
            dma,
            dma,
        ],
        compiler_params=pltpu.CompilerParams(
            collective_id=0, has_side_effects=True, vmem_limit_bytes=67043328
        ),
    )(
        mix_weight.T,
        saved_lse.T,
        loss_scale[None, :],
        targets[None, :],
        hidden,
        proj_weight,
        out_weight,
    )
    gh, gm, gp, go = pl.pallas_call(
        place,
        out_shape=outs,
        in_specs=[hbm] * 4,
        out_specs=(hbm,) * 4,
        scratch_shapes=[pltpu.VMEM(o.shape, o.dtype) for o in outs] + [dma((11,)), dma((11,))],
    )(*found)
    return gh, gm.T, gp, go


def solution(mesh):
    finer = Mesh(mesh.devices.reshape(4, 2, 2, 4, 2), AXES)
    in_specs = (
        P(DP, None),
        P(),
        P(None, None, VOC),
        P(None, VOC),
        P(DP, None),
        P(DP),
        P(DP),
    )
    out_specs = (P(DP, VOC), P(DP, None), P(None, DP, VOC), P(DP, VOC))
    return jax.shard_map(
        shards, mesh=finer, in_specs=in_specs, out_specs=out_specs, check_vma=False
    )
```

```python
import functools

import jax
import jax.numpy as jnp
from jax import lax
from jax.experimental import pallas as pl
from jax.experimental.pallas import tpu as pltpu
from jax.sharding import Mesh
from jax.sharding import PartitionSpec as P

AXES = ("x", "zl", "zh", "y", "c")
DP = ("x", "zl")
VOC = ("zh", "y", "c")
MESH_ID = pl.DeviceIdType.MESH
F32 = jnp.float32
BF16 = jnp.bfloat16

T = 128
K = 4
R = T * K
U = 128
D = 2048
VL = 4096
VH = VL // 2
NC = 8
C = VH // NC
W2 = 2 * C


def nt(a, b):
    return lax.dot_general(a, b, (((1,), (1,)), ((), ())), preferred_element_type=F32)


def nn(a, b):
    return lax.dot_general(a, b, (((1,), (0,)), ((), ())), preferred_element_type=F32)


def kernel(
    mix_hbm,
    lse_hbm,
    scale_hbm,
    target_hbm,
    hidden_hbm,
    proj_hbm,
    w_hbm,
    gh_out,
    gm_out,
    gp_out,
    go_out,
    mix_t,
    lse_t,
    scale,
    target,
    hidden,
    proj,
    w,
    comp,
    comp_t,
    gl,
    part,
    r1x,
    rfx,
    gcb,
    rd,
    r1a,
    rfa,
    rfb,
    wt,
    hs,
    hst,
    gpx,
    gpall,
    gmla,
    prods,
    prodr,
    gms,
    gmr,
    hts,
    hrecv,
    info2,
    lsec,
    coefc,
    tgtc,
    tl,
    tacc,
    pbuf,
    gh_v,
    gm_v,
    gp_v,
    sem_w,
    sem_i,
    p_s,
    p_r,
    sem_o,
    ag_s,
    ag_r,
    hs_s,
    hs_r,
    tl_s,
    tl_r,
    x_s,
    x_r,
    x_h,
    zx_s,
    zx_r,
    zx_l,
    d_s,
    d_r,
    a_s,
    a_r,
    b_s,
    b_r,
    h_s,
    h_r,
    g_s,
    g_r,
    gm_s,
    gm_r,
):
    x = lax.axis_index("x")
    zl = lax.axis_index("zl")
    zh = lax.axis_index("zh")
    y = lax.axis_index("y")
    c = lax.axis_index("c")
    z = zh * 2 + zl
    v = zh * 8 + y * 2 + c
    d = x * 2 + zl

    def m4(i):
        return lax.rem(i + 4, 4)

    def dev(x_=None, z_=None, y_=None, c_=None):
        zz = z if z_ is None else z_
        return (
            x if x_ is None else x_,
            lax.rem(zz, 2),
            lax.div(zz, 2),
            y if y_ is None else y_,
            c if c_ is None else c_,
        )

    def rc(src, dst, ss, rs, to):
        return pltpu.make_async_remote_copy(
            src_ref=src, dst_ref=dst, send_sem=ss, recv_sem=rs, device_id=to, device_id_type=MESH_ID
        )

    partner_c = dev(c_=1 - c)
    partner_z = (x, 1 - zl, zh, y, c)

    hidden_copy = pltpu.make_async_copy(hidden_hbm, hidden, sem_w.at[0])
    proj_copy = pltpu.make_async_copy(proj_hbm, proj, sem_w.at[1])
    w_copy = pltpu.make_async_copy(
        w_hbm.at[:, pl.ds(pl.multiple_of(zl * VH, VH), VH)], w, sem_w.at[2]
    )
    small_copies = [
        pltpu.make_async_copy(src, dst, sem_w.at[3 + i])
        for i, (src, dst) in enumerate(
            ((mix_hbm, mix_t), (lse_hbm, lse_t), (scale_hbm, scale), (target_hbm, target))
        )
    ]
    hidden_copy.start()
    proj_copy.start()

    q32 = z * 8 + y * 2 + c

    def mate(o):
        p = lax.rem(q32 + o, 32)
        zz = lax.div(p, 8)
        return (x, lax.rem(zz, 2), lax.div(zz, 2), lax.rem(lax.div(p, 2), 4), lax.rem(p, 2))

    barrier = pltpu.get_barrier_semaphore()

    def greet(o, carry):
        pl.semaphore_signal(barrier, inc=1, device_id=mate(o), device_id_type=MESH_ID)
        return carry

    lax.fori_loop(1, 32, greet, 0)
    for o in range(1, 4):
        pl.semaphore_signal(barrier, inc=1, device_id=dev(x_=m4(x + o)), device_id_type=MESH_ID)

    own_cols = pl.multiple_of(v * U, U)

    def blk(col, z_, y_, c_, r0=0, n=2 * T):
        block = lax.rem(z_, 2) * 16 + lax.div(z_, 2) * 8 + y_ * 2 + c_
        return comp.at[block, pl.ds(col * 2 * T + r0, n)]

    def pos(col):
        return (y, z) if col == 0 else (z, y)

    def at_ab(col, a_, b_, c_, r0=0, n=2 * T):
        return blk(col, b_, a_, c_, r0, n) if col == 0 else blk(col, a_, b_, c_, r0, n)

    def dev_ab(col, a_, b_):
        return dev(y_=a_, z_=b_) if col == 0 else dev(z_=a_, y_=b_)

    def ag_copy(col, i, ref, to):
        r = 30 + i if col is None else col * 15 + i
        return rc(ref, ref, ag_s, ag_r.at[r], to)

    def ag_send(col, i, ref, to):
        ag_copy(col, i, ref, to).start()

    def ag_wait(col, i, ref):
        ag_copy(col, i, ref, partner_c).wait_recv()

    def second(col, i, ref):
        a, b = pos(col)
        ag_send(col, 3 + 3 * i, ref, dev_ab(col, a, m4(b + 1)))
        ag_send(col, 3 + 3 * i + 1, ref, dev_ab(col, a, m4(b - 1)))

    def across(i, ref):
        ag_send(None, i, ref, partner_c)

    def flip(col, a_, b_, c_):
        z_, y_ = (b_, a_) if col == 0 else (a_, b_)
        row = pl.multiple_of(lax.rem(z_, 2) * R + col * 2 * T, 2 * T)
        unit = lax.div(z_, 2) * 8 + y_ * 2 + c_
        comp_t[pl.ds(pl.multiple_of(unit * U, U), U), pl.ds(row, 2 * T)] = jnp.transpose(
            comp[lax.rem(z_, 2) * 16 + unit, pl.ds(col * 2 * T, 2 * T)]
        )

    def gauge(col, a_, b_, c_):
        z_, y_ = (b_, a_) if col == 0 else (a_, b_)
        g = lax.rem(z_, 2)
        unit = lax.div(z_, 2) * 8 + y_ * 2 + c_
        weight = wt[
            pl.ds(pl.multiple_of(g * T, T), T), pl.ds(pl.multiple_of(unit * U, U), U)
        ].astype(F32)
        for k in (2 * col, 2 * col + 1):
            tacc[g * K + k] += comp[g * 16 + unit, pl.ds(k * T, T)].astype(F32) * weight

    hidden_copy.wait()
    proj_copy.wait()
    for cp in small_copies:
        cp.start()
    w_copy.start()
    pre = jnp.tanh(nn(hidden[...], jnp.concatenate([proj[k] for k in range(K)], axis=1)))
    for k in range(K):
        comp[zl * 16 + v, pl.ds(k * T, T)] = pre[:, k * U : (k + 1) * U].astype(BF16)
    pl.semaphore_wait(barrier, 34)
    for col in range(2):
        a, b = pos(col)
        own = at_ab(col, a, b, c)
        ag_send(col, 0, own, dev_ab(col, m4(a + 1), b))
        ag_send(col, 1, own, dev_ab(col, m4(a - 1), b))

    for cp in small_copies:
        cp.wait()
    mix_logits = nt(mix_t[...], hidden[...])
    info2[zl, 0:4] = lse_t[...]
    info2[zl, 4:8] = mix_logits - jnp.log(jnp.sum(jnp.exp(mix_logits), axis=0, keepdims=True))
    info2[zl, 8:9] = scale[...]
    info2[zl, 9:10] = target[...].astype(F32)
    info2[zl, 10:16] = jnp.zeros((6, T), F32)

    def row_columns(g):
        cols = jnp.transpose(jnp.concatenate([info2[g], jnp.zeros((112, T), F32)], axis=0))
        local = cols[:, 9:10] - (v * VL + zl * VH).astype(F32)
        for k in range(K):
            rows = pl.ds(pl.multiple_of(g * R + k * T, T), T)
            lsec[rows, :] = jnp.broadcast_to(cols[:, k : k + 1], (T, 128))
            tgtc[rows, :] = jnp.broadcast_to(local, (T, 128))

    row_columns(zl)
    info_copy = rc(info2.at[zl], info2.at[zl], sem_i.at[0], sem_i.at[1], partner_z)
    info_copy.start()

    for col in range(2):
        a, b = pos(col)
        own = at_ab(col, a, b, c)
        second(col, 0, own)
        across(0, own)

    def hs_copy(i):
        p = m4(x + (0, 1, -1, 2)[i])
        return rc(
            hidden.at[:, pl.ds(pl.multiple_of(p * 512, 512), 512)], hs.at[i], hs_s, hs_r, dev(x_=p)
        )

    for i in range(1, 4):
        hs_copy(i).start()
    hs[0] = hidden[:, pl.ds(pl.multiple_of(x * 512, 512), 512)]

    def pick(n, carry):
        rows = pl.ds(pl.multiple_of(n * 512, 512), 512)
        acc = jnp.zeros((2 * T, 512), F32)
        for q in range(4):
            lane = lax.broadcasted_iota(jnp.int32, (T, 512), 1).astype(F32) + float(q * 512)
            hot = jnp.concatenate(
                [
                    (lane == tgtc[pl.ds(g * R, T), :][:, 0:1]).astype(F32).astype(BF16)
                    for g in range(2)
                ],
                axis=0,
            )
            acc = acc + nt(hot, w[rows, pl.ds(q * 512, 512)])
        wt[:, rows] = acc.astype(BF16)
        return carry

    for col in range(2):
        a, b = pos(col)
        prev, nxt = m4(a - 1), m4(a + 1)
        ag_wait(col, 0, at_ab(col, prev, b, c))
        ag_send(col, 2, at_ab(col, prev, b, c, 0, T), dev_ab(col, nxt, b))
        ag_wait(col, 1, at_ab(col, nxt, b, c))
        ag_send(col, 2, at_ab(col, nxt, b, c, T, T), dev_ab(col, prev, b))
    for i, step in ((1, -1), (2, 1)):
        for col in range(2):
            a, b = pos(col)
            second(col, i, at_ab(col, m4(a + step), b, c))
            across(i, at_ab(col, m4(a + step), b, c))

    def near(i):
        for col in range(2):
            a, b = pos(col)
            a_ = m4(a + (0, -1, 1, 2)[i])
            prev, nxt = m4(b - 1), m4(b + 1)
            ag_wait(col, 3 + 3 * i, at_ab(col, a_, prev, c))
            ag_send(col, 3 + 3 * i + 2, at_ab(col, a_, prev, c, 0, T), dev_ab(col, a, nxt))
            ag_wait(col, 3 + 3 * i + 1, at_ab(col, a_, nxt, c))
            ag_send(col, 3 + 3 * i + 2, at_ab(col, a_, nxt, c, T, T), dev_ab(col, a, prev))
            across(i, at_ab(col, a_, prev, c))
            across(i, at_ab(col, a_, nxt, c))

    def flip_near(i):
        for col in range(2):
            a, b = pos(col)
            a_ = m4(a + (0, -1, 1, 2)[i])
            for step in (0, -1, 1):
                flip(col, a_, m4(b + step), c)
                gauge(col, a_, m4(b + step), c)

    def far(i):
        for col in range(2):
            a, b = pos(col)
            a_ = m4(a + (0, -1, 1, 2)[i])
            b_ = m4(b + 2)
            ag_wait(col, 3 + 3 * i + 2, at_ab(col, a_, b_, c))
            across(i, at_ab(col, a_, b_, c))
            flip(col, a_, b_, c)
            gauge(col, a_, b_, c)

    def partner_wait(i):
        ag_wait(None, i, comp.at[pl.ds(0, 4)])

    def on_partner(i, act):
        for col in range(2):
            a, b = pos(col)
            a_ = m4(a + (0, -1, 1, 2)[i])

            def step(b_, carry):
                act(col, a_, b_, 1 - c)
                return carry

            lax.fori_loop(0, 4, step, 0)

    def both(*where):
        flip(*where)
        gauge(*where)

    tacc[...] = jnp.zeros_like(tacc)
    near(0)
    info_in = rc(info2.at[1 - zl], info2.at[1 - zl], sem_i.at[0], sem_i.at[1], partner_z)
    info_in.wait_recv()
    row_columns(1 - zl)
    w_copy.wait()
    lax.fori_loop(0, 2, pick, 0)
    for col in range(2):
        a, b = pos(col)
        two = m4(a + 2)
        ag_wait(col, 2, at_ab(col, two, b, c))
        second(col, 3, at_ab(col, two, b, c))
        across(3, at_ab(col, two, b, c))
    lax.fori_loop(2, 4, pick, 0)
    near(1)
    near(2)
    for i in range(3):
        flip_near(i)
    far(0)
    near(3)
    partner_wait(0)
    on_partner(0, both)
    far(1)
    far(2)
    flip_near(3)
    partner_wait(1)
    on_partner(1, both)
    partner_wait(2)
    on_partner(2, both)
    far(3)
    partner_wait(3)
    on_partner(3, gauge)

    lane_t = lax.broadcasted_iota(jnp.int32, (T, 128), 1)
    acc = jnp.zeros((T, 128), F32)
    for g in range(2):
        for k in range(K):
            acc = jnp.where(lane_t == g * K + k, jnp.sum(tacc[g * K + k], axis=1, keepdims=True), acc)
    tl[0] = jnp.transpose(acc)[0:8]

    def tl_copy(o):
        return rc(tl.at[0], tl.at[o], tl_s, tl_r, mate(o))

    def tl_start(o, carry):
        tl_copy(o).start()
        return carry

    lax.fori_loop(1, 32, tl_start, 0)

    lane_w = lax.broadcasted_iota(jnp.int32, (2 * T, 128), 1).astype(F32)

    def block_logits(p, m, put):
        rows = pl.ds(pl.multiple_of(m * 2 * T, 2 * T), 2 * T)
        g, part_rows = lax.div(m, 2), pl.ds(pl.multiple_of(lax.rem(m, 2) * 2 * T, 2 * T), 2 * T)
        vectors = jnp.concatenate([comp[g * 16 + u, part_rows] for u in range(16)], axis=1)
        logit = nn(vectors, w[:, pl.ds(pl.multiple_of(p * W2, W2), W2)])
        shift = jnp.asarray(p * W2, F32)
        lse_m, tgt_m = lsec[rows, :], tgtc[rows, :] - shift
        for e in range(W2 // 128):
            prob = jnp.exp(logit[:, e * 128 : (e + 1) * 128] - lse_m)
            hot = jnp.where(lane_w + float(e * 128) == tgt_m, 1.0, 0.0)
            put(rows, e, prob - hot)

    def hold(m, carry):
        def put(rows, e, val):
            pbuf[rows, pl.ds(e * 128, 128)] = val

        block_logits(0, m, put)
        return carry

    lax.fori_loop(0, 4, hold, 0)
    on_partner(3, flip)

    tl_all = rc(tl.at[pl.ds(1, 31)], tl.at[pl.ds(1, 31)], tl_s, tl_r, partner_c)
    tl_all.wait_recv()
    target_logit = jnp.sum(tl[...], axis=0)
    coef_rows = []
    gml_rows = []
    for g in range(2):
        lse_g = info2[g, 0:4]
        lm_g = info2[g, 4:8]
        scale_g = info2[g, 8:9]
        weights = jnp.exp(lm_g + target_logit[g * K : (g + 1) * K] - lse_g)
        resp = weights / jnp.sum(weights, axis=0, keepdims=True)
        coef_rows.append(scale_g * resp)
        gml_rows.append(-scale_g * (resp - jnp.exp(lm_g)))
    table = jnp.concatenate(coef_rows + [jnp.zeros((120, 128), F32)], axis=0)
    cols = jnp.transpose(table)
    for g in range(2):
        for k in range(K):
            coefc[pl.ds(g * R + k * T, T), :] = jnp.broadcast_to(
                cols[:, g * K + k : g * K + k + 1], (T, 128)
            )
    mine = jnp.where(zl == 0, gml_rows[0], gml_rows[1])
    high = mine.astype(BF16).astype(F32)
    gmla[0] = jnp.concatenate([high, mine - high, jnp.zeros((8, T), F32)], axis=0).astype(BF16)
    for i in range(1, 4):
        rc(gmla.at[0], gmla.at[i], gm_s, gm_r, dev(x_=m4(x + (0, 1, -1, 2)[i]))).start()

    def ring(piece, me, right, left, r1, rf, ss, r1_sem, rf_sem, r1_all, rf_all):
        two, one, back = m4(me + 2), m4(me + 1), m4(me - 1)
        copies = (
            lambda: rc(piece(two, 0), r1(0), ss, r1_sem, right),
            lambda: rc(piece(one, 1), rf(0, 1), ss, rf_sem, right),
            lambda: rc(piece(two, 1), r1(1), ss, r1_sem, left),
            lambda: rc(piece(back, 0), rf(1, 0), ss, rf_sem, left),
            lambda: rc(piece(one, 0), rf(0, 0), ss, rf_sem, right),
            lambda: rc(piece(back, 1), rf(1, 1), ss, rf_sem, left),
        )

        def first(which=(0, 2, 1, 3)):
            for i in which:
                copies[i]().start()

        def add(ref, other):
            ref[...] = (ref[...].astype(F32) + other[...].astype(F32)).astype(BF16)

        def forward():
            rc(r1_all, r1_all, ss, r1_sem, right).wait_recv()
            add(piece(one, 0), r1(0))
            copies[4]().start()
            add(piece(back, 1), r1(1))
            copies[5]().start()

        def arrive():
            rc(rf_all, rf_all, ss, rf_sem, right).wait_recv()

        return first, forward, arrive

    x_right, x_left = dev(x_=m4(x + 1)), dev(x_=m4(x - 1))

    def x_ring(cc, e=None):
        lanes = pl.ds(0, C) if e is None else pl.ds(e * 128, 128)
        sem = 2 * cc if e is None else 2 * NC + 2 + 2 * e
        return ring(
            lambda t, h: part.at[cc, t * 2 + h, :, lanes],
            x,
            x_right,
            x_left,
            lambda i: r1x.at[cc, i, :, lanes],
            lambda i, h: rfx.at[cc, i, h, :, lanes],
            x_s,
            x_r.at[sem],
            x_r.at[sem + 1],
            r1x.at[cc, :, :, lanes],
            rfx.at[cc, :, :, :, lanes],
        )

    def grad_out(p, tiles, send=True):
        cols = pl.ds(p * W2, W2)
        order = ((2, 0), (2, 1), (1, 1), (-1, 0), (1, 0), (-1, 1), (0, 0), (0, 1))
        for i in tiles:
            step, h = order[i]
            t = m4(x + step)
            rows = pl.ds(pl.multiple_of(t * 512 + h * 256, 256), 256)
            res = nn(comp_t[rows, :], gl[:, cols]).astype(BF16)
            for e in range(2):
                part[2 * p + e, t * 2 + h] = res[:, e * C : (e + 1) * C]
            if send and i < 4:
                for e in range(2):
                    x_ring(2 * p + e)[0](((0, 2, 1, 3)[i],))

    def scale_first(m, carry):
        rows = pl.ds(pl.multiple_of(m * 2 * T, 2 * T), 2 * T)
        coef_m = coefc[rows, :]
        for e in range(W2 // 128):
            gl[rows, pl.ds(e * 128, 128)] = (coef_m * pbuf[rows, pl.ds(e * 128, 128)]).astype(BF16)
        return carry

    lax.fori_loop(0, 4, scale_first, 0)

    def grad_logits(p):
        def rows_of(m, carry):
            coef_m = coefc[pl.ds(pl.multiple_of(m * 2 * T, 2 * T), 2 * T), :]

            def put(rows, e, val):
                gl[rows, pl.ds(pl.multiple_of(p * W2 + e * 128, 128), 128)] = (coef_m * val).astype(
                    BF16
                )

            block_logits(p, m, put)
            return carry

        lax.fori_loop(0, 4, rows_of, 0)

    def comp_grad(bat):
        def tile(i, carry):
            g, h, j = lax.div(i, 4), lax.rem(lax.div(i, 2), 2), lax.rem(i, 2)
            rows = pl.ds(pl.multiple_of(g * R + bat * 2 * T, 2 * T), 2 * T)
            units = pl.ds(pl.multiple_of((h * 2 + j) * 512, 512), 512)
            res = nt(gl[rows, :], w[units, :])
            z_ = h * 2 + g
            for jj in range(4):
                y_ = j * 2 + jj // 2
                val = res[:, jj * 128 : (jj + 1) * 128].astype(BF16)
                gcb[jj % 2, 2 * bat, z_, y_] = val[0:T]
                gcb[jj % 2, 2 * bat + 1, y_, z_] = val[T : 2 * T]
            return carry

        lax.fori_loop(0, 8, tile, 0)
        two = pl.ds(2 * bat, 2)
        swap = rc(gcb.at[1 - c, two], rd.at[two], d_s.at[bat], d_r.at[bat], partner_c)
        swap.start()
        return swap

    def a_ring(k):
        me = z if k % 2 == 0 else y
        mk = (lambda p: dev(z_=p)) if k % 2 == 0 else (lambda p: dev(y_=p))
        return ring(
            lambda t, h: gcb.at[c, k, t, pl.ds(2 * h, 2)],
            me,
            mk(m4(me + 1)),
            mk(m4(me - 1)),
            lambda i: r1a.at[k, i],
            lambda i, h: rfa.at[k, i, h],
            a_s,
            a_r.at[2 * k],
            a_r.at[2 * k + 1],
            r1a.at[k],
            rfa.at[k],
        )

    def b_copies(k):
        first, me = (z, y) if k % 2 == 0 else (y, z)
        mk = (lambda p: dev(y_=p)) if k % 2 == 0 else (lambda p: dev(z_=p))
        return [
            rc(gcb.at[c, k, first, t], rfb.at[k, o - 1], b_s, b_r.at[k], mk(t))
            for o in range(1, 4)
            for t in [m4(me + o)]
        ]

    def merge(bat, swap):
        swap.wait_recv()

        def add(i, carry):
            p, q = lax.div(i, 4), lax.rem(i, 4)
            for k in (2 * bat, 2 * bat + 1):
                gcb[c, k, p, q] = (
                    gcb[c, k, p, q].astype(F32) + rd[k, p, q].astype(F32)
                ).astype(BF16)
            return carry

        lax.fori_loop(0, 16, add, 0)
        for k in (2 * bat, 2 * bat + 1):
            a_ring(k)[0]()

    def forward_a(bat):
        for k in (2 * bat, 2 * bat + 1):
            a_ring(k)[1]()

    def finish_a(bat):
        for k in (2 * bat, 2 * bat + 1):
            a_ring(k)[2]()
            me = z if k % 2 == 0 else y
            for h in range(2):
                for e in range(2):
                    q = 2 * h + e
                    gcb[c, k, me, q] = (
                        gcb[c, k, me, q].astype(F32)
                        + rfa[k, 0, h, e].astype(F32)
                        + rfa[k, 1, h, e].astype(F32)
                    ).astype(BF16)
            for cp in b_copies(k):
                cp.start()

    def finish_b(bat):
        for k in (2 * bat, 2 * bat + 1):
            rc(rfb.at[k], rfb.at[k], b_s, b_r.at[k], partner_c).wait_recv()
            first, me = (z, y) if k % 2 == 0 else (y, z)
            total = gcb[c, k, first, me].astype(F32)
            for o in range(3):
                total = total + rfb[k, o].astype(F32)
            cf = comp[zl * 16 + v, pl.ds(k * T, T)].astype(F32)
            gpx[k] = (total * (1.0 - cf * cf)).astype(BF16)

    def x_finish(cc, e=None):
        lanes = pl.ds(0, C) if e is None else pl.ds(e * 128, 128)
        x_ring(cc, e)[2]()
        for h in range(2):
            part[cc, x * 2 + h, :, lanes] = (
                part[cc, x * 2 + h, :, lanes].astype(F32)
                + rfx[cc, 0, h, :, lanes].astype(F32)
                + rfx[cc, 1, h, :, lanes].astype(F32)
            ).astype(BF16)
        if e is None:
            cols = pl.ds(pl.multiple_of(zl * VH + cc * C, C), C)
        else:
            cols = pl.ds(pl.multiple_of(zl * VH + cc * C + e * 128, 128), 128)
        dst = go_out.at[:, cols]
        rc(part.at[cc, x * 2 + 1 - zl, :, lanes], dst, zx_s, zx_r, partner_z).start()
        pltpu.make_async_copy(part.at[cc, x * 2 + zl, :, lanes], dst, zx_l).start()

    def last_ring(e):
        lanes = pl.ds(e * 128, 128)
        cc = NC - 1

        def piece(t, h):
            return part.at[cc, t * 2 + h, :, lanes]

        def rf(i, h):
            return rfx.at[cc, i, h, :, lanes]

        def r1(i):
            return r1x.at[cc, i, :, lanes]

        def half(h):
            return x_h.at[2 * e + h]

        two, one, back = m4(x + 2), m4(x + 1), m4(x - 1)
        leave, stay = m4(x + 1 - 2 * zl), m4(x - 1 + 2 * zl)
        r1_all = r1x.at[cc, :, :, lanes]

        def first():
            rc(piece(two, 0), r1(0), x_s, x_r.at[2 * NC + e], x_right).start()
            rc(piece(two, 1), r1(1), x_s, x_r.at[2 * NC + e], x_left).start()
            rc(
                piece(leave, 1 - zl), rf(zl, 1 - zl), x_s, half(1 - zl), dev(x_=leave)
            ).start()

        def forward():
            rc(r1_all, r1_all, x_s, x_r.at[2 * NC + e], x_right).wait_recv()
            for t, h in ((one, 0), (back, 1)):
                ref = piece(t, h)
                ref[...] = (ref[...].astype(F32) + r1(h)[...].astype(F32)).astype(BF16)
                rc(ref, rf(h, h), x_s, half(h), dev(x_=t)).start()

        def last():
            rc(piece(stay, zl), rf(1 - zl, zl), x_s, half(zl), dev(x_=stay)).start()

        def finish(h):
            got = rfx.at[cc, :, h, :, lanes]
            rc(got, got, x_s, half(h), x_right).wait_recv()
            ref = piece(x, h)
            ref[...] = (
                ref[...].astype(F32) + rf(0, h)[...].astype(F32) + rf(1, h)[...].astype(F32)
            ).astype(BF16)
            return ref, go_out.at[:, pl.ds(pl.multiple_of(zl * VH + cc * C + e * 128, 128), 128)]

        def cross():
            ref, dst = finish(1 - zl)
            rc(ref, dst, zx_s, zx_r, partner_z).start()

        def keep():
            ref, dst = finish(zl)
            pltpu.make_async_copy(ref, dst, zx_l).start()

        return first, forward, last, cross, keep

    first_half, second_half, every = range(4), range(4, 8), range(8)
    grad_out(0, every)
    grad_logits(1)
    grad_out(1, every)
    x_ring(0)[1]()
    grad_logits(2)
    grad_logits(3)
    x_ring(1)[1]()
    swap0 = comp_grad(0)
    x_ring(2)[1]()
    grad_out(2, first_half)
    merge(0, swap0)
    swap1 = comp_grad(1)
    forward_a(0)
    x_ring(3)[1]()
    grad_out(2, second_half)
    merge(1, swap1)
    finish_a(0)
    hs_all = rc(hs.at[pl.ds(1, 3)], hs.at[pl.ds(1, 3)], hs_s, hs_r, partner_c)
    hs_all.wait_recv()
    for i in range(4):
        hst[:, pl.ds(i * T, T)] = jnp.transpose(hs[i])
    grad_out(3, first_half, False)
    forward_a(1)
    grad_out(3, second_half, False)
    x_ring(4)[1]()
    finish_b(0)
    finish_a(1)
    x_finish(0)
    x_finish(1)
    x_finish(2)
    finish_b(1)

    def slot(i, r0=0, n=T):
        return gpall.at[:, pl.ds(i * T + r0, n)]

    g_copies = (
        rc(gpx, slot(1), g_s, g_r.at[0], x_right),
        rc(gpx, slot(2), g_s, g_r.at[1], x_left),
        rc(slot(1, 0, T // 2), slot(3, 0, T // 2), g_s, g_r.at[2], x_right),
        rc(slot(2, T // 2, T // 2), slot(3, T // 2, T // 2), g_s, g_r.at[2], x_left),
    )
    g_copies[0].start()
    g_copies[1].start()
    x_ring(6, 0)[0]()

    def h_copy(o):
        p = lax.rem(v + o, 16)
        to = (x, zl, lax.div(p, 8), lax.rem(lax.div(p, 2), 4), lax.rem(p, 2))
        return rc(hts.at[o], hrecv.at[o], h_s, h_r, to)

    def h_tile(o):
        p = lax.rem(v + o, 16)
        rows = pl.ds(pl.multiple_of(p * U, U), U)
        acc = nt(gpx[0], proj[0, rows, :])
        for k in range(1, K):
            acc = acc + nt(gpx[k], proj[k, rows, :])
        return acc

    def h_step(o, carry):
        hts[o] = h_tile(o).astype(BF16)
        h_copy(o).start()
        return carry

    lax.fori_loop(1, 9, h_step, 0)
    x_ring(6, 1)[0]()
    lax.fori_loop(9, 16, h_step, 0)
    hrecv[0] = h_tile(0).astype(BF16)
    gpall[:, pl.ds(0, T)] = gpx[...]
    x_finish(3)
    x_finish(4)
    g_copies[0].wait_recv()
    g_copies[2].start()
    g_copies[1].wait_recv()
    g_copies[3].start()
    x_ring(5)[1]()
    last_ring(0)[0]()

    rc(slot(3), slot(3), g_s, g_r.at[2], x_right).wait_recv()
    x_ring(6, 0)[1]()
    x_ring(6, 1)[1]()
    last_ring(1)[0]()

    def product(half, k):
        return nn(hst[pl.ds(pl.multiple_of(half * 256, 256), 256), :], gpall[k])

    def mix_product(half):
        rows = pl.ds(pl.multiple_of(half * 256, 256), 256)
        res = nt(gmla[0], hst[rows, pl.ds(0, T)])
        for i in range(1, 4):
            res = res + nt(gmla[i], hst[rows, pl.ds(i * T, T)])
        return res[0:4] + res[4:8]

    for k in range(K):
        prods[k] = product(1 - zl, k).astype(BF16)
    gm_all = rc(gmla.at[pl.ds(1, 3)], gmla.at[pl.ds(1, 3)], gm_s, gm_r, partner_c)
    gm_all.wait_recv()
    gms[...] = mix_product(1 - zl)
    p_copies = (
        rc(prods, prodr, p_s.at[0], p_r.at[0], partner_z),
        rc(gms, gmr, p_s.at[1], p_r.at[1], partner_z),
    )
    for cp in p_copies:
        cp.start()
    x_finish(5)
    last_ring(0)[1]()
    last_ring(1)[1]()
    last_ring(0)[2]()
    last_ring(1)[2]()
    x_finish(6, 0)
    x_finish(6, 1)
    last_ring(0)[3]()
    last_ring(1)[3]()
    h_all = rc(hts.at[pl.ds(1, 15)], hrecv.at[pl.ds(1, 15)], h_s, h_r, partner_c)
    h_all.wait_recv()
    mw = jnp.concatenate(
        [mix_t[:, pl.ds(own_cols, U)].astype(F32)] * 2 + [jnp.zeros((8, U), F32)], axis=0
    ).astype(BF16)
    gh = lax.dot_general(gmla[0], mw, (((0,), (0,)), ((), ())), preferred_element_type=F32)
    for o in range(16):
        gh = gh + hrecv[o].astype(F32)
    gh_v[...] = gh.astype(BF16)
    out_copies = (
        pltpu.make_async_copy(gh_v, gh_out, sem_o.at[0]),
        pltpu.make_async_copy(gp_v, gp_out, sem_o.at[1]),
        pltpu.make_async_copy(gm_v, gm_out, sem_o.at[2]),
    )
    out_copies[0].start()
    last_ring(0)[4]()
    last_ring(1)[4]()
    for cp in p_copies:
        cp.wait_recv()
    for k in range(K):
        gp_v[k] = (product(zl, k) + prodr[k].astype(F32)).astype(BF16)
    gm_v[...] = mix_product(zl) + gmr[...]
    out_copies[1].start()
    out_copies[2].start()

    for cp in (info_copy, swap0, swap1, *p_copies, tl_all, hs_all, h_all, gm_all):
        cp.wait_send()
    for ref, sem in (
        (comp.at[pl.ds(0, 31)], ag_s),
        (part.at[pl.ds(0, 6)], x_s),
        (part.at[0], zx_s),
        (gcb.at[0, pl.ds(0, 3)], a_s),
        (gcb.at[0, 0, pl.ds(0, 3)], b_s),
        (gpall.at[:, pl.ds(0, 3 * T)], g_s),
    ):
        rc(ref, ref, sem, zx_r, partner_z).wait_send()
    half_out = go_out.at[:, pl.ds(0, VH)]
    rc(half_out, half_out, zx_s, zx_r, partner_z).wait_recv()
    pltpu.make_async_copy(part.at[0], part.at[0], zx_l).wait()
    for cp in out_copies:
        cp.wait()


def place(gh, gm, gp, go, gh_o, gm_o, gp_o, go_o, b_gh, b_gm, b_gp, b_go, s_in, s_out):
    pairs = [(gh, b_gh, gh_o), (gm, b_gm, gm_o), (gp, b_gp, gp_o)]
    for i in range(8):
        rows = pl.ds(i * 32, 32)
        pairs.append((go.at[rows], b_go.at[rows], go_o.at[rows]))
    loads = [pltpu.make_async_copy(s, b, s_in.at[i]) for i, (s, b, _) in enumerate(pairs)]
    stores = [pltpu.make_async_copy(b, t, s_out.at[i]) for i, (_, b, t) in enumerate(pairs)]
    for cp in reversed(loads):
        cp.start()
    for i in reversed(range(len(pairs))):
        loads[i].wait()
        stores[i].start()
    for cp in stores:
        cp.wait()


def shards(hidden, mix_weight, proj_weight, out_weight, saved_lse, targets, loss_scale):
    hbm = pl.BlockSpec(memory_space=pltpu.HBM)
    dma = pltpu.SemaphoreType.DMA
    outs = (
        jax.ShapeDtypeStruct((T, U), BF16),
        jax.ShapeDtypeStruct((K, 256), F32),
        jax.ShapeDtypeStruct((K, 256, U), BF16),
        jax.ShapeDtypeStruct((256, VL), BF16),
    )
    found = pl.pallas_call(
        kernel,
        out_shape=outs,
        in_specs=[hbm] * 7,
        out_specs=(hbm, hbm, hbm, hbm),
        scratch_shapes=[
            pltpu.VMEM((K, D), BF16),
            pltpu.VMEM((K, T), F32),
            pltpu.VMEM((1, T), F32),
            pltpu.VMEM((1, T), jnp.int32),
            pltpu.VMEM((T, D), BF16),
            pltpu.VMEM((K, D, U), BF16),
            pltpu.VMEM((D, VH), BF16),
            pltpu.VMEM((32, R, U), BF16),
            pltpu.VMEM((D, 2 * R), BF16),
            pltpu.VMEM((2 * R, VH), BF16),
            pltpu.VMEM((NC, 8, 256, C), BF16),
            pltpu.VMEM((NC, 2, 256, C), BF16),
            pltpu.VMEM((NC, 2, 2, 256, C), BF16),
            pltpu.VMEM((2, 4, 4, 4, T, U), BF16),
            pltpu.VMEM((4, 4, 4, T, U), BF16),
            pltpu.VMEM((4, 2, 2, T, U), BF16),
            pltpu.VMEM((4, 2, 2, 2, T, U), BF16),
            pltpu.VMEM((4, 3, T, U), BF16),
            pltpu.VMEM((2 * T, D), BF16),
            pltpu.VMEM((4, T, 512), BF16),
            pltpu.VMEM((512, 4 * T), BF16),
            pltpu.VMEM((K, T, U), BF16),
            pltpu.VMEM((K, 4 * T, U), BF16),
            pltpu.VMEM((4, 16, T), BF16),
            pltpu.VMEM((K, 256, U), BF16),
            pltpu.VMEM((K, 256, U), BF16),
            pltpu.VMEM((K, 256), F32),
            pltpu.VMEM((K, 256), F32),
            pltpu.VMEM((16, T, U), BF16),
            pltpu.VMEM((16, T, U), BF16),
            pltpu.VMEM((2, 16, T), F32),
            pltpu.VMEM((2 * R, 128), F32),
            pltpu.VMEM((2 * R, 128), F32),
            pltpu.VMEM((2 * R, 128), F32),
            pltpu.VMEM((32, 8, T), F32),
            pltpu.VMEM((2 * K, T, U), F32),
            pltpu.VMEM((2 * R, W2), F32),
            pltpu.VMEM((T, U), BF16),
            pltpu.VMEM((K, 256), F32),
            pltpu.VMEM((K, 256, U), BF16),
            dma((7,)),
            dma((2,)),
            dma((2,)),
            dma((2,)),
            dma((3,)),
            dma,
            dma((34,)),
            dma,
            dma,
            dma,
            dma,
            dma,
            dma((22,)),
            dma((4,)),
            dma,
            dma,
            dma,
            dma((2,)),
            dma((2,)),
            dma,
            dma((8,)),
            dma,
            dma((4,)),
            dma,
            dma,
            dma,
            dma((3,)),
            dma,
            dma,
        ],
        compiler_params=pltpu.CompilerParams(
            collective_id=0, has_side_effects=True, vmem_limit_bytes=67043328
        ),
    )(
        mix_weight.T,
        saved_lse.T,
        loss_scale[None, :],
        targets[None, :],
        hidden,
        proj_weight,
        out_weight,
    )
    gh, gm, gp, go = pl.pallas_call(
        place,
        out_shape=outs,
        in_specs=[hbm] * 4,
        out_specs=(hbm,) * 4,
        scratch_shapes=[pltpu.VMEM(o.shape, o.dtype) for o in outs] + [dma((11,)), dma((11,))],
    )(*found)
    return gh, gm.T, gp, go


def solution(mesh):
    finer = Mesh(mesh.devices.reshape(4, 2, 2, 4, 2), AXES)
    in_specs = (
        P(DP, None),
        P(),
        P(None, None, VOC),
        P(None, VOC),
        P(DP, None),
        P(DP),
        P(DP),
    )
    out_specs = (P(DP, VOC), P(DP, None), P(None, DP, VOC), P(DP, VOC))
    return jax.shard_map(
        shards, mesh=finer, in_specs=in_specs, out_specs=out_specs, check_vma=False
    )
```
